256 devices in a mesh: gx: 8 (over y, core), gy: 4 (over z_hi), gz: 8 (over z_lo, x).
Axes of the slice: x: 4, y: 4, z: 8 (z_hi: 4, z_lo: 2; z = z_hi * 2 + z_lo), core: 2. Of those that a mesh axis runs over, the one named last changes fastest.
Arguments:
- features: bfloat16 [32, 24, 32, 1024], P(None, 'gx', 'gy', 'gz'), may hold values from -6 to 6
- edge_state: bfloat16 [3, 32, 24, 32, 1024], P(None, None, 'gx', 'gy', 'gz'), may hold values from -6 to 6
- multiplicity: int32 [24, 32, 1024], P('gx', 'gy', 'gz'), may hold values from 0 to 8, as said below
- edge_in: bfloat16 [3, 32, 96], replicated, may hold values from -0.625 to 0.625
- edge_out: bfloat16 [3, 32, 32], replicated, may hold values from -1 to 1
- edge_bias: float32 [3, 32], replicated, may hold values from -3 to 3
- node_in: bfloat16 [3, 32, 64], replicated, may hold values from -0.75 to 0.75
- node_out: bfloat16 [3, 32, 32], replicated, may hold values from -1 to 1
- node_bias: float32 [3, 32], replicated, may hold values from -3 to 3
Outputs:
- updated_features: bfloat16 [32, 24, 32, 1024], P(None, 'gx', 'gy', 'gz')
The draws below stay inside these ranges and needn't reach their ends.
Inputs may be any that keep to these rules, and one draw needn't show every extreme that they name: multiplicity(n) is the number of fluid blocks that hold a stored copy of node n; copies are the shared outermost layers of adjacent blocks as described in the reference program, and the nodes inside a void block count 0.
All inputs are finite; a program needn't handle non-finite values.
Results may differ from the reference program's by a relative error of at most 0.009.
Values sent between devices are 32-bit elements; how exact they have to be, the bound alone decides.
No kernel may reach another device: no remote copies, remote signals or barrier semaphores. Data moves between devices by JAX's collectives and lax.ppermute only.
A program may use at most 64 MiB of HBM per device.

```python
import jax
import jax.numpy as jnp
from jax import lax

H = 32
LAYERS = 3
CX = 3
CY = 8
CZ = 128
NX = 24
NY = 32
NZ = 1024


def members(cells, width, blocks):
    position = jnp.arange(cells)[:, None]
    owner = position // width
    local_pos = position % width
    block_ids = jnp.arange(blocks)[None, :]
    held = (block_ids == owner) | (local_pos == width - 1) & (block_ids == owner + 1) | (local_pos == 0) & (block_ids == owner - 1)
    return held.astype(jnp.int32)


def draw_multiplicity(key, part):
    blocks_x, blocks_y, blocks_z = (NX // CX, NY // CY, NZ // CZ)
    chance = jax.random.randint(jax.random.fold_in(key, 11), (blocks_x, blocks_y, blocks_z), 0, 4)
    fluid = (chance < 3).astype(jnp.int32)
    index_x = jnp.arange(blocks_x)[:, None, None]
    index_y = jnp.arange(blocks_y)[None, :, None]
    index_z = jnp.arange(blocks_z)[None, None, :]
    corner = ((index_x < 2) & (index_y < 2) & (index_z < 2)).astype(jnp.int32)
    far_block = (index_x == blocks_x - 1) & (index_y == blocks_y - 1) & (index_z == blocks_z - 1)
    fluid = jnp.where(far_block, 0, jnp.maximum(fluid, corner)).astype(jnp.int32)
    held_x = members(NX, CX, blocks_x)
    held_y = members(NY, CY, blocks_y)
    held_z = members(NZ, CZ, blocks_z)
    return jnp.einsum('xa,yb,zc,abc->xyz', held_x, held_y, held_z, fluid).astype(jnp.int32)


def steps_of(stream_key, shape, cuts, smallest, largest):
    level, own = 1.0, jax.random.fold_in(stream_key, 6)
    for dim, parts in cuts:
        heights = jnp.exp(jax.random.uniform(jax.random.fold_in(own, dim), (parts,), jnp.float32, smallest / len(cuts), largest / len(cuts)))
        level = level * jnp.repeat(heights, shape[dim] // parts).reshape([-1 if axis == dim else 1 for axis in range(len(shape))])
    return level


def scatter_about(own_key, shape, scale, limit, pieces=(), dtype=jnp.bfloat16):
    values = jax.random.normal(own_key, shape, jnp.float32) * scale
    if len(pieces) > 0:
        values = steps_of(own_key, shape, pieces, -0.22, 0.18) * values
    return jnp.clip(values, min=-limit, max=limit).astype(dtype)


def setup_inputs(seed: int = 0) -> dict:
    arg_keys = jax.random.split(jax.random.key(seed), 10)
    return {
        "features": scatter_about(arg_keys[0], (H, NX, NY, NZ), 1.0, 6.0, ((1, 8), (2, 4), (3, 8))),
        "edge_state": scatter_about(arg_keys[1], (3, H, NX, NY, NZ), 1.0, 6.0, ((2, 8), (3, 4), (4, 8))),
        "multiplicity": draw_multiplicity(jax.random.fold_in(arg_keys[9], 71), 0),
        "edge_in": scatter_about(arg_keys[3], (LAYERS, H, 3 * H), (3 * H) ** -0.5, 0.625),
        "edge_out": scatter_about(arg_keys[4], (LAYERS, H, H), H ** -0.5, 1.0),
        "edge_bias": scatter_about(arg_keys[5], (LAYERS, H), 0.5, 3.0, (), jnp.float32),
        "node_in": scatter_about(arg_keys[6], (LAYERS, H, 2 * H), (2 * H) ** -0.5, 0.75),
        "node_out": scatter_about(arg_keys[7], (LAYERS, H, H), H ** -0.5, 1.0),
        "node_bias": scatter_about(arg_keys[8], (LAYERS, H), 0.5, 3.0, (), jnp.float32),
    }


def ahead(values, axis_pos):
    length = values.shape[axis_pos]
    remainder = lax.slice_in_dim(values, 1, length, axis=axis_pos)
    filler = jnp.zeros_like(lax.slice_in_dim(values, 0, 1, axis=axis_pos))
    return jnp.concatenate([remainder, filler], axis=axis_pos)


def behind(values, axis_pos):
    length = values.shape[axis_pos]
    remainder = lax.slice_in_dim(values, 0, length - 1, axis=axis_pos)
    filler = jnp.zeros_like(lax.slice_in_dim(values, 0, 1, axis=axis_pos))
    return jnp.concatenate([filler, remainder], axis=axis_pos)


def edge_layer(hidden_nodes, edges, counts, fluid, weight_in, weight_out, bias_in, spatial, count_dims):
    channels = hidden_nodes.shape[0]
    shape = hidden_nodes.shape
    flat = hidden_nodes.reshape(channels, -1)
    stacked = jnp.concatenate([weight_in[:, :channels], weight_in[:, channels:2 * channels]], axis=0)
    projected = jnp.dot(stacked, flat, preferred_element_type=jnp.float32)
    own_part = projected[:channels].reshape(shape)
    other_part = projected[channels:].reshape(shape)
    bias = bias_in.astype(jnp.float32).reshape((channels,) + (1,) * (hidden_nodes.ndim - 1))
    incoming = jnp.zeros(shape, jnp.float32)
    updated = []
    for direction in range(3):
        edge_now = edges[direction]
        edge_term = jnp.dot(weight_in[:, 2 * channels:], edge_now.reshape(channels, -1), preferred_element_type=jnp.float32).reshape(shape)
        preact = own_part + ahead(other_part, spatial[direction]) + edge_term + bias
        edge_hidden = jax.nn.silu(preact).astype(jnp.bfloat16)
        message = jnp.dot(weight_out, edge_hidden.reshape(channels, -1), preferred_element_type=jnp.float32).reshape(shape)
        updated.append((edge_now + message).astype(jnp.bfloat16))
        shared_count = jnp.minimum(counts, ahead(counts, count_dims[direction]))
        weight_edge = jnp.where(fluid & (shared_count > 0), 1.0 / jnp.maximum(shared_count, 1).astype(jnp.float32), 0.0).astype(jnp.float32)
        weighted = weight_edge[None] * message
        incoming = incoming + weighted + behind(weighted, spatial[direction])
    return incoming, jnp.stack(updated)


def node_layer(hidden_nodes, incoming_rounded, weight_in, weight_out, bias_in):
    channels = hidden_nodes.shape[0]
    shape = hidden_nodes.shape
    node_pre = jnp.dot(weight_in[:, :channels], hidden_nodes.reshape(channels, -1), preferred_element_type=jnp.float32)
    node_pre = node_pre + jnp.dot(weight_in[:, channels:], incoming_rounded.reshape(channels, -1), preferred_element_type=jnp.float32)
    node_pre = node_pre + bias_in.astype(jnp.float32)[:, None]
    node_hidden = jax.nn.silu(node_pre).astype(jnp.bfloat16)
    result = jnp.dot(weight_out, node_hidden, preferred_element_type=jnp.float32).reshape(shape)
    return (hidden_nodes + result).astype(jnp.bfloat16)


def copy_sums(values, block_axis, local_axis):
    width = values.shape[local_axis]
    head_part = lax.index_in_dim(values, 0, local_axis, keepdims=False)
    tail_part = lax.index_in_dim(values, width - 1, local_axis, keepdims=False)
    front = (slice(None),) * local_axis
    return values.at[front + (0,)].add(behind(tail_part, block_axis)).at[front + (width - 1,)].add(ahead(head_part, block_axis))


def reference(features, edge_state, multiplicity, edge_in, edge_out, edge_bias, node_in, node_out, node_bias):
    blocks_x, blocks_y, blocks_z = NX // CX, NY // CY, NZ // CZ

    def to_slabs(values):
        lead = values.ndim - 3
        shaped = values.reshape(values.shape[:lead] + (blocks_x, CX, blocks_y, CY, blocks_z, CZ))
        return jnp.moveaxis(shaped, lead, 0)

    counts = to_slabs(multiplicity)
    fluid = (counts[:, 1, :, 1, :, 1] > 0).reshape(blocks_x, 1, blocks_y, 1, blocks_z, 1)
    hidden_nodes = to_slabs(features)
    edges = to_slabs(edge_state)
    for layer_index in range(LAYERS):
        def per_slab(items):
            return edge_layer(items[0], items[1], items[2], items[3], edge_in[layer_index], edge_out[layer_index], edge_bias[layer_index], (1, 3, 5), (0, 2, 4))

        incoming, edges = lax.map(per_slab, (hidden_nodes, edges, counts, fluid))
        incoming = copy_sums(copy_sums(copy_sums(incoming, 0, 2), 3, 4), 5, 6)
        incoming_rounded = incoming.astype(jnp.bfloat16)

        def per_node_slab(items):
            return node_layer(items[0], items[1], node_in[layer_index], node_out[layer_index], node_bias[layer_index])

        hidden_nodes = lax.map(per_node_slab, (hidden_nodes, incoming_rounded))
    result = jnp.moveaxis(hidden_nodes, 0, 1)
    return result.reshape(result.shape[0], NX, NY, NZ)
```

```python
import functools

import jax
import jax.numpy as jnp
from jax import lax
from jax.experimental import pallas as pl
from jax.experimental.pallas import tpu as pltpu
from jax.sharding import PartitionSpec as P

F32 = jnp.float32
BF16 = jnp.bfloat16
LANES = 128


def swap_pairs(count, offset):
    pairs = []
    for i in range(offset, count, 2):
        j = (i + 1) % count
        pairs += [(i, j), (j, i)]
    return pairs


def exchange(values, axis):
    count = lax.axis_size(axis)
    even, odd = values
    got_odd = lax.ppermute(odd, axis, swap_pairs(count, 1))
    got_even = lax.ppermute(even, axis, swap_pairs(count, 0))
    return got_even, got_odd


def silu(v):
    return v / (1.0 + jnp.exp(-v))


def column(row):
    width = row.shape[1]
    eye = lax.broadcasted_iota(jnp.int32, (width, width), 0) == lax.broadcasted_iota(
        jnp.int32, (width, width), 1
    )
    return jnp.sum(jnp.where(eye, row, 0.0), axis=1, keepdims=True)


def tile(values, k):
    return values[:, k * LANES : (k + 1) * LANES]


def place(position, count, got_even, got_odd):
    is_even = position % 2 == 0
    low = jnp.where(is_even, got_odd, got_even)
    high = jnp.where(is_even, got_even, got_odd)
    low = jnp.where(position > 0, low, 0.0)
    high = jnp.where(position < count - 1, high, 0.0)
    return low, high


def edge_stage(sizes, layer, last, h_ref, e_in, e_out, w_ref, win, wout, bias, p_ref, sxe, sxo, pos):
    nx, ny = sizes
    lane = lax.broadcasted_iota(jnp.int32, (32, LANES), 1)
    span = ny * LANES
    w_in, w_out = win[layer], wout[layer]
    b = column(bias[layer : layer + 1, :])
    zero_tile = jnp.zeros((32, LANES), BF16)
    prev_x = None
    for x in range(nx):
        cur = h_ref[:, x * span : (x + 1) * span]
        ahead_x = h_ref[:, (x + 1) * span : (x + 2) * span] if x + 1 < nx else jnp.zeros_like(cur)
        ahead_y = jnp.concatenate([cur[:, LANES:], zero_tile], axis=1)
        ahead_z = jnp.concatenate(
            [
                jnp.where(
                    lane < LANES - 1, pltpu.roll(tile(cur, y).astype(F32), LANES - 1, 1), 0.0
                ).astype(BF16)
                for y in range(ny)
            ],
            axis=1,
        )
        weighted = []
        for d, shifted in enumerate((ahead_x, ahead_y, ahead_z)):
            edge = e_in[d, :, x * span : (x + 1) * span]
            pre = jnp.dot(
                w_in, jnp.concatenate([cur, shifted, edge], axis=0), preferred_element_type=F32
            )
            hid = silu(pre + b).astype(BF16)
            msg = jnp.dot(w_out, hid, preferred_element_type=F32)
            if not last:
                e_out[d, :, x * span : (x + 1) * span] = (edge.astype(F32) + msg).astype(BF16)
            weighted.append(
                [tile(msg, y) * w_ref[d, x * ny + y : x * ny + y + 1, :] for y in range(ny)]
            )
        wx, wy, wz = weighted
        for y in range(ny):
            acc = wx[y] + wy[y] + wz[y] + pltpu.roll(wz[y], 1, 1)
            if y > 0:
                acc = acc + wy[y - 1]
            if x > 0:
                acc = acc + prev_x[y]
            p_ref[:, (x * ny + y) * LANES : (x * ny + y + 1) * LANES] = acc
        prev_x = wx
    low = slice(0, span)
    high = slice((nx - 1) * span, nx * span)

    @pl.when(pos % 2 == 0)
    def _():
        sxe[...] = p_ref[:, high]
        sxo[...] = p_ref[:, low]

    @pl.when(pos % 2 == 1)
    def _():
        sxe[...] = p_ref[:, low]
        sxo[...] = p_ref[:, high]


def first_kernel(
    sizes, f_ref, es_ref, m_ref, win, wout, bias, h_ref, e_ref, w_ref, p_ref, sxe, sxo, e0, buf
):
    nx, ny = sizes
    rows = nx * ny

    def unpack(source, dest):
        buf[...] = source.astype(F32).reshape(buf.shape)
        for r in range(rows):
            dest[..., r * LANES : (r + 1) * LANES] = buf[pl.ds(r, 32, stride=rows), :].astype(BF16)

    unpack(f_ref[...], h_ref)
    for d in range(3):
        unpack(es_ref[d], e0.at[d])
    counts = m_ref[...]
    fluid = counts[1, 1:2, 1:2] > 0
    lane = lax.broadcasted_iota(jnp.int32, (ny, LANES), 1)
    sub = lax.broadcasted_iota(jnp.int32, (ny, LANES), 0)
    for x in range(nx):
        here = counts[x]
        for d in range(3):
            if d == 0:
                there = counts[x + 1] if x + 1 < nx else jnp.zeros_like(here)
            elif d == 1:
                there = jnp.where(sub < ny - 1, pltpu.roll(here, ny - 1, 0), 0)
            else:
                there = jnp.where(lane < LANES - 1, pltpu.roll(here, LANES - 1, 1), 0)
            shared = jnp.minimum(here, there)
            share = 1.0 / jnp.maximum(shared, 1).astype(F32)
            w_ref[d, x * ny : (x + 1) * ny, :] = jnp.where(fluid & (shared > 0), share, 0.0)
    edge_stage(
        sizes, 0, False, h_ref, e0, e_ref, w_ref, win, wout, bias, p_ref, sxe, sxo, lax.axis_index("gx")
    )


def y_faces(sizes, xcount, ycount, p_ref, rxe, rxo, sye, syo):
    nx, ny = sizes
    low_x, high_x = place(lax.axis_index("gx"), xcount, rxe[...], rxo[...])
    faces = []
    for y in (0, ny - 1):
        pieces = []
        for x in range(nx):
            t = p_ref[:, (x * ny + y) * LANES : (x * ny + y + 1) * LANES]
            if x == 0:
                t = t + tile(low_x, y)
            if x == nx - 1:
                t = t + tile(high_x, y)
            pieces.append(t)
        faces.append(jnp.concatenate(pieces, axis=1))
    low, high = faces
    is_even = lax.axis_index("gy") % 2 == 0
    sye[...] = jnp.where(is_even, high, low)
    syo[...] = jnp.where(is_even, low, high)


def folded_tile(sizes, p_ref, low_x, high_x, low_y, high_y, x, y):
    nx, ny = sizes
    t = p_ref[:, (x * ny + y) * LANES : (x * ny + y + 1) * LANES]
    if x == 0:
        t = t + tile(low_x, y)
    if x == nx - 1:
        t = t + tile(high_x, y)
    if y == 0:
        t = t + tile(low_y, x)
    if y == ny - 1:
        t = t + tile(high_y, x)
    return t


def z_faces(sizes, xcount, ycount, p_ref, rxe, rxo, rye, ryo, sz):
    nx, ny = sizes
    low_x, high_x = place(lax.axis_index("gx"), xcount, rxe[...], rxo[...])
    low_y, high_y = place(lax.axis_index("gy"), ycount, rye[...], ryo[...])
    lane = lax.broadcasted_iota(jnp.int32, (32, LANES), 1)
    acc = jnp.zeros((32, LANES), F32)
    for x in range(nx):
        for y in range(ny):
            k = x * ny + y
            t = folded_tile(sizes, p_ref, low_x, high_x, low_y, high_y, x, y)
            mine = (lane == 2 * k) | (lane == (2 * k - 1) % LANES)
            acc = jnp.where(mine, pltpu.roll(t, 2 * k, 1) if k else t, acc)
    sz[...] = acc


def node_stage(
    sizes, counts, layer, h_in, p_ref, rxe, rxo, rye, ryo, rze, rzo, nin, nout, nbias, write
):
    nx, ny = sizes
    xcount, ycount, zcount = counts
    low_x, high_x = place(lax.axis_index("gx"), xcount, rxe[...], rxo[...])
    low_y, high_y = place(lax.axis_index("gy"), ycount, rye[...], ryo[...])
    low_z, high_z = place(lax.axis_index("gz"), zcount, rze[...], rzo[...])
    lane = lax.broadcasted_iota(jnp.int32, (32, LANES), 1)
    joined = jnp.where(lane % 2 == 0, pltpu.roll(low_z, 1, 1), pltpu.roll(high_z, LANES - 1, 1))
    w_in, w_out = nin[layer], nout[layer]
    b = column(nbias[layer : layer + 1, :])
    ends = (lane == 0) | (lane == LANES - 1)
    for x in range(nx):
        pieces = []
        for y in range(ny):
            k = x * ny + y
            t = folded_tile(sizes, p_ref, low_x, high_x, low_y, high_y, x, y)
            back = pltpu.roll(joined, LANES - 2 * k, 1) if k else joined
            pieces.append((t + jnp.where(ends, back, 0.0)).astype(BF16))
        span = slice(x * ny * LANES, (x + 1) * ny * LANES)
        cur = h_in[:, span]
        stacked = jnp.concatenate([cur, jnp.concatenate(pieces, axis=1)], axis=0)
        hid = silu(jnp.dot(w_in, stacked, preferred_element_type=F32) + b).astype(BF16)
        res = jnp.dot(w_out, hid, preferred_element_type=F32)
        write(x, cur.astype(F32) + res)


def middle_kernel(
    sizes, counts, layer, last, h_in, e_in, w_ref, p_in, rxe, rxo, rye, ryo, rze, rzo,
    nin, nout, nbias, win, wout, bias, *outs,
):
    nx, ny = sizes
    if last:
        h_out, p_ref, sxe, sxo = outs
        e_out = None
    else:
        h_out, e_out, p_ref, sxe, sxo = outs

    def write(x, value):
        h_out[:, x * ny * LANES : (x + 1) * ny * LANES] = value.astype(BF16)

    node_stage(
        sizes, counts, layer, h_in, p_in, rxe, rxo, rye, ryo, rze, rzo, nin, nout, nbias, write
    )
    edge_stage(
        sizes, layer + 1, last, h_out, e_in, e_out, w_ref, win, wout, bias, p_ref, sxe, sxo,
        lax.axis_index("gx"),
    )


def last_kernel(
    sizes, counts, layer, h_in, p_in, rxe, rxo, rye, ryo, rze, rzo, nin, nout, nbias, out, buf
):
    nx, ny = sizes
    rows = nx * ny

    def write(x, value):
        for y in range(ny):
            buf[pl.ds(x * ny + y, 32, stride=rows), :] = tile(value, y)

    node_stage(
        sizes, counts, layer, h_in, p_in, rxe, rxo, rye, ryo, rze, rzo, nin, nout, nbias, write
    )
    out[...] = buf[...].reshape(out.shape).astype(BF16)


def call(body, args, outs, scratch=()):
    vmem = pl.BlockSpec(memory_space=pltpu.VMEM)
    return pl.pallas_call(
        body,
        out_shape=[jax.ShapeDtypeStruct(s, d) for s, d in outs],
        in_specs=[vmem] * len(args),
        out_specs=[vmem] * len(outs),
        scratch_shapes=list(scratch),
    )(*args)


def on_device(
    features, edge_state, multiplicity, edge_in, edge_out, edge_bias, node_in, node_out, node_bias
):
    ch, nx, ny, nz = features.shape
    layers = edge_in.shape[0]
    sizes = (nx, ny)
    counts = tuple(lax.axis_size(a) for a in ("gx", "gy", "gz"))
    rows = nx * ny
    nodes = rows * nz
    h_t = ((ch, nodes), BF16)
    e_t = ((3, ch, nodes), BF16)
    p_t = ((ch, nodes), F32)
    sx_t = ((ch, ny * nz), F32)
    sy_t = ((ch, nx * nz), F32)
    sz_t = ((ch, LANES), F32)
    h, e, w, p, sxe, sxo = call(
        functools.partial(first_kernel, sizes),
        (features, edge_state, multiplicity, edge_in, edge_out, edge_bias),
        (h_t, e_t, ((3, rows, nz), F32), p_t, sx_t, sx_t),
        (pltpu.VMEM((3, ch, nodes), BF16), pltpu.VMEM((ch * rows, nz), F32)),
    )
    for layer in range(layers):
        rxe, rxo = exchange((sxe, sxo), "gx")
        sye, syo = call(
            functools.partial(y_faces, sizes, counts[0], counts[1]), (p, rxe, rxo), (sy_t, sy_t)
        )
        rye, ryo = exchange((sye, syo), "gy")
        (sz,) = call(
            functools.partial(z_faces, sizes, counts[0], counts[1]),
            (p, rxe, rxo, rye, ryo),
            (sz_t,),
        )
        rze, rzo = exchange((sz, sz), "gz")
        got = (rxe, rxo, rye, ryo, rze, rzo)
        if layer + 1 < layers:
            last = layer + 2 == layers
            res = call(
                functools.partial(middle_kernel, sizes, counts, layer, last),
                (h, e, w, p, *got, node_in, node_out, node_bias, edge_in, edge_out, edge_bias),
                (h_t, p_t, sx_t, sx_t) if last else (h_t, e_t, p_t, sx_t, sx_t),
            )
            if last:
                h, p, sxe, sxo = res
            else:
                h, e, p, sxe, sxo = res
        else:
            (out,) = call(
                functools.partial(last_kernel, sizes, counts, layer),
                (h, p, *got, node_in, node_out, node_bias),
                ((features.shape, BF16),),
                (pltpu.VMEM((ch * rows, nz), F32),),
            )
    return out


def solution(mesh):
    placed = (
        P(None, "gx", "gy", "gz"),
        P(None, None, "gx", "gy", "gz"),
        P("gx", "gy", "gz"),
        P(),
        P(),
        P(),
        P(),
        P(),
        P(),
    )
    return jax.shard_map(
        on_device, mesh=mesh, in_specs=placed, out_specs=P(None, "gx", "gy", "gz"), check_vma=False
    )
```

```python
import functools

import jax
import jax.numpy as jnp
from jax import lax
from jax.experimental import pallas as pl
from jax.experimental.pallas import tpu as pltpu
from jax.sharding import PartitionSpec as P

F32 = jnp.float32
BF16 = jnp.bfloat16
LANES = 128


def swap_pairs(count, offset):
    pairs = []
    for i in range(offset, count, 2):
        j = (i + 1) % count
        pairs += [(i, j), (j, i)]
    return pairs


def exchange(values, axis):
    count = lax.axis_size(axis)
    even, odd = values
    got_odd = lax.ppermute(odd, axis, swap_pairs(count, 1))
    got_even = lax.ppermute(even, axis, swap_pairs(count, 0))
    return got_even, got_odd


def silu(v):
    return v / (1.0 + jnp.exp(-v))


def column(row):
    width = row.shape[1]
    eye = lax.broadcasted_iota(jnp.int32, (width, width), 0) == lax.broadcasted_iota(
        jnp.int32, (width, width), 1
    )
    return jnp.sum(jnp.where(eye, row, 0.0), axis=1, keepdims=True)


def tile(values, k):
    return values[:, k * LANES : (k + 1) * LANES]


def place(position, count, got_even, got_odd):
    is_even = position % 2 == 0
    low = jnp.where(is_even, got_odd, got_even)
    high = jnp.where(is_even, got_even, got_odd)
    low = jnp.where(position > 0, low, 0.0)
    high = jnp.where(position < count - 1, high, 0.0)
    return low, high


def edge_stage(sizes, layer, last, h_ref, e_in, e_out, w_ref, win, wout, bias, p_ref, sxe, sxo, pos):
    nx, ny = sizes
    lane = lax.broadcasted_iota(jnp.int32, (32, LANES), 1)
    span = ny * LANES
    w_in, w_out = win[layer], wout[layer]
    b = column(bias[layer : layer + 1, :])
    zero_tile = jnp.zeros((32, LANES), BF16)
    prev_x = None
    for x in range(nx):
        cur = h_ref[:, x * span : (x + 1) * span]
        ahead_x = h_ref[:, (x + 1) * span : (x + 2) * span] if x + 1 < nx else jnp.zeros_like(cur)
        ahead_y = jnp.concatenate([cur[:, LANES:], zero_tile], axis=1)
        ahead_z = jnp.concatenate(
            [
                jnp.where(
                    lane < LANES - 1, pltpu.roll(tile(cur, y).astype(F32), LANES - 1, 1), 0.0
                ).astype(BF16)
                for y in range(ny)
            ],
            axis=1,
        )
        weighted = []
        for d, shifted in enumerate((ahead_x, ahead_y, ahead_z)):
            edge = e_in[d, :, x * span : (x + 1) * span]
            pre = jnp.dot(
                w_in, jnp.concatenate([cur, shifted, edge], axis=0), preferred_element_type=F32
            )
            hid = silu(pre + b).astype(BF16)
            msg = jnp.dot(w_out, hid, preferred_element_type=F32)
            if not last:
                e_out[d, :, x * span : (x + 1) * span] = (edge.astype(F32) + msg).astype(BF16)
            weighted.append(
                [tile(msg, y) * w_ref[d, x * ny + y : x * ny + y + 1, :] for y in range(ny)]
            )
        wx, wy, wz = weighted
        for y in range(ny):
            acc = wx[y] + wy[y] + wz[y] + pltpu.roll(wz[y], 1, 1)
            if y > 0:
                acc = acc + wy[y - 1]
            if x > 0:
                acc = acc + prev_x[y]
            p_ref[:, (x * ny + y) * LANES : (x * ny + y + 1) * LANES] = acc
        prev_x = wx
    low = slice(0, span)
    high = slice((nx - 1) * span, nx * span)

    @pl.when(pos % 2 == 0)
    def _():
        sxe[...] = p_ref[:, high]
        sxo[...] = p_ref[:, low]

    @pl.when(pos % 2 == 1)
    def _():
        sxe[...] = p_ref[:, low]
        sxo[...] = p_ref[:, high]


def first_kernel(
    sizes, f_ref, es_ref, m_ref, win, wout, bias, h_ref, e_ref, w_ref, p_ref, sxe, sxo, e0, buf
):
    nx, ny = sizes
    rows = nx * ny

    def unpack(source, dest):
        buf[...] = source.astype(F32).reshape(buf.shape)
        for r in range(rows):
            dest[..., r * LANES : (r + 1) * LANES] = buf[pl.ds(r, 32, stride=rows), :].astype(BF16)

    unpack(f_ref[...], h_ref)
    for d in range(3):
        unpack(es_ref[d], e0.at[d])
    counts = m_ref[...]
    fluid = counts[1, 1:2, 1:2] > 0
    lane = lax.broadcasted_iota(jnp.int32, (ny, LANES), 1)
    sub = lax.broadcasted_iota(jnp.int32, (ny, LANES), 0)
    for x in range(nx):
        here = counts[x]
        for d in range(3):
            if d == 0:
                there = counts[x + 1] if x + 1 < nx else jnp.zeros_like(here)
            elif d == 1:
                there = jnp.where(sub < ny - 1, pltpu.roll(here, ny - 1, 0), 0)
            else:
                there = jnp.where(lane < LANES - 1, pltpu.roll(here, LANES - 1, 1), 0)
            shared = jnp.minimum(here, there)
            share = 1.0 / jnp.maximum(shared, 1).astype(F32)
            w_ref[d, x * ny : (x + 1) * ny, :] = jnp.where(fluid & (shared > 0), share, 0.0)
    edge_stage(
        sizes, 0, False, h_ref, e0, e_ref, w_ref, win, wout, bias, p_ref, sxe, sxo, lax.axis_index("gx")
    )


def y_faces(sizes, xcount, ycount, p_ref, rxe, rxo, sye, syo):
    nx, ny = sizes
    low_x, high_x = place(lax.axis_index("gx"), xcount, rxe[...], rxo[...])
    faces = []
    for y in (0, ny - 1):
        pieces = []
        for x in range(nx):
            t = p_ref[:, (x * ny + y) * LANES : (x * ny + y + 1) * LANES]
            if x == 0:
                t = t + tile(low_x, y)
            if x == nx - 1:
                t = t + tile(high_x, y)
            pieces.append(t)
        faces.append(jnp.concatenate(pieces, axis=1))
    low, high = faces
    is_even = lax.axis_index("gy") % 2 == 0
    sye[...] = jnp.where(is_even, high, low)
    syo[...] = jnp.where(is_even, low, high)


def folded_tile(sizes, p_ref, low_x, high_x, low_y, high_y, x, y):
    nx, ny = sizes
    t = p_ref[:, (x * ny + y) * LANES : (x * ny + y + 1) * LANES]
    if x == 0:
        t = t + tile(low_x, y)
    if x == nx - 1:
        t = t + tile(high_x, y)
    if y == 0:
        t = t + tile(low_y, x)
    if y == ny - 1:
        t = t + tile(high_y, x)
    return t


def z_faces(sizes, xcount, ycount, p_ref, rxe, rxo, rye, ryo, sz):
    nx, ny = sizes
    low_x, high_x = place(lax.axis_index("gx"), xcount, rxe[...], rxo[...])
    low_y, high_y = place(lax.axis_index("gy"), ycount, rye[...], ryo[...])
    lane = lax.broadcasted_iota(jnp.int32, (32, LANES), 1)
    acc = jnp.zeros((32, LANES), F32)
    for x in range(nx):
        for y in range(ny):
            k = x * ny + y
            t = folded_tile(sizes, p_ref, low_x, high_x, low_y, high_y, x, y)
            mine = (lane == 2 * k) | (lane == (2 * k - 1) % LANES)
            acc = jnp.where(mine, pltpu.roll(t, 2 * k, 1) if k else t, acc)
    sz[...] = acc


def node_stage(
    sizes, counts, layer, h_in, p_ref, rxe, rxo, rye, ryo, rze, rzo, nin, nout, nbias, write
):
    nx, ny = sizes
    xcount, ycount, zcount = counts
    low_x, high_x = place(lax.axis_index("gx"), xcount, rxe[...], rxo[...])
    low_y, high_y = place(lax.axis_index("gy"), ycount, rye[...], ryo[...])
    low_z, high_z = place(lax.axis_index("gz"), zcount, rze[...], rzo[...])
    lane = lax.broadcasted_iota(jnp.int32, (32, LANES), 1)
    joined = jnp.where(lane % 2 == 0, pltpu.roll(low_z, 1, 1), pltpu.roll(high_z, LANES - 1, 1))
    w_in, w_out = nin[layer], nout[layer]
    b = column(nbias[layer : layer + 1, :])
    ends = (lane == 0) | (lane == LANES - 1)
    for x in range(nx):
        pieces = []
        for y in range(ny):
            k = x * ny + y
            t = folded_tile(sizes, p_ref, low_x, high_x, low_y, high_y, x, y)
            back = pltpu.roll(joined, LANES - 2 * k, 1) if k else joined
            pieces.append((t + jnp.where(ends, back, 0.0)).astype(BF16))
        span = slice(x * ny * LANES, (x + 1) * ny * LANES)
        cur = h_in[:, span]
        stacked = jnp.concatenate([cur, jnp.concatenate(pieces, axis=1)], axis=0)
        hid = silu(jnp.dot(w_in, stacked, preferred_element_type=F32) + b).astype(BF16)
        res = jnp.dot(w_out, hid, preferred_element_type=F32)
        write(x, cur.astype(F32) + res)


def middle_kernel(
    sizes, counts, layer, last, h_in, e_in, w_ref, p_in, rxe, rxo, rye, ryo, rze, rzo,
    nin, nout, nbias, win, wout, bias, *outs,
):
    nx, ny = sizes
    if last:
        h_out, p_ref, sxe, sxo = outs
        e_out = None
    else:
        h_out, e_out, p_ref, sxe, sxo = outs

    def write(x, value):
        h_out[:, x * ny * LANES : (x + 1) * ny * LANES] = value.astype(BF16)

    node_stage(
        sizes, counts, layer, h_in, p_in, rxe, rxo, rye, ryo, rze, rzo, nin, nout, nbias, write
    )
    edge_stage(
        sizes, layer + 1, last, h_out, e_in, e_out, w_ref, win, wout, bias, p_ref, sxe, sxo,
        lax.axis_index("gx"),
    )


def last_kernel(
    sizes, counts, layer, h_in, p_in, rxe, rxo, rye, ryo, rze, rzo, nin, nout, nbias, out, buf
):
    nx, ny = sizes
    rows = nx * ny

    def write(x, value):
        for y in range(ny):
            buf[pl.ds(x * ny + y, 32, stride=rows), :] = tile(value, y)

    node_stage(
        sizes, counts, layer, h_in, p_in, rxe, rxo, rye, ryo, rze, rzo, nin, nout, nbias, write
    )
    out[...] = buf[...].reshape(out.shape).astype(BF16)


def call(body, args, outs, scratch=(), first=False, last=False):
    vmem = pl.BlockSpec(memory_space=pltpu.VMEM)
    if not first:
        args = [pltpu.with_memory_space_constraint(a, pltpu.VMEM) for a in args]
    return pl.pallas_call(
        body,
        out_shape=[jax.ShapeDtypeStruct(s, d) if last else pltpu.VMEM(s, d) for s, d in outs],
        in_specs=[vmem] * len(args),
        out_specs=[vmem] * len(outs),
        scratch_shapes=list(scratch),
    )(*args)


def on_device(
    features, edge_state, multiplicity, edge_in, edge_out, edge_bias, node_in, node_out, node_bias
):
    ch, nx, ny, nz = features.shape
    layers = edge_in.shape[0]
    sizes = (nx, ny)
    counts = tuple(lax.axis_size(a) for a in ("gx", "gy", "gz"))
    rows = nx * ny
    nodes = rows * nz
    h_t = ((ch, nodes), BF16)
    e_t = ((3, ch, nodes), BF16)
    p_t = ((ch, nodes), F32)
    sx_t = ((ch, ny * nz), F32)
    sy_t = ((ch, nx * nz), F32)
    sz_t = ((ch, LANES), F32)
    h, e, w, p, sxe, sxo = call(
        functools.partial(first_kernel, sizes),
        (features, edge_state, multiplicity, edge_in, edge_out, edge_bias),
        (h_t, e_t, ((3, rows, nz), F32), p_t, sx_t, sx_t),
        (pltpu.VMEM((3, ch, nodes), BF16), pltpu.VMEM((ch * rows, nz), F32)),
        first=True,
    )
    for layer in range(layers):
        rxe, rxo = exchange((sxe, sxo), "gx")
        sye, syo = call(
            functools.partial(y_faces, sizes, counts[0], counts[1]), (p, rxe, rxo), (sy_t, sy_t)
        )
        rye, ryo = exchange((sye, syo), "gy")
        (sz,) = call(
            functools.partial(z_faces, sizes, counts[0], counts[1]),
            (p, rxe, rxo, rye, ryo),
            (sz_t,),
        )
        rze, rzo = exchange((sz, sz), "gz")
        got = (rxe, rxo, rye, ryo, rze, rzo)
        if layer + 1 < layers:
            last = layer + 2 == layers
            res = call(
                functools.partial(middle_kernel, sizes, counts, layer, last),
                (h, e, w, p, *got, node_in, node_out, node_bias, edge_in, edge_out, edge_bias),
                (h_t, p_t, sx_t, sx_t) if last else (h_t, e_t, p_t, sx_t, sx_t),
            )
            if last:
                h, p, sxe, sxo = res
            else:
                h, e, p, sxe, sxo = res
        else:
            (out,) = call(
                functools.partial(last_kernel, sizes, counts, layer),
                (h, p, *got, node_in, node_out, node_bias),
                ((features.shape, BF16),),
                (pltpu.VMEM((ch * rows, nz), F32),),
                last=True,
            )
    return out


def solution(mesh):
    placed = (
        P(None, "gx", "gy", "gz"),
        P(None, None, "gx", "gy", "gz"),
        P("gx", "gy", "gz"),
        P(),
        P(),
        P(),
        P(),
        P(),
        P(),
    )
    return jax.shard_map(
        on_device, mesh=mesh, in_specs=placed, out_specs=P(None, "gx", "gy", "gz"), check_vma=False
    )
```

```python
import functools

import jax
import jax.numpy as jnp
from jax import lax
from jax.experimental import pallas as pl
from jax.experimental.pallas import tpu as pltpu
from jax.sharding import PartitionSpec as P

F32 = jnp.float32
BF16 = jnp.bfloat16
LANES = 128
AXES = ("gx", "gy", "gz")


def even_pairs(count):
    return [(i, i ^ 1) for i in range(count)]


def odd_pairs(axis, spare):
    sizes = [lax.axis_size(a) for a in AXES]
    at, other = AXES.index(axis), AXES.index(spare)
    pairs = []
    for i in range(sizes[0]):
        for j in range(sizes[1]):
            for k in range(sizes[2]):
                here = [i, j, k]
                there = list(here)
                if 0 < here[at] < sizes[at] - 1:
                    there[at] = ((here[at] + 1) ^ 1) - 1
                else:
                    there[other] = here[other] ^ 1
                flat = [(v[0] * sizes[1] + v[1]) * sizes[2] + v[2] for v in (here, there)]
                pairs.append(tuple(flat))
    return pairs


def exchange(even, odd, axis, spare):
    got_even = lax.ppermute(even, axis, even_pairs(lax.axis_size(axis)))
    got_odd = lax.ppermute(odd, AXES, odd_pairs(axis, spare))
    return got_even, got_odd


def silu(v):
    return v / (1.0 + jnp.exp(-v))


def column(row):
    width = row.shape[1]
    eye = lax.broadcasted_iota(jnp.int32, (width, width), 0) == lax.broadcasted_iota(
        jnp.int32, (width, width), 1
    )
    return jnp.sum(jnp.where(eye, row, 0.0), axis=1, keepdims=True)


def tile(values, k):
    return values[:, k * LANES : (k + 1) * LANES]


def turn(values, shift):
    shift %= LANES
    return pltpu.roll(values, shift, 1) if shift else values


def place(axis, got_even, got_odd):
    position, count = lax.axis_index(axis), lax.axis_size(axis)
    is_even = position % 2 == 0
    low = jnp.where(is_even, got_odd, got_even)
    high = jnp.where(is_even, got_even, got_odd)
    low = jnp.where(position > 0, low, 0.0)
    high = jnp.where(position < count - 1, high, 0.0)
    return low, high


def lanes_of(rows=32):
    return lax.broadcasted_iota(jnp.int32, (rows, LANES), 1)


def perceptron(w_in, bias, w_out, pieces):
    stacked = jnp.concatenate([p.astype(BF16) for p in pieces], axis=0)
    pre = jnp.dot(w_in, stacked, preferred_element_type=F32) + bias
    return jnp.dot(w_out, silu(pre).astype(BF16), preferred_element_type=F32)


def rim_edges(sizes, h, e, w, w_in, w_out, bias):
    nx, ny = sizes
    lane = lanes_of()
    at, y_at = lane % 4, (lane // 4) % ny
    x_step = 4 * ny
    outer = len(h) == 5
    a, b, d, t = h[:4]
    o = h[4] if outer else jnp.zeros_like(a)
    ahead_z = [
        jnp.where(at < 3, turn(a, -1), 0.0),
        jnp.where(at < 3, turn(b, -1), d),
        jnp.where(at < 2, turn(d, -1), jnp.where(at == 2, o, turn(o, 2))),
        jnp.where(at == 0, a, jnp.where(at < 3, turn(t, -1), 0.0)),
    ]
    if outer:
        ahead_z.append(jnp.where(at == 0, t, jnp.where(at == 3, turn(t, 2), 0.0)))
    ahead_x = [jnp.where(lane < x_step * (nx - 1), turn(v, -x_step), 0.0) for v in h]
    ahead_y = [jnp.where(y_at < ny - 1, turn(v, -4), 0.0) for v in h]
    cur = jnp.concatenate(h, axis=1)
    updated, weighted = [], []
    for k, shifted in enumerate((ahead_x, ahead_y, ahead_z)):
        edge = jnp.concatenate(e[k], axis=1)
        msg = perceptron(w_in, bias, w_out, [cur, jnp.concatenate(shifted, axis=1), edge])
        updated.append(edge + msg)
        weighted.append([tile(msg, i) * w[i][k : k + 1, :] for i in range(len(h))])
    wx, wy, wz = weighted
    wo = wz[4] if outer else jnp.zeros_like(a)
    behind = [
        jnp.where(at == 0, wz[3], turn(wz[0], 1)),
        jnp.where(at == 0, 0.0, turn(wz[1], 1)),
        jnp.where(at == 3, wz[1], jnp.where(at == 0, 0.0, turn(wz[2], 1))),
        jnp.where(at == 0, wo, jnp.where(at == 1, turn(wo, -2), turn(wz[3], 1))),
    ]
    sums = [
        wx[i] + wy[i] + wz[i] + turn(wx[i], x_step) + turn(wy[i], 4) + behind[i] for i in range(4)
    ]
    return updated, sums


def quarters(lane, parts):
    q = lane // 32
    return jnp.where(
        q == 0, parts[0], jnp.where(q == 1, parts[1], jnp.where(q == 2, parts[2], parts[3]))
    )


def rim_x_faces(sums):
    lane = lanes_of()
    low = quarters(lane, [turn(v, 32 * i) for i, v in enumerate(sums)])
    high = quarters(lane, [turn(v, 32 * i - 64) for i, v in enumerate(sums)])
    return low, high


def rim_add_x(sums, low, high):
    q = lanes_of() // 32
    return [
        v
        + jnp.where(q == 0, turn(low, -32 * i), 0.0)
        + jnp.where(q == 2, turn(high, 64 - 32 * i), 0.0)
        for i, v in enumerate(sums)
    ]


def rim_y_faces(sums):
    group = (lanes_of() // 4) % 8
    packed = jnp.zeros_like(sums[0])
    for i, v in enumerate(sums):
        packed = jnp.where(group == i, turn(v, 4 * i), packed)
        packed = jnp.where(group == 4 + i, turn(v, 4 * i - 12), packed)
    return packed


def rim_add_y(sums, low, high):
    group = (lanes_of() // 4) % 8
    return [
        v
        + jnp.where(group == 0, turn(low, -16 - 4 * i), 0.0)
        + jnp.where(group == 7, turn(high, 28 - 4 * i), 0.0)
        for i, v in enumerate(sums)
    ]


def rim_join_z(sums):
    a, b, d, t = sums
    at = lanes_of() % 4
    return [
        a + jnp.where(at == 3, turn(d, 3), 0.0),
        b + jnp.where(at == 0, turn(t, -3), 0.0),
        d + jnp.where(at == 0, turn(a, -3), 0.0),
        t + jnp.where(at == 3, turn(b, 3), 0.0),
    ]


def edge_stage(sizes, last, h_ref, slab_of, w_ref, w_in, w_out, bias, p_ref, done):
    nx, ny = sizes
    lane = lanes_of()
    span = ny * LANES
    zero_tile = jnp.zeros((32, LANES), BF16)
    prev_x = None
    for x in range(nx):
        cur = h_ref[:, x * span : (x + 1) * span]
        ahead_x = h_ref[:, (x + 1) * span : (x + 2) * span] if x + 1 < nx else jnp.zeros_like(cur)
        ahead_y = jnp.concatenate([cur[:, LANES:], zero_tile], axis=1)
        ahead_z = jnp.concatenate(
            [
                jnp.where(lane < LANES - 1, turn(tile(cur, y).astype(F32), -1), 0.0).astype(BF16)
                for y in range(ny)
            ],
            axis=1,
        )
        edges, edges_out = slab_of(x)
        weighted = []
        for d, shifted in enumerate((ahead_x, ahead_y, ahead_z)):
            edge = edges[d, :, x * span : (x + 1) * span]
            msg = perceptron(w_in, bias, w_out, [cur, shifted, edge])
            if not last:
                edges_out[d, :, x * span : (x + 1) * span] = (edge.astype(F32) + msg).astype(BF16)
            weighted.append([tile(msg, y) * w_ref[x * ny + y, d : d + 1, :] for y in range(ny)])
        wx, wy, wz = weighted
        for y in range(ny):
            acc = wx[y] + wy[y] + wz[y] + turn(wz[y], 1)
            if y > 0:
                acc = acc + wy[y - 1]
            if x > 0:
                acc = acc + prev_x[y]
            p_ref[:, (x * ny + y) * LANES : (x * ny + y + 1) * LANES] = acc
        prev_x = wx
        done(x)


def write_x_faces(sizes, p_ref, sums, sxe, sxo):
    nx, ny = sizes
    span = ny * LANES
    low_rim, high_rim = rim_x_faces(sums)
    is_even = lax.axis_index("gx") % 2 == 0
    sxe[:, span:] = jnp.where(is_even, high_rim, low_rim)
    sxo[:, span:] = jnp.where(is_even, low_rim, high_rim)
    low = slice(0, span)
    high = slice((nx - 1) * span, nx * span)

    @pl.when(is_even)
    def _():
        sxe[:, :span] = p_ref[:, high]
        sxo[:, :span] = p_ref[:, low]

    @pl.when(jnp.logical_not(is_even))
    def _():
        sxe[:, :span] = p_ref[:, low]
        sxo[:, :span] = p_ref[:, high]


def unpack_kernel(sizes, f_ref, es_ref, m_ref, h_ref, e_ref, w_ref, own_ref, sze, szo, buf):
    nx, ny = sizes
    rows = nx * ny
    counts = m_ref[...]
    fluid = counts[1, 1:2, 1:2] > 0
    lane = lax.broadcasted_iota(jnp.int32, (ny, LANES), 1)
    sub = lax.broadcasted_iota(jnp.int32, (ny, LANES), 0)
    for x in range(nx):
        here = counts[x]
        shares = []
        for d in range(3):
            if d == 0:
                there = counts[x + 1] if x + 1 < nx else jnp.zeros_like(here)
            elif d == 1:
                there = jnp.where(sub < ny - 1, pltpu.roll(here, ny - 1, 0), 0)
            else:
                there = jnp.where(lane < LANES - 1, pltpu.roll(here, LANES - 1, 1), 0)
            shared = jnp.minimum(here, there)
            share = 1.0 / jnp.maximum(shared, 1).astype(F32)
            shares.append(jnp.where(fluid & (shared > 0), share, 0.0))
        for y in range(ny):
            for d in range(3):
                w_ref[x * ny + y, d : d + 1, :] = shares[d][y : y + 1, :]
            w_ref[x * ny + y, 3:8, :] = jnp.zeros((5, LANES), F32)

    def collect(first, size, row_of):
        group = lanes_of(size) // 4
        found = [jnp.zeros((size, LANES), F32)] * 4
        for k in range(rows):
            turned = turn(row_of(k), 4 * k)
            for i, shift in enumerate((-1, 0, 1, -2)):
                found[i] = jnp.where(group == (k + shift) % 32, turned, found[i])
        for i, shift in enumerate((4, 0, -4, 8)):
            own_ref[i, first : first + size, :] = turn(found[i], shift)

    for field in range(4):
        source = f_ref[...] if field == 0 else es_ref[field - 1]
        buf[field] = source.astype(F32).reshape(buf.shape[1:])

        def row_of(k, field=field):
            t = buf[field, pl.ds(k, 32, stride=rows), :]
            if field == 0:
                h_ref[:, k * LANES : (k + 1) * LANES] = t.astype(BF16)
            else:
                e_ref[field - 1, :, k * LANES : (k + 1) * LANES] = t.astype(BF16)
            return t

        collect(32 * field, 32, row_of)
    collect(128, 8, lambda k: w_ref[k])
    is_even = lax.axis_index("gz") % 2 == 0
    sze[...] = jnp.where(is_even, own_ref[0], own_ref[1])
    szo[...] = jnp.where(is_even, own_ref[1], own_ref[0])


def first_edges(sizes, h_ref, e_ref, w_ref, win, wout, bias, e_out, p_ref, buf, sems):
    span = sizes[1] * LANES

    def copy_of(x):
        part = pl.ds(x * span, span)
        return pltpu.make_async_copy(buf.at[:, :, part], e_out.at[:, :, part], sems.at[x])

    edge_stage(
        sizes, False, h_ref, lambda x: (e_ref, buf), w_ref, win[0], wout[0], column(bias[0:1, :]),
        p_ref, lambda x: copy_of(x).start(),
    )
    for x in range(sizes[0]):
        copy_of(x).wait()


def first_rim(
    sizes, p_ref, own_ref, rze, rzo, win, wout, bias, hr_out, er_out, wr_out, pr_out, sxe, sxo
):
    at = lanes_of(own_ref.shape[1]) % 4
    own_a, own_b, upper, lower = (own_ref[i] for i in range(4))
    prev, nxt = place("gz", rze[...], rzo[...])
    tiles = [
        own_a,
        own_b,
        jnp.where(at == 3, turn(upper, 3), nxt),
        jnp.where(at == 0, turn(lower, -3), prev),
        jnp.where(
            at == 0,
            turn(lower, -2),
            jnp.where(at == 1, upper, jnp.where(at == 2, turn(nxt, -1), turn(prev, 3))),
        ),
    ]
    h = [t[0:32] for t in tiles]
    e = [[t[32 * (d + 1) : 32 * (d + 2)] for t in tiles] for d in range(3)]
    w = [t[128:136] for t in tiles]
    updated, sums = rim_edges(sizes, h, e, w, win[0], wout[0], column(bias[0:1, :]))
    for i in range(4):
        hr_out[:, i * LANES : (i + 1) * LANES] = h[i].astype(BF16)
        wr_out[:, i * LANES : (i + 1) * LANES] = w[i]
    for d in range(3):
        er_out[d] = updated[d][:, : 4 * LANES].astype(BF16)
    write_x_faces(sizes, p_ref, sums, sxe, sxo)
    for i in range(4):
        pr_out[:, i * LANES : (i + 1) * LANES] = sums[i]


def y_faces(sizes, p_ref, pr_ref, rxe, rxo, sye, syo, pr_out):
    nx, ny = sizes
    low_x, high_x = place("gx", rxe[...], rxo[...])
    faces = []
    for y in (0, ny - 1):
        pieces = []
        for x in range(nx):
            t = p_ref[:, (x * ny + y) * LANES : (x * ny + y + 1) * LANES]
            if x == 0:
                t = t + tile(low_x, y)
            if x == nx - 1:
                t = t + tile(high_x, y)
            pieces.append(t)
        faces.append(jnp.concatenate(pieces, axis=1))
    low, high = faces
    sums = rim_add_x([tile(pr_ref, i) for i in range(4)], tile(low_x, ny), tile(high_x, ny))
    packed = rim_y_faces(sums)
    for i in range(4):
        pr_out[:, i * LANES : (i + 1) * LANES] = sums[i]
    is_even = lax.axis_index("gy") % 2 == 0
    sye[:, : nx * LANES] = jnp.where(is_even, high, low)
    syo[:, : nx * LANES] = jnp.where(is_even, low, high)
    sye[:, nx * LANES :] = packed
    syo[:, nx * LANES :] = packed


def node_stage(
    sizes, layer, h_in, p_ref, hr_in, pr_ref, rxe, rxo, rye, ryo, nin, nout, nbias, write
):
    nx, ny = sizes
    low_x, high_x = place("gx", rxe[...], rxo[...])
    low_y, high_y = place("gy", rye[...], ryo[...])
    w_in, w_out = nin[layer], nout[layer]
    b = column(nbias[layer : layer + 1, :])
    sums = rim_add_y([tile(pr_ref, i) for i in range(4)], tile(low_y, nx), tile(high_y, nx))
    rim = rim_join_z(sums)
    cur = hr_in[...]
    rim_h = cur.astype(F32) + perceptron(w_in, b, w_out, [cur, jnp.concatenate(rim, axis=1)])
    for x in range(nx):
        pieces = []
        for y in range(ny):
            t = p_ref[:, (x * ny + y) * LANES : (x * ny + y + 1) * LANES]
            if x == 0:
                t = t + tile(low_x, y)
            if x == nx - 1:
                t = t + tile(high_x, y)
            if y == 0:
                t = t + tile(low_y, x)
            if y == ny - 1:
                t = t + tile(high_y, x)
            pieces.append(t.astype(BF16))
        span = slice(x * ny * LANES, (x + 1) * ny * LANES)
        cur = h_in[:, span]
        res = perceptron(w_in, b, w_out, [cur, jnp.concatenate(pieces, axis=1)])
        write(x, cur.astype(F32) + res)
    return rim_h


def middle_kernel(sizes, layer, last, h_in, p_in, hr_in, er_in, wr_in, pr_in, rxe, rxo, rye, ryo,
                  nin, nout, nbias, win, wout, bias, e_in, w_in, *rest):
    nx, ny = sizes
    span = ny * LANES
    if last:
        h_out, p_out, hr_out, pr_out, sxe, sxo, e_buf, w_buf, sems = rest
        e_out = er_out = e_new = None
    else:
        e_out, h_out, p_out, hr_out, er_out, pr_out, sxe, sxo, e_buf, w_buf, sems, e_new = rest

    def fetch(x):
        part = pl.ds(x * span, span)
        return pltpu.make_async_copy(e_in.at[:, :, part], e_buf.at[:, :, part], sems.at[x])

    def store(x):
        part = pl.ds(x * span, span)
        return pltpu.make_async_copy(e_new.at[:, :, part], e_out.at[:, :, part], sems.at[nx + 1 + x])

    fetch_w = pltpu.make_async_copy(w_in, w_buf, sems.at[nx])
    fetch_w.start()
    for x in range(nx):
        fetch(x).start()

    def write(x, value):
        h_out[:, x * span : (x + 1) * span] = value.astype(BF16)

    rim_h = node_stage(
        sizes, layer, h_in, p_in, hr_in, pr_in, rxe, rxo, rye, ryo, nin, nout, nbias, write
    ).astype(BF16)
    hr_out[...] = rim_h
    layer += 1
    b = column(bias[layer : layer + 1, :])
    updated, sums = rim_edges(
        sizes,
        [tile(rim_h, i).astype(F32) for i in range(4)],
        [[tile(er_in[d], i).astype(F32) for i in range(4)] for d in range(3)],
        [tile(wr_in, i) for i in range(4)],
        win[layer], wout[layer], b,
    )
    for i in range(4):
        pr_out[:, i * LANES : (i + 1) * LANES] = sums[i]
    if not last:
        for d in range(3):
            er_out[d] = updated[d].astype(BF16)
    fetch_w.wait()

    def slab_of(x):
        fetch(x).wait()
        return e_buf, e_new

    edge_stage(
        sizes, last, h_out, slab_of, w_buf, win[layer], wout[layer], b, p_out,
        (lambda x: None) if last else (lambda x: store(x).start()),
    )
    write_x_faces(sizes, p_out, sums, sxe, sxo)
    if not last:
        for x in range(nx):
            store(x).wait()


def last_kernel(
    sizes, layer, h_in, p_in, hr_in, pr_in, rxe, rxo, rye, ryo, nin, nout, nbias, out, res, buf
):
    nx, ny = sizes
    rows = nx * ny

    def write(x, value):
        res[:, x * ny * LANES : (x + 1) * ny * LANES] = value

    rim_h = node_stage(
        sizes, layer, h_in, p_in, hr_in, pr_in, rxe, rxo, rye, ryo, nin, nout, nbias, write
    )
    lane = lanes_of()
    upper = turn(tile(rim_h, 0), -4)
    lower = tile(rim_h, 1)
    for k in range(rows):
        t = res[:, k * LANES : (k + 1) * LANES]
        t = jnp.where(lane < 3, turn(lower, -4 * k), t)
        t = jnp.where(lane >= LANES - 3, turn(upper, -4 * k), t)
        buf[pl.ds(k, 32, stride=rows), :] = t
    out[...] = buf[...].reshape(out.shape).astype(BF16)


def call(body, fast, slow, outs, scratch=(), flops=0):
    vmem = pl.BlockSpec(memory_space=pltpu.VMEM)
    anywhere = pl.BlockSpec(memory_space=pl.ANY)
    fast = [pltpu.with_memory_space_constraint(a, pltpu.VMEM) for a in fast]
    slow_spec = anywhere if fast else vmem
    return pl.pallas_call(
        body,
        out_shape=[
            pltpu.VMEM(s, d) if where == "fast" else jax.ShapeDtypeStruct(s, d)
            for s, d, where in outs
        ],
        in_specs=[vmem] * len(fast) + [slow_spec] * len(slow),
        out_specs=[anywhere if where == "slow" else vmem for _, _, where in outs],
        scratch_shapes=list(scratch),
        cost_estimate=pl.CostEstimate(flops=flops, bytes_accessed=0, transcendentals=0),
    )(*fast, *slow)


def on_device(
    features, edge_state, multiplicity, edge_in, edge_out, edge_bias, node_in, node_out, node_bias
):
    ch, nx, ny, nz = features.shape
    layers = edge_in.shape[0]
    sizes = (nx, ny)
    rows = nx * ny
    nodes = rows * nz
    h_t = ((ch, nodes), BF16, "fast")
    p_t = ((ch, nodes), F32, "fast")
    e_shape = (3, ch, nodes)
    e_t = (e_shape, BF16, "slow")
    w_shape = (rows, 8, nz)
    sx_t = ((ch, (ny + 1) * nz), F32, "fast")
    sy_t = ((ch, (nx + 1) * nz), F32, "fast")
    hr_t = ((ch, 4 * LANES), BF16, "fast")
    er_t = ((3, ch, 4 * LANES), BF16, "fast")
    wr_t = ((8, 4 * LANES), F32, "fast")
    pr_t = ((ch, 4 * LANES), F32, "fast")
    z_rows = 4 * ch + 8
    sz_t = ((z_rows, LANES), F32, "fast")
    e_scratch = pltpu.VMEM(e_shape, BF16)
    work = 2 * 5 * 3 * ch * ch * nodes

    h, e0, w, own, sze, szo = call(
        functools.partial(unpack_kernel, sizes),
        (),
        (features, edge_state, multiplicity),
        (h_t, (e_shape, BF16, "fast"), (w_shape, F32, "fast"), ((4, z_rows, LANES), F32, "fast"),
         sz_t, sz_t),
        (pltpu.VMEM((4, ch * rows, nz), F32),),
    )
    rze, rzo = exchange(sze, szo, "gz", "gx")
    e, p = call(
        functools.partial(first_edges, sizes),
        (h, e0, w, edge_in, edge_out, edge_bias),
        (),
        (e_t, p_t),
        (e_scratch, pltpu.SemaphoreType.DMA((nx,))),
        flops=4 * work,
    )
    hr, er, wr, pr, sxe, sxo = call(
        functools.partial(first_rim, sizes),
        (p, own, rze, rzo, edge_in, edge_out, edge_bias),
        (),
        (hr_t, er_t, wr_t, pr_t, sx_t, sx_t),
    )
    for layer in range(layers):
        rxe, rxo = exchange(sxe, sxo, "gx", "gz")
        sye, syo, pr = call(
            functools.partial(y_faces, sizes), (p, pr, rxe, rxo), (), (sy_t, sy_t, pr_t)
        )
        rye, ryo = exchange(sye, syo, "gy", "gx")
        got = (rxe, rxo, rye, ryo)
        node = (node_in, node_out, node_bias)
        if layer + 1 < layers:
            last = layer + 2 == layers
            outs = (h_t, p_t, hr_t, pr_t, sx_t, sx_t) if last else (
                e_t, h_t, p_t, hr_t, er_t, pr_t, sx_t, sx_t)
            scratch = (e_scratch, pltpu.VMEM(w_shape, F32), pltpu.SemaphoreType.DMA((2 * nx + 1,)))
            res = call(
                functools.partial(middle_kernel, sizes, layer, last),
                (h, p, hr, er, wr, pr, *got, *node, edge_in, edge_out, edge_bias),
                (e, w),
                outs,
                scratch if last else scratch + (e_scratch,),
            )
            if last:
                h, p, hr, pr, sxe, sxo = res
            else:
                e, h, p, hr, er, pr, sxe, sxo = res
        else:
            (out,) = call(
                functools.partial(last_kernel, sizes, layer),
                (h, p, hr, pr, *got, *node),
                (),
                ((features.shape, BF16, "out"),),
                (pltpu.VMEM((ch, nodes), F32), pltpu.VMEM((ch * rows, nz), F32)),
            )
    return out


def solution(mesh):
    placed = (
        P(None, "gx", "gy", "gz"),
        P(None, None, "gx", "gy", "gz"),
        P("gx", "gy", "gz"),
        P(),
        P(),
        P(),
        P(),
        P(),
        P(),
    )
    return jax.shard_map(
        on_device, mesh=mesh, in_specs=placed, out_specs=P(None, "gx", "gy", "gz"), check_vma=False
    )
```

```python
import functools

import jax
import jax.numpy as jnp
from jax import lax
from jax.experimental import pallas as pl
from jax.experimental.pallas import tpu as pltpu
from jax.sharding import PartitionSpec as P

F32 = jnp.float32
BF16 = jnp.bfloat16
LANES = 128
AXES = ("gx", "gy", "gz")


def even_pairs(count):
    return [(i, i ^ 1) for i in range(count)]


def odd_pairs(axis, spare):
    sizes = [lax.axis_size(a) for a in AXES]
    at, other = AXES.index(axis), AXES.index(spare)
    pairs = []
    for i in range(sizes[0]):
        for j in range(sizes[1]):
            for k in range(sizes[2]):
                here = [i, j, k]
                there = list(here)
                if 0 < here[at] < sizes[at] - 1:
                    there[at] = ((here[at] + 1) ^ 1) - 1
                else:
                    there[other] = here[other] ^ 1
                flat = [(v[0] * sizes[1] + v[1]) * sizes[2] + v[2] for v in (here, there)]
                pairs.append(tuple(flat))
    return pairs


def exchange(even, odd, axis, spare):
    got_even = lax.ppermute(even, axis, even_pairs(lax.axis_size(axis)))
    got_odd = lax.ppermute(odd, AXES, odd_pairs(axis, spare))
    return got_even, got_odd


def silu(v):
    half = 0.5 * v
    return half + half * jnp.tanh(half)


def column(row):
    width = row.shape[1]
    eye = lax.broadcasted_iota(jnp.int32, (width, width), 0) == lax.broadcasted_iota(
        jnp.int32, (width, width), 1
    )
    return jnp.sum(jnp.where(eye, row, 0.0), axis=1, keepdims=True)


def tile(values, k):
    return values[:, k * LANES : (k + 1) * LANES]


def turn(values, shift):
    shift %= LANES
    return pltpu.roll(values, shift, 1) if shift else values


def place(axis, got_even, got_odd):
    position, count = lax.axis_index(axis), lax.axis_size(axis)
    is_even = position % 2 == 0
    low = jnp.where(is_even, got_odd, got_even)
    high = jnp.where(is_even, got_even, got_odd)
    low = jnp.where(position > 0, low, 0.0)
    high = jnp.where(position < count - 1, high, 0.0)
    return low, high


def lanes_of(rows=32):
    return lax.broadcasted_iota(jnp.int32, (rows, LANES), 1)


def perceptron(w_in, bias, w_out, pieces):
    stacked = jnp.concatenate([p.astype(BF16) for p in pieces], axis=0)
    pre = jnp.dot(w_in, stacked, preferred_element_type=F32) + bias
    return jnp.dot(w_out, silu(pre).astype(BF16), preferred_element_type=F32)


def rim_edges(sizes, h, e, w, w_in, w_out, bias):
    nx, ny = sizes
    lane = lanes_of()
    at, y_at = lane % 4, (lane // 4) % ny
    x_step = 4 * ny
    outer = len(h) == 5
    a, b, d, t = h[:4]
    o = h[4] if outer else jnp.zeros_like(a)
    ahead_z = [
        jnp.where(at < 3, turn(a, -1), 0.0),
        jnp.where(at < 3, turn(b, -1), d),
        jnp.where(at < 2, turn(d, -1), jnp.where(at == 2, o, turn(o, 2))),
        jnp.where(at == 0, a, jnp.where(at < 3, turn(t, -1), 0.0)),
    ]
    if outer:
        ahead_z.append(jnp.where(at == 0, t, jnp.where(at == 3, turn(t, 2), 0.0)))
    ahead_x = [jnp.where(lane < x_step * (nx - 1), turn(v, -x_step), 0.0) for v in h]
    ahead_y = [jnp.where(y_at < ny - 1, turn(v, -4), 0.0) for v in h]
    cur = jnp.concatenate(h, axis=1)
    updated, weighted = [], []
    for k, shifted in enumerate((ahead_x, ahead_y, ahead_z)):
        edge = jnp.concatenate(e[k], axis=1)
        msg = perceptron(w_in, bias, w_out, [cur, jnp.concatenate(shifted, axis=1), edge])
        updated.append(edge + msg)
        weighted.append([tile(msg, i) * w[i][k : k + 1, :] for i in range(len(h))])
    wx, wy, wz = weighted
    wo = wz[4] if outer else jnp.zeros_like(a)
    behind = [
        jnp.where(at == 0, wz[3], turn(wz[0], 1)),
        jnp.where(at == 0, 0.0, turn(wz[1], 1)),
        jnp.where(at == 3, wz[1], jnp.where(at == 0, 0.0, turn(wz[2], 1))),
        jnp.where(at == 0, wo, jnp.where(at == 1, turn(wo, -2), turn(wz[3], 1))),
    ]
    sums = [
        wx[i] + wy[i] + wz[i] + turn(wx[i], x_step) + turn(wy[i], 4) + behind[i] for i in range(4)
    ]
    return updated, sums


def quarters(lane, parts):
    q = lane // 32
    return jnp.where(
        q == 0, parts[0], jnp.where(q == 1, parts[1], jnp.where(q == 2, parts[2], parts[3]))
    )


def rim_x_faces(sums):
    lane = lanes_of()
    low = quarters(lane, [turn(v, 32 * i) for i, v in enumerate(sums)])
    high = quarters(lane, [turn(v, 32 * i - 64) for i, v in enumerate(sums)])
    return low, high


def rim_add_x(sums, low, high):
    q = lanes_of() // 32
    return [
        v
        + jnp.where(q == 0, turn(low, -32 * i), 0.0)
        + jnp.where(q == 2, turn(high, 64 - 32 * i), 0.0)
        for i, v in enumerate(sums)
    ]


def rim_y_faces(sums):
    group = (lanes_of() // 4) % 8
    packed = jnp.zeros_like(sums[0])
    for i, v in enumerate(sums):
        packed = jnp.where(group == i, turn(v, 4 * i), packed)
        packed = jnp.where(group == 4 + i, turn(v, 4 * i - 12), packed)
    return packed


def rim_add_y(sums, low, high):
    group = (lanes_of() // 4) % 8
    return [
        v
        + jnp.where(group == 0, turn(low, -16 - 4 * i), 0.0)
        + jnp.where(group == 7, turn(high, 28 - 4 * i), 0.0)
        for i, v in enumerate(sums)
    ]


def rim_join_z(sums):
    a, b, d, t = sums
    at = lanes_of() % 4
    return [
        a + jnp.where(at == 3, turn(d, 3), 0.0),
        b + jnp.where(at == 0, turn(t, -3), 0.0),
        d + jnp.where(at == 0, turn(a, -3), 0.0),
        t + jnp.where(at == 3, turn(b, 3), 0.0),
    ]


def span_of(first, count):
    return slice(first * LANES, (first + count) * LANES)


def ahead_along_z(values):
    lane = lanes_of()
    return jnp.concatenate(
        [
            jnp.where(lane < LANES - 1, turn(tile(values, k).astype(F32), -1), 0.0).astype(BF16)
            for k in range(values.shape[1] // LANES)
        ],
        axis=1,
    )


def edge_rows(sizes, first, count, last, h_ref, e_in, e_out, w_ref, w_in, w_out, bias, p_ref):
    nx, ny = sizes
    whole = first + count == ny
    prev_x = None
    for x in range(nx):
        k0 = x * ny + first
        rows = span_of(k0, count)
        cur = h_ref[:, rows]
        ahead_x = h_ref[:, span_of(k0 + ny, count)] if x + 1 < nx else jnp.zeros_like(cur)
        ahead_y = cur[:, LANES:]
        if whole:
            ahead_y = jnp.concatenate([ahead_y, jnp.zeros((32, LANES), BF16)], axis=1)
        weighted = []
        for d, shifted in enumerate((ahead_x, ahead_y, ahead_along_z(cur))):
            n = shifted.shape[1]
            part = slice(k0 * LANES, k0 * LANES + n)
            edge = e_in[d, :, part]
            msg = perceptron(w_in, bias, w_out, [cur[:, :n], shifted, edge])
            if not last:
                e_out[d, :, part] = (edge.astype(F32) + msg).astype(BF16)
            weighted.append(
                [tile(msg, i) * w_ref[k0 + i, d : d + 1, :] for i in range(n // LANES)]
            )
        wx, wy, wz = weighted
        for i in range(count):
            acc = wx[i] + wz[i] + turn(wz[i], 1)
            if i < len(wy):
                acc = acc + wy[i]
            if i > 0:
                acc = acc + wy[i - 1]
            if x > 0:
                acc = acc + prev_x[i]
            p_ref[:, span_of(k0 + i, 1)] = acc
        prev_x = wx


def write_x_faces(sizes, p_ref, sums, sxe, sxo):
    nx, ny = sizes
    span = ny * LANES
    low_rim, high_rim = rim_x_faces(sums)
    is_even = lax.axis_index("gx") % 2 == 0
    sxe[:, span:] = jnp.where(is_even, high_rim, low_rim)
    sxo[:, span:] = jnp.where(is_even, low_rim, high_rim)
    low = slice(0, span)
    high = slice((nx - 1) * span, nx * span)

    @pl.when(is_even)
    def _():
        sxe[:, :span] = p_ref[:, high]
        sxo[:, :span] = p_ref[:, low]

    @pl.when(jnp.logical_not(is_even))
    def _():
        sxe[:, :span] = p_ref[:, low]
        sxo[:, :span] = p_ref[:, high]


def unpack_kernel(
    sizes, f_in, es_in, m_in, h_ref, e_ref, w_ref, own_ref, sze, szo, buf, f_ref, es_ref, m_ref, sems
):
    nx, ny = sizes
    rows = nx * ny
    fetches = [pltpu.make_async_copy(m_in, m_ref, sems.at[0])]
    fetches.append(pltpu.make_async_copy(f_in, f_ref, sems.at[1]))
    for d in range(3):
        fetches.append(pltpu.make_async_copy(es_in.at[d], es_ref.at[d], sems.at[2 + d]))
    for fetch in fetches:
        fetch.start()
    fetches[0].wait()
    counts = m_ref[...]
    fluid = counts[1, 1:2, 1:2] > 0
    lane = lax.broadcasted_iota(jnp.int32, (ny, LANES), 1)
    sub = lax.broadcasted_iota(jnp.int32, (ny, LANES), 0)
    for x in range(nx):
        here = counts[x]
        shares = []
        for d in range(3):
            if d == 0:
                there = counts[x + 1] if x + 1 < nx else jnp.zeros_like(here)
            elif d == 1:
                there = jnp.where(sub < ny - 1, pltpu.roll(here, ny - 1, 0), 0)
            else:
                there = jnp.where(lane < LANES - 1, pltpu.roll(here, LANES - 1, 1), 0)
            shared = jnp.minimum(here, there)
            share = 1.0 / jnp.maximum(shared, 1).astype(F32)
            shares.append(jnp.where(fluid & (shared > 0), share, 0.0))
        for y in range(ny):
            for d in range(3):
                w_ref[x * ny + y, d : d + 1, :] = shares[d][y : y + 1, :]
            w_ref[x * ny + y, 3:8, :] = jnp.zeros((5, LANES), F32)

    def collect(first, size, row_of):
        group = lanes_of(size) // 4
        found = [jnp.zeros((size, LANES), F32)] * 4
        for k in range(rows):
            turned = turn(row_of(k), 4 * k)
            for i, shift in enumerate((-1, 0, 1, -2)):
                found[i] = jnp.where(group == (k + shift) % 32, turned, found[i])
        for i, shift in enumerate((4, 0, -4, 8)):
            own_ref[i, first : first + size, :] = turn(found[i], shift)

    for field in range(4):
        fetches[1 + field].wait()
        source = f_ref[...] if field == 0 else es_ref[field - 1]
        buf[field] = source.astype(F32).reshape(buf.shape[1:])

        def row_of(k, field=field):
            t = buf[field, pl.ds(k, 32, stride=rows), :]
            if field == 0:
                h_ref[:, k * LANES : (k + 1) * LANES] = t.astype(BF16)
            else:
                e_ref[field - 1, :, k * LANES : (k + 1) * LANES] = t.astype(BF16)
            return t

        collect(32 * field, 32, row_of)
    collect(128, 8, lambda k: w_ref[k])
    is_even = lax.axis_index("gz") % 2 == 0
    sze[...] = jnp.where(is_even, own_ref[0], own_ref[1])
    szo[...] = jnp.where(is_even, own_ref[1], own_ref[0])


def first_edges(sizes, h_ref, e_ref, w_ref, win, wout, bias, e_out, p_ref):
    edge_rows(
        sizes, 0, sizes[1], False, h_ref, e_ref, e_out, w_ref, win[0], wout[0], column(bias[0:1, :]),
        p_ref,
    )


def first_rim(
    sizes, p_ref, own_ref, rze, rzo, win, wout, bias, hr_out, er_out, wr_out, pr_out, sxe, sxo
):
    at = lanes_of(own_ref.shape[1]) % 4
    own_a, own_b, upper, lower = (own_ref[i] for i in range(4))
    prev, nxt = place("gz", rze[...], rzo[...])
    tiles = [
        own_a,
        own_b,
        jnp.where(at == 3, turn(upper, 3), nxt),
        jnp.where(at == 0, turn(lower, -3), prev),
        jnp.where(
            at == 0,
            turn(lower, -2),
            jnp.where(at == 1, upper, jnp.where(at == 2, turn(nxt, -1), turn(prev, 3))),
        ),
    ]
    h = [t[0:32] for t in tiles]
    e = [[t[32 * (d + 1) : 32 * (d + 2)] for t in tiles] for d in range(3)]
    w = [t[128:136] for t in tiles]
    updated, sums = rim_edges(sizes, h, e, w, win[0], wout[0], column(bias[0:1, :]))
    for i in range(4):
        hr_out[:, i * LANES : (i + 1) * LANES] = h[i].astype(BF16)
        wr_out[:, i * LANES : (i + 1) * LANES] = w[i]
    for d in range(3):
        er_out[d] = updated[d][:, : 4 * LANES].astype(BF16)
    write_x_faces(sizes, p_ref, sums, sxe, sxo)
    for i in range(4):
        pr_out[:, i * LANES : (i + 1) * LANES] = sums[i]


def y_faces(sizes, p_ref, pr_ref, rxe, rxo, sye, syo, pr_out):
    nx, ny = sizes
    low_x, high_x = place("gx", rxe[...], rxo[...])
    faces = []
    for y in (0, ny - 1):
        pieces = []
        for x in range(nx):
            t = p_ref[:, (x * ny + y) * LANES : (x * ny + y + 1) * LANES]
            if x == 0:
                t = t + tile(low_x, y)
            if x == nx - 1:
                t = t + tile(high_x, y)
            pieces.append(t)
        faces.append(jnp.concatenate(pieces, axis=1))
    low, high = faces
    sums = rim_add_x([tile(pr_ref, i) for i in range(4)], tile(low_x, ny), tile(high_x, ny))
    packed = rim_y_faces(sums)
    for i in range(4):
        pr_out[:, i * LANES : (i + 1) * LANES] = sums[i]
    is_even = lax.axis_index("gy") % 2 == 0
    sye[:, : nx * LANES] = jnp.where(is_even, high, low)
    syo[:, : nx * LANES] = jnp.where(is_even, low, high)
    sye[:, nx * LANES :] = packed
    syo[:, nx * LANES :] = packed


def incoming(sizes, p_ref, faces_x, faces_y, x, y):
    nx, ny = sizes
    t = p_ref[:, span_of(x * ny + y, 1)]
    if x == 0:
        t = t + tile(faces_x[0], y)
    if x == nx - 1:
        t = t + tile(faces_x[1], y)
    if y == 0:
        t = t + tile(faces_y[0], x)
    if y == ny - 1:
        t = t + tile(faces_y[1], x)
    return t.astype(BF16)


def inner_nodes(sizes, layer, h_in, p_in, rxe, rxo, nin, nout, nbias, write):
    nx, ny = sizes
    faces_x = place("gx", rxe[...], rxo[...])
    w_in, w_out = nin[layer], nout[layer]
    b = column(nbias[layer : layer + 1, :])
    for x in range(nx):
        pieces = [incoming(sizes, p_in, faces_x, None, x, y) for y in range(1, ny - 1)]
        rows = span_of(x * ny + 1, ny - 2)
        cur = h_in[:, rows]
        res = perceptron(w_in, b, w_out, [cur, jnp.concatenate(pieces, axis=1)])
        write(rows, cur.astype(F32) + res)


def outer_nodes(sizes, layer, h_in, p_in, hr_in, pr_in, rxe, rxo, rye, ryo, nin, nout, nbias):
    nx, ny = sizes
    faces_x = place("gx", rxe[...], rxo[...])
    faces_y = place("gy", rye[...], ryo[...])
    w_in, w_out = nin[layer], nout[layer]
    b = column(nbias[layer : layer + 1, :])
    sums = [tile(pr_in, i) for i in range(4)]
    rim = rim_join_z(rim_add_y(sums, tile(faces_y[0], nx), tile(faces_y[1], nx)))
    outer = [(x, y) for x in range(nx) for y in (0, ny - 1)]
    cur = jnp.concatenate(
        [hr_in[...]] + [h_in[:, span_of(x * ny + y, 1)] for x, y in outer], axis=1
    )
    inc = jnp.concatenate(
        [t.astype(BF16) for t in rim]
        + [incoming(sizes, p_in, faces_x, faces_y, x, y) for x, y in outer],
        axis=1,
    )
    new = cur.astype(F32) + perceptron(w_in, b, w_out, [cur, inc])
    return new[:, : 4 * LANES], new[:, 4 * LANES :]


def inner_kernel(
    sizes, layer, last, h_in, p_in, rxe, rxo, syo, nin, nout, nbias, win, wout, bias, e_in, w_in,
    h_out, p_out, e_out, w_out, syo_out, sems,
):
    ny = sizes[1]
    fetch_e = pltpu.make_async_copy(e_in, e_out, sems.at[0])
    fetch_w = pltpu.make_async_copy(w_in, w_out, sems.at[1])
    fetch_e.start()
    fetch_w.start()
    syo_out[...] = syo[...]

    def write(rows, value):
        h_out[:, rows] = value.astype(BF16)

    inner_nodes(sizes, layer, h_in, p_in, rxe, rxo, nin, nout, nbias, write)
    layer += 1
    fetch_e.wait()
    fetch_w.wait()
    edge_rows(
        sizes, 1, ny - 2, last, h_out, e_out, e_out, w_out, win[layer], wout[layer],
        column(bias[layer : layer + 1, :]), p_out,
    )


def outer_kernel(
    sizes, layer, last, h_in, p_in, hr_in, er_in, wr_in, pr_in, rxe, rxo, rye, ryo, nin, nout, nbias,
    win, wout, bias, w_ref, h_new, p_new, e_new, *outs,
):
    nx, ny = sizes
    if last:
        h_out, p_out, hr_out, pr_out, sxe, sxo = outs
    else:
        h_out, p_out, e_out, hr_out, er_out, pr_out, sxe, sxo = outs
    rim_h, edge_h = outer_nodes(
        sizes, layer, h_in, p_in, hr_in, pr_in, rxe, rxo, rye, ryo, nin, nout, nbias
    )
    rim_h, edge_h = rim_h.astype(BF16), edge_h.astype(BF16)
    hr_out[...] = rim_h
    outer = [(x, y) for x in range(nx) for y in (0, ny - 1)]
    for i, (x, y) in enumerate(outer):
        h_out[:, span_of(x * ny + y, 1)] = tile(edge_h, i)
    layer += 1
    b = column(bias[layer : layer + 1, :])
    w_in, w_out = win[layer], wout[layer]
    updated, sums = rim_edges(
        sizes,
        [tile(rim_h, i).astype(F32) for i in range(4)],
        [[tile(er_in[d], i).astype(F32) for i in range(4)] for d in range(3)],
        [tile(wr_in, i) for i in range(4)],
        w_in, w_out, b,
    )
    for i in range(4):
        pr_out[:, i * LANES : (i + 1) * LANES] = sums[i]
    if not last:
        for d in range(3):
            er_out[d] = updated[d].astype(BF16)
    zero = jnp.zeros((32, LANES), BF16)
    mine = {place_of: tile(edge_h, i) for i, place_of in enumerate(outer)}
    cross = [(x, y) for x in range(nx) for y in (0, ny - 2, ny - 1)]
    from_y, to_y = [], []
    for x, y in cross:
        from_y.append(mine[x, y] if (x, y) in mine else h_new[:, span_of(x * ny + y, 1)])
        to_y.append(
            h_new[:, span_of(x * ny + 1, 1)] if y == 0 else mine[x, ny - 1] if y == ny - 2 else zero
        )
    ahead_x = jnp.concatenate([edge_h[:, 2 * LANES :], zero, zero], axis=1)
    weighted = []
    for d, (at, cur, ahead) in enumerate((
        (outer, edge_h, ahead_x),
        (cross, jnp.concatenate(from_y, axis=1), jnp.concatenate(to_y, axis=1)),
        (outer, edge_h, ahead_along_z(edge_h)),
    )):
        edge = jnp.concatenate([e_new[d, :, span_of(x * ny + y, 1)] for x, y in at], axis=1)
        msg = perceptron(w_in, b, w_out, [cur, ahead, edge])
        if not last:
            value = (edge.astype(F32) + msg).astype(BF16)
            for i, (x, y) in enumerate(at):
                e_out[d, :, span_of(x * ny + y, 1)] = tile(value, i)
        weighted.append(
            {
                (x, y): tile(msg, i) * w_ref[x * ny + y, d : d + 1, :]
                for i, (x, y) in enumerate(at)
            }
        )
    wx, wy, wz = weighted
    for x in range(nx):
        for y in (0, ny - 1):
            acc = wx[x, y] + wz[x, y] + turn(wz[x, y], 1) + wy[x, y]
            if x > 0:
                acc = acc + wx[x - 1, y]
            if y > 0:
                acc = acc + wy[x, y - 1]
            p_out[:, span_of(x * ny + y, 1)] = acc
        for y, add in ((1, wy[x, 0]), (ny - 2, wy[x, ny - 2])):
            p_out[:, span_of(x * ny + y, 1)] = p_new[:, span_of(x * ny + y, 1)] + add
    write_x_faces(sizes, p_out, sums, sxe, sxo)


def last_inner(sizes, layer, h_in, p_in, rxe, rxo, syo, nin, nout, nbias, res, syo_out):
    syo_out[...] = syo[...]

    def write(rows, value):
        res[:, rows] = value

    inner_nodes(sizes, layer, h_in, p_in, rxe, rxo, nin, nout, nbias, write)


def last_kernel(
    sizes, layer, h_in, p_in, hr_in, pr_in, rxe, rxo, rye, ryo, nin, nout, nbias, res, out, buf
):
    nx, ny = sizes
    rows = nx * ny
    rim_h, edge_h = outer_nodes(
        sizes, layer, h_in, p_in, hr_in, pr_in, rxe, rxo, rye, ryo, nin, nout, nbias
    )
    lane = lanes_of()
    upper = turn(tile(rim_h, 0), -4)
    lower = tile(rim_h, 1)
    for k in range(rows):
        x, y = divmod(k, ny)
        inside = 0 < y < ny - 1
        t = res[:, span_of(k, 1)] if inside else tile(edge_h, 2 * x + (y > 0))
        t = jnp.where(lane < 3, turn(lower, -4 * k), t)
        t = jnp.where(lane >= LANES - 3, turn(upper, -4 * k), t)
        buf[pl.ds(k, 32, stride=rows), :] = t
    out[...] = buf[...].reshape(out.shape).astype(BF16)


def call(body, fast, slow, outs, scratch=(), flops=0, aliases=()):
    vmem = pl.BlockSpec(memory_space=pltpu.VMEM)
    anywhere = pl.BlockSpec(memory_space=pl.ANY)
    fast = [pltpu.with_memory_space_constraint(a, pltpu.VMEM) for a in fast]
    if not fast:
        anywhere = pl.BlockSpec(memory_space=pltpu.HBM)
        slow = [pltpu.with_memory_space_constraint(a, pltpu.HBM) for a in slow]
    return pl.pallas_call(
        body,
        out_shape=[
            pltpu.VMEM(s, d) if where == "fast" else jax.ShapeDtypeStruct(s, d)
            for s, d, where in outs
        ],
        in_specs=[vmem] * len(fast) + [anywhere] * len(slow),
        out_specs=[vmem] * len(outs),
        scratch_shapes=list(scratch),
        input_output_aliases=dict(aliases),
        compiler_params=pltpu.CompilerParams(vmem_limit_bytes=12 * 2**20),
        cost_estimate=pl.CostEstimate(flops=flops, bytes_accessed=0, transcendentals=0),
    )(*fast, *slow)


def on_device(
    features, edge_state, multiplicity, edge_in, edge_out, edge_bias, node_in, node_out, node_bias
):
    ch, nx, ny, nz = features.shape
    layers = edge_in.shape[0]
    sizes = (nx, ny)
    rows = nx * ny
    nodes = rows * nz
    h_t = ((ch, nodes), BF16, "fast")
    p_t = ((ch, nodes), F32, "fast")
    e_shape = (3, ch, nodes)
    e_t = (e_shape, BF16, "fast")
    w_t = ((rows, 8, nz), F32, "fast")
    sx_t = ((ch, (ny + 1) * nz), F32, "fast")
    sy_t = ((ch, (nx + 1) * nz), F32, "fast")
    hr_t = ((ch, 4 * LANES), BF16, "fast")
    er_t = ((3, ch, 4 * LANES), BF16, "fast")
    wr_t = ((8, 4 * LANES), F32, "fast")
    pr_t = ((ch, 4 * LANES), F32, "fast")
    z_rows = 4 * ch + 8
    sz_t = ((z_rows, LANES), F32, "fast")
    work = 4 * 2 * 5 * 3 * ch * ch * nodes

    h, e0, w, own, sze, szo = call(
        functools.partial(unpack_kernel, sizes),
        (),
        (features, edge_state, multiplicity),
        (h_t, e_t, w_t, ((4, z_rows, LANES), F32, "fast"), sz_t, sz_t),
        (
            pltpu.VMEM((4, ch * rows, nz), F32),
            pltpu.VMEM(features.shape, BF16),
            pltpu.VMEM(edge_state.shape, BF16),
            pltpu.VMEM(multiplicity.shape, jnp.int32),
            pltpu.SemaphoreType.DMA((5,)),
        ),
    )
    rze, rzo = exchange(sze, szo, "gz", "gx")
    edge = (edge_in, edge_out, edge_bias)
    node = (node_in, node_out, node_bias)
    e, p = call(
        functools.partial(first_edges, sizes), (h, e0, w, *edge), (), (e_t, p_t), flops=work
    )
    hr, er, wr, pr, sxe, sxo = call(
        functools.partial(first_rim, sizes),
        (p, own, rze, rzo, *edge),
        (),
        (hr_t, er_t, wr_t, pr_t, sx_t, sx_t),
    )
    for layer in range(layers):
        got_x = exchange(sxe, sxo, "gx", "gz")
        sye, syo, pr = call(
            functools.partial(y_faces, sizes), (p, pr, *got_x), (), (sy_t, sy_t, pr_t)
        )
        even = lax.ppermute(sye, "gy", even_pairs(lax.axis_size("gy")))
        if layer + 1 < layers:
            last = layer + 2 == layers
            h_new, p_new, e_new, w_new, syo = call(
                functools.partial(inner_kernel, sizes, layer, last),
                (h, p, *got_x, syo, *node, *edge),
                (e, w),
                (h_t, p_t, e_t, w_t, sy_t),
                (pltpu.SemaphoreType.DMA((2,)),),
                flops=work,
            )
        else:
            res, syo = call(
                functools.partial(last_inner, sizes, layer),
                (h, p, *got_x, syo, *node),
                (),
                (((ch, nodes), F32, "fast"), sy_t),
                flops=work,
            )
        got = (*got_x, even, lax.ppermute(syo, AXES, odd_pairs("gy", "gx")))
        if layer + 1 < layers:
            outs = (hr_t, pr_t, sx_t, sx_t) if last else (e_t, hr_t, er_t, pr_t, sx_t, sx_t)
            args = (h, p, hr, er, wr, pr, *got, *node, *edge, w_new, h_new, p_new, e_new)
            n = len(args)
            moved = call(
                functools.partial(outer_kernel, sizes, layer, last),
                args,
                (),
                (h_t, p_t, *outs),
                aliases=((n - 3, 0), (n - 2, 1)) + (() if last else ((n - 1, 2),)),
            )
            if last:
                h, p, hr, pr, sxe, sxo = moved
            else:
                h, p, e, hr, er, pr, sxe, sxo = moved
        else:
            (out,) = call(
                functools.partial(last_kernel, sizes, layer),
                (h, p, hr, pr, *got, *node, res),
                (),
                ((features.shape, BF16, "out"),),
                (pltpu.VMEM((ch * rows, nz), F32),),
            )
    return out


def solution(mesh):
    placed = (
        P(None, "gx", "gy", "gz"),
        P(None, None, "gx", "gy", "gz"),
        P("gx", "gy", "gz"),
        P(),
        P(),
        P(),
        P(),
        P(),
        P(),
    )
    return jax.shard_map(
        on_device, mesh=mesh, in_specs=placed, out_specs=P(None, "gx", "gy", "gz"), check_vma=False
    )
```

```python
import functools

import jax
import jax.numpy as jnp
from jax import lax
from jax.experimental import pallas as pl
from jax.experimental.pallas import tpu as pltpu
from jax.sharding import PartitionSpec as P

F32 = jnp.float32
BF16 = jnp.bfloat16
LANES = 128
AXES = ("gx", "gy", "gz")


def even_pairs(count):
    return [(i, i ^ 1) for i in range(count)]


def odd_pairs(axis, spare):
    sizes = [lax.axis_size(a) for a in AXES]
    at, other = AXES.index(axis), AXES.index(spare)
    pairs = []
    for i in range(sizes[0]):
        for j in range(sizes[1]):
            for k in range(sizes[2]):
                here = [i, j, k]
                there = list(here)
                if 0 < here[at] < sizes[at] - 1:
                    there[at] = ((here[at] + 1) ^ 1) - 1
                else:
                    there[other] = here[other] ^ 1
                flat = [(v[0] * sizes[1] + v[1]) * sizes[2] + v[2] for v in (here, there)]
                pairs.append(tuple(flat))
    return pairs


def exchange(even, odd, axis, spare):
    got_even = lax.ppermute(even, axis, even_pairs(lax.axis_size(axis)))
    got_odd = lax.ppermute(odd, AXES, odd_pairs(axis, spare))
    return got_even, got_odd


def silu(v):
    half = 0.5 * v
    return half + half * jnp.tanh(half)


def column(row):
    width = row.shape[1]
    eye = lax.broadcasted_iota(jnp.int32, (width, width), 0) == lax.broadcasted_iota(
        jnp.int32, (width, width), 1
    )
    return jnp.sum(jnp.where(eye, row, 0.0), axis=1, keepdims=True)


def tile(values, k):
    return values[:, k * LANES : (k + 1) * LANES]


def turn(values, shift):
    shift %= LANES
    return pltpu.roll(values, shift, 1) if shift else values


def place(axis, got_even, got_odd):
    position, count = lax.axis_index(axis), lax.axis_size(axis)
    is_even = position % 2 == 0
    low = jnp.where(is_even, got_odd, got_even)
    high = jnp.where(is_even, got_even, got_odd)
    low = jnp.where(position > 0, low, 0.0)
    high = jnp.where(position < count - 1, high, 0.0)
    return low, high


def lanes_of(rows=32):
    return lax.broadcasted_iota(jnp.int32, (rows, LANES), 1)


def perceptron(w_in, bias, w_out, pieces):
    stacked = jnp.concatenate([p.astype(BF16) for p in pieces], axis=0)
    pre = jnp.dot(w_in, stacked, preferred_element_type=F32) + bias
    return jnp.dot(w_out, silu(pre).astype(BF16), preferred_element_type=F32)


def rim_edges(sizes, h, e, w, w_in, w_out, bias):
    nx, ny = sizes
    lane = lanes_of()
    at, y_at = lane % 4, (lane // 4) % ny
    x_step = 4 * ny
    outer = len(h) == 5
    a, b, d, t = h[:4]
    o = h[4] if outer else jnp.zeros_like(a)
    ahead_z = [
        jnp.where(at < 3, turn(a, -1), 0.0),
        jnp.where(at < 3, turn(b, -1), d),
        jnp.where(at < 2, turn(d, -1), jnp.where(at == 2, o, turn(o, 2))),
        jnp.where(at == 0, a, jnp.where(at < 3, turn(t, -1), 0.0)),
    ]
    if outer:
        ahead_z.append(jnp.where(at == 0, t, jnp.where(at == 3, turn(t, 2), 0.0)))
    ahead_x = [jnp.where(lane < x_step * (nx - 1), turn(v, -x_step), 0.0) for v in h]
    ahead_y = [jnp.where(y_at < ny - 1, turn(v, -4), 0.0) for v in h]
    cur = jnp.concatenate(h, axis=1)
    updated, weighted = [], []
    for k, shifted in enumerate((ahead_x, ahead_y, ahead_z)):
        edge = jnp.concatenate(e[k], axis=1)
        msg = perceptron(w_in, bias, w_out, [cur, jnp.concatenate(shifted, axis=1), edge])
        updated.append(edge + msg)
        weighted.append([tile(msg, i) * w[i][k : k + 1, :] for i in range(len(h))])
    wx, wy, wz = weighted
    wo = wz[4] if outer else jnp.zeros_like(a)
    behind = [
        jnp.where(at == 0, wz[3], turn(wz[0], 1)),
        jnp.where(at == 0, 0.0, turn(wz[1], 1)),
        jnp.where(at == 3, wz[1], jnp.where(at == 0, 0.0, turn(wz[2], 1))),
        jnp.where(at == 0, wo, jnp.where(at == 1, turn(wo, -2), turn(wz[3], 1))),
    ]
    sums = [
        wx[i] + wy[i] + wz[i] + turn(wx[i], x_step) + turn(wy[i], 4) + behind[i] for i in range(4)
    ]
    return updated, sums


def quarters(lane, parts):
    q = lane // 32
    return jnp.where(
        q == 0, parts[0], jnp.where(q == 1, parts[1], jnp.where(q == 2, parts[2], parts[3]))
    )


def rim_x_faces(sums):
    lane = lanes_of()
    low = quarters(lane, [turn(v, 32 * i) for i, v in enumerate(sums)])
    high = quarters(lane, [turn(v, 32 * i - 64) for i, v in enumerate(sums)])
    return low, high


def rim_add_x(sums, low, high):
    q = lanes_of() // 32
    return [
        v
        + jnp.where(q == 0, turn(low, -32 * i), 0.0)
        + jnp.where(q == 2, turn(high, 64 - 32 * i), 0.0)
        for i, v in enumerate(sums)
    ]


def rim_y_faces(sums):
    group = (lanes_of() // 4) % 8
    packed = jnp.zeros_like(sums[0])
    for i, v in enumerate(sums):
        packed = jnp.where(group == i, turn(v, 4 * i), packed)
        packed = jnp.where(group == 4 + i, turn(v, 4 * i - 12), packed)
    return packed


def rim_add_y(sums, low, high):
    group = (lanes_of() // 4) % 8
    return [
        v
        + jnp.where(group == 0, turn(low, -16 - 4 * i), 0.0)
        + jnp.where(group == 7, turn(high, 28 - 4 * i), 0.0)
        for i, v in enumerate(sums)
    ]


def rim_join_z(sums):
    a, b, d, t = sums
    at = lanes_of() % 4
    return [
        a + jnp.where(at == 3, turn(d, 3), 0.0),
        b + jnp.where(at == 0, turn(t, -3), 0.0),
        d + jnp.where(at == 0, turn(a, -3), 0.0),
        t + jnp.where(at == 3, turn(b, 3), 0.0),
    ]


def span_of(first, count):
    return slice(first * LANES, (first + count) * LANES)


def ahead_along_z(values):
    lane = lanes_of()
    return jnp.concatenate(
        [
            jnp.where(lane < LANES - 1, turn(tile(values, k).astype(F32), -1), 0.0).astype(BF16)
            for k in range(values.shape[1] // LANES)
        ],
        axis=1,
    )


def edge_rows(sizes, first, count, last, h_ref, e_in, e_out, w_ref, w_in, w_out, bias, p_ref):
    nx, ny = sizes
    whole = first + count == ny
    prev_x = None
    for x in range(nx):
        k0 = x * ny + first
        rows = span_of(k0, count)
        cur = h_ref[:, rows]
        ahead_x = h_ref[:, span_of(k0 + ny, count)] if x + 1 < nx else jnp.zeros_like(cur)
        ahead_y = cur[:, LANES:]
        if whole:
            ahead_y = jnp.concatenate([ahead_y, jnp.zeros((32, LANES), BF16)], axis=1)
        weighted = []
        for d, shifted in enumerate((ahead_x, ahead_y, ahead_along_z(cur))):
            n = shifted.shape[1]
            part = slice(k0 * LANES, k0 * LANES + n)
            edge = e_in[d, :, part]
            msg = perceptron(w_in, bias, w_out, [cur[:, :n], shifted, edge])
            if not last:
                e_out[d, :, part] = (edge.astype(F32) + msg).astype(BF16)
            weighted.append(
                [tile(msg, i) * w_ref[k0 + i, d : d + 1, :] for i in range(n // LANES)]
            )
        wx, wy, wz = weighted
        for i in range(count):
            acc = wx[i] + wz[i] + turn(wz[i], 1)
            if i < len(wy):
                acc = acc + wy[i]
            if i > 0:
                acc = acc + wy[i - 1]
            if x > 0:
                acc = acc + prev_x[i]
            p_ref[:, span_of(k0 + i, 1)] = acc
        prev_x = wx


def write_x_faces(sizes, p_ref, sums, sxe, sxo):
    nx, ny = sizes
    span = ny * LANES
    low_rim, high_rim = rim_x_faces(sums)
    is_even = lax.axis_index("gx") % 2 == 0
    sxe[:, span:] = jnp.where(is_even, high_rim, low_rim)
    sxo[:, span:] = jnp.where(is_even, low_rim, high_rim)
    low = slice(0, span)
    high = slice((nx - 1) * span, nx * span)

    @pl.when(is_even)
    def _():
        sxe[:, :span] = p_ref[:, high]
        sxo[:, :span] = p_ref[:, low]

    @pl.when(jnp.logical_not(is_even))
    def _():
        sxe[:, :span] = p_ref[:, low]
        sxo[:, :span] = p_ref[:, high]


def unpack_kernel(
    sizes, f_in, es_in, m_in, h_ref, e_ref, w_ref, own_ref, sze, szo, buf, f_ref, es_ref, m_ref, sems
):
    nx, ny = sizes
    rows = nx * ny
    fetches = [pltpu.make_async_copy(m_in, m_ref, sems.at[0])]
    fetches.append(pltpu.make_async_copy(f_in, f_ref, sems.at[1]))
    for d in range(3):
        fetches.append(pltpu.make_async_copy(es_in.at[d], es_ref.at[d], sems.at[2 + d]))
    for fetch in fetches:
        fetch.start()
    fetches[0].wait()
    counts = m_ref[...]
    fluid = counts[1, 1:2, 1:2] > 0
    lane = lax.broadcasted_iota(jnp.int32, (ny, LANES), 1)
    sub = lax.broadcasted_iota(jnp.int32, (ny, LANES), 0)
    for x in range(nx):
        here = counts[x]
        shares = []
        for d in range(3):
            if d == 0:
                there = counts[x + 1] if x + 1 < nx else jnp.zeros_like(here)
            elif d == 1:
                there = jnp.where(sub < ny - 1, pltpu.roll(here, ny - 1, 0), 0)
            else:
                there = jnp.where(lane < LANES - 1, pltpu.roll(here, LANES - 1, 1), 0)
            shared = jnp.minimum(here, there)
            share = 1.0 / jnp.maximum(shared, 1).astype(F32)
            shares.append(jnp.where(fluid & (shared > 0), share, 0.0))
        for y in range(ny):
            for d in range(3):
                w_ref[x * ny + y, d : d + 1, :] = shares[d][y : y + 1, :]
            w_ref[x * ny + y, 3:8, :] = jnp.zeros((5, LANES), F32)

    def collect(first, size, row_of):
        group = lanes_of(size) // 4
        found = [jnp.zeros((size, LANES), F32)] * 4
        for k in range(rows):
            turned = turn(row_of(k), 4 * k)
            for i, shift in enumerate((-1, 0, 1, -2)):
                found[i] = jnp.where(group == (k + shift) % 32, turned, found[i])
        for i, shift in enumerate((4, 0, -4, 8)):
            own_ref[i, first : first + size, :] = turn(found[i], shift)

    for field in range(4):
        fetches[1 + field].wait()
        source = f_ref[...] if field == 0 else es_ref[field - 1]
        buf[field] = source.astype(F32).reshape(buf.shape[1:])

        def row_of(k, field=field):
            t = buf[field, pl.ds(k, 32, stride=rows), :]
            if field == 0:
                h_ref[:, k * LANES : (k + 1) * LANES] = t.astype(BF16)
            else:
                e_ref[field - 1, :, k * LANES : (k + 1) * LANES] = t.astype(BF16)
            return t

        collect(32 * field, 32, row_of)
    collect(128, 8, lambda k: w_ref[k])
    is_even = lax.axis_index("gz") % 2 == 0
    sze[...] = jnp.where(is_even, own_ref[0], own_ref[1])
    szo[...] = jnp.where(is_even, own_ref[1], own_ref[0])


def first_edges(sizes, h_ref, e_ref, w_ref, win, wout, bias, e_out, p_ref):
    edge_rows(
        sizes, 0, sizes[1], False, h_ref, e_ref, e_out, w_ref, win[0], wout[0], column(bias[0:1, :]),
        p_ref,
    )


def first_rim(
    sizes, p_ref, own_ref, rze, rzo, win, wout, bias, hr_out, er_out, wr_out, pr_out, sxe, sxo
):
    at = lanes_of(own_ref.shape[1]) % 4
    own_a, own_b, upper, lower = (own_ref[i] for i in range(4))
    prev, nxt = place("gz", rze[...], rzo[...])
    tiles = [
        own_a,
        own_b,
        jnp.where(at == 3, turn(upper, 3), nxt),
        jnp.where(at == 0, turn(lower, -3), prev),
        jnp.where(
            at == 0,
            turn(lower, -2),
            jnp.where(at == 1, upper, jnp.where(at == 2, turn(nxt, -1), turn(prev, 3))),
        ),
    ]
    h = [t[0:32] for t in tiles]
    e = [[t[32 * (d + 1) : 32 * (d + 2)] for t in tiles] for d in range(3)]
    w = [t[128:136] for t in tiles]
    updated, sums = rim_edges(sizes, h, e, w, win[0], wout[0], column(bias[0:1, :]))
    for i in range(4):
        hr_out[:, i * LANES : (i + 1) * LANES] = h[i].astype(BF16)
        wr_out[:, i * LANES : (i + 1) * LANES] = w[i]
    for d in range(3):
        er_out[d] = updated[d][:, : 4 * LANES].astype(BF16)
    write_x_faces(sizes, p_ref, sums, sxe, sxo)
    for i in range(4):
        pr_out[:, i * LANES : (i + 1) * LANES] = sums[i]


def y_faces(sizes, p_ref, pr_ref, rxe, rxo, sye, syo, pr_out):
    nx, ny = sizes
    low_x, high_x = place("gx", rxe[...], rxo[...])
    faces = []
    for y in (0, ny - 1):
        pieces = []
        for x in range(nx):
            t = p_ref[:, (x * ny + y) * LANES : (x * ny + y + 1) * LANES]
            if x == 0:
                t = t + tile(low_x, y)
            if x == nx - 1:
                t = t + tile(high_x, y)
            pieces.append(t)
        faces.append(jnp.concatenate(pieces, axis=1))
    low, high = faces
    sums = rim_add_x([tile(pr_ref, i) for i in range(4)], tile(low_x, ny), tile(high_x, ny))
    packed = rim_y_faces(sums)
    for i in range(4):
        pr_out[:, i * LANES : (i + 1) * LANES] = sums[i]
    is_even = lax.axis_index("gy") % 2 == 0
    sye[:, : nx * LANES] = jnp.where(is_even, high, low)
    syo[:, : nx * LANES] = jnp.where(is_even, low, high)
    sye[:, nx * LANES :] = packed
    syo[:, nx * LANES :] = packed


def incoming(sizes, p_ref, faces_x, faces_y, x, y):
    nx, ny = sizes
    t = p_ref[:, span_of(x * ny + y, 1)]
    if x == 0:
        t = t + tile(faces_x[0], y)
    if x == nx - 1:
        t = t + tile(faces_x[1], y)
    if y == 0:
        t = t + tile(faces_y[0], x)
    if y == ny - 1:
        t = t + tile(faces_y[1], x)
    return t.astype(BF16)


def inner_nodes(sizes, layer, h_in, p_in, rxe, rxo, nin, nout, nbias, write):
    nx, ny = sizes
    faces_x = place("gx", rxe[...], rxo[...])
    w_in, w_out = nin[layer], nout[layer]
    b = column(nbias[layer : layer + 1, :])
    for x in range(nx):
        pieces = [incoming(sizes, p_in, faces_x, None, x, y) for y in range(1, ny - 1)]
        rows = span_of(x * ny + 1, ny - 2)
        cur = h_in[:, rows]
        res = perceptron(w_in, b, w_out, [cur, jnp.concatenate(pieces, axis=1)])
        write(rows, cur.astype(F32) + res)


def outer_nodes(sizes, layer, h_in, p_in, hr_in, pr_in, rxe, rxo, rye, ryo, nin, nout, nbias):
    nx, ny = sizes
    faces_x = place("gx", rxe[...], rxo[...])
    faces_y = place("gy", rye[...], ryo[...])
    w_in, w_out = nin[layer], nout[layer]
    b = column(nbias[layer : layer + 1, :])
    sums = [tile(pr_in, i) for i in range(4)]
    rim = rim_join_z(rim_add_y(sums, tile(faces_y[0], nx), tile(faces_y[1], nx)))
    outer = [(x, y) for x in range(nx) for y in (0, ny - 1)]
    cur = jnp.concatenate(
        [hr_in[...]] + [h_in[:, span_of(x * ny + y, 1)] for x, y in outer], axis=1
    )
    inc = jnp.concatenate(
        [t.astype(BF16) for t in rim]
        + [incoming(sizes, p_in, faces_x, faces_y, x, y) for x, y in outer],
        axis=1,
    )
    new = cur.astype(F32) + perceptron(w_in, b, w_out, [cur, inc])
    return new[:, : 4 * LANES], new[:, 4 * LANES :]


def inner_kernel(
    sizes, layer, last, h_in, p_in, rxe, rxo, nin, nout, nbias, win, wout, bias, e_in, w_in,
    h_out, p_out, e_out, w_out, sems,
):
    ny = sizes[1]
    fetch_e = pltpu.make_async_copy(e_in, e_out, sems.at[0])
    fetch_w = pltpu.make_async_copy(w_in, w_out, sems.at[1])
    fetch_e.start()
    fetch_w.start()

    def write(rows, value):
        h_out[:, rows] = value.astype(BF16)

    inner_nodes(sizes, layer, h_in, p_in, rxe, rxo, nin, nout, nbias, write)
    layer += 1
    fetch_e.wait()
    fetch_w.wait()
    edge_rows(
        sizes, 1, ny - 2, last, h_out, e_out, e_out, w_out, win[layer], wout[layer],
        column(bias[layer : layer + 1, :]), p_out,
    )


def outer_kernel(
    sizes, layer, last, h_in, p_in, hr_in, er_in, wr_in, pr_in, rxe, rxo, rye, ryo, nin, nout, nbias,
    win, wout, bias, w_ref, h_new, p_new, e_new, *outs,
):
    nx, ny = sizes
    if last:
        h_out, p_out, hr_out, pr_out, sxe, sxo = outs
    else:
        h_out, p_out, e_out, hr_out, er_out, pr_out, sxe, sxo = outs
    rim_h, edge_h = outer_nodes(
        sizes, layer, h_in, p_in, hr_in, pr_in, rxe, rxo, rye, ryo, nin, nout, nbias
    )
    rim_h, edge_h = rim_h.astype(BF16), edge_h.astype(BF16)
    hr_out[...] = rim_h
    outer = [(x, y) for x in range(nx) for y in (0, ny - 1)]
    for i, (x, y) in enumerate(outer):
        h_out[:, span_of(x * ny + y, 1)] = tile(edge_h, i)
    layer += 1
    b = column(bias[layer : layer + 1, :])
    w_in, w_out = win[layer], wout[layer]
    updated, sums = rim_edges(
        sizes,
        [tile(rim_h, i).astype(F32) for i in range(4)],
        [[tile(er_in[d], i).astype(F32) for i in range(4)] for d in range(3)],
        [tile(wr_in, i) for i in range(4)],
        w_in, w_out, b,
    )
    for i in range(4):
        pr_out[:, i * LANES : (i + 1) * LANES] = sums[i]
    if not last:
        for d in range(3):
            er_out[d] = updated[d].astype(BF16)
    zero = jnp.zeros((32, LANES), BF16)
    mine = {place_of: tile(edge_h, i) for i, place_of in enumerate(outer)}
    cross = [(x, y) for x in range(nx) for y in (0, ny - 2, ny - 1)]
    from_y, to_y = [], []
    for x, y in cross:
        from_y.append(mine[x, y] if (x, y) in mine else h_new[:, span_of(x * ny + y, 1)])
        to_y.append(
            h_new[:, span_of(x * ny + 1, 1)] if y == 0 else mine[x, ny - 1] if y == ny - 2 else zero
        )
    ahead_x = jnp.concatenate([edge_h[:, 2 * LANES :], zero, zero], axis=1)
    weighted = []
    for d, (at, cur, ahead) in enumerate((
        (outer, edge_h, ahead_x),
        (cross, jnp.concatenate(from_y, axis=1), jnp.concatenate(to_y, axis=1)),
        (outer, edge_h, ahead_along_z(edge_h)),
    )):
        edge = jnp.concatenate([e_new[d, :, span_of(x * ny + y, 1)] for x, y in at], axis=1)
        msg = perceptron(w_in, b, w_out, [cur, ahead, edge])
        if not last:
            value = (edge.astype(F32) + msg).astype(BF16)
            for i, (x, y) in enumerate(at):
                e_out[d, :, span_of(x * ny + y, 1)] = tile(value, i)
        weighted.append(
            {
                (x, y): tile(msg, i) * w_ref[x * ny + y, d : d + 1, :]
                for i, (x, y) in enumerate(at)
            }
        )
    wx, wy, wz = weighted
    for x in range(nx):
        for y in (0, ny - 1):
            acc = wx[x, y] + wz[x, y] + turn(wz[x, y], 1) + wy[x, y]
            if x > 0:
                acc = acc + wx[x - 1, y]
            if y > 0:
                acc = acc + wy[x, y - 1]
            p_out[:, span_of(x * ny + y, 1)] = acc
        for y, add in ((1, wy[x, 0]), (ny - 2, wy[x, ny - 2])):
            p_out[:, span_of(x * ny + y, 1)] = p_new[:, span_of(x * ny + y, 1)] + add
    write_x_faces(sizes, p_out, sums, sxe, sxo)


def last_inner(sizes, layer, h_in, p_in, rxe, rxo, nin, nout, nbias, res):
    def write(rows, value):
        res[:, rows] = value

    inner_nodes(sizes, layer, h_in, p_in, rxe, rxo, nin, nout, nbias, write)


def last_kernel(
    sizes, layer, h_in, p_in, hr_in, pr_in, rxe, rxo, rye, ryo, nin, nout, nbias, res, out, buf
):
    nx, ny = sizes
    rows = nx * ny
    rim_h, edge_h = outer_nodes(
        sizes, layer, h_in, p_in, hr_in, pr_in, rxe, rxo, rye, ryo, nin, nout, nbias
    )
    lane = lanes_of()
    upper = turn(tile(rim_h, 0), -4)
    lower = tile(rim_h, 1)
    for k in range(rows):
        x, y = divmod(k, ny)
        inside = 0 < y < ny - 1
        t = res[:, span_of(k, 1)] if inside else tile(edge_h, 2 * x + (y > 0))
        t = jnp.where(lane < 3, turn(lower, -4 * k), t)
        t = jnp.where(lane >= LANES - 3, turn(upper, -4 * k), t)
        buf[pl.ds(k, 32, stride=rows), :] = t
    out[...] = buf[...].reshape(out.shape).astype(BF16)


def call(body, fast, slow, outs, scratch=(), flops=0, aliases=()):
    vmem = pl.BlockSpec(memory_space=pltpu.VMEM)
    anywhere = pl.BlockSpec(memory_space=pl.ANY)
    fast = [pltpu.with_memory_space_constraint(a, pltpu.VMEM) for a in fast]
    if not fast:
        anywhere = pl.BlockSpec(memory_space=pltpu.HBM)
        slow = [pltpu.with_memory_space_constraint(a, pltpu.HBM) for a in slow]
    return pl.pallas_call(
        body,
        out_shape=[
            pltpu.VMEM(s, d) if where == "fast" else jax.ShapeDtypeStruct(s, d)
            for s, d, where in outs
        ],
        in_specs=[vmem] * len(fast) + [anywhere] * len(slow),
        out_specs=[vmem] * len(outs),
        scratch_shapes=list(scratch),
        input_output_aliases=dict(aliases),
        compiler_params=pltpu.CompilerParams(vmem_limit_bytes=12 * 2**20),
        cost_estimate=pl.CostEstimate(flops=flops, bytes_accessed=0, transcendentals=0),
    )(*fast, *slow)


def on_device(
    features, edge_state, multiplicity, edge_in, edge_out, edge_bias, node_in, node_out, node_bias
):
    ch, nx, ny, nz = features.shape
    layers = edge_in.shape[0]
    sizes = (nx, ny)
    rows = nx * ny
    nodes = rows * nz
    h_t = ((ch, nodes), BF16, "fast")
    p_t = ((ch, nodes), F32, "fast")
    e_shape = (3, ch, nodes)
    e_t = (e_shape, BF16, "fast")
    w_t = ((rows, 8, nz), F32, "fast")
    sx_t = ((ch, (ny + 1) * nz), F32, "fast")
    sy_t = ((ch, (nx + 1) * nz), F32, "fast")
    hr_t = ((ch, 4 * LANES), BF16, "fast")
    er_t = ((3, ch, 4 * LANES), BF16, "fast")
    wr_t = ((8, 4 * LANES), F32, "fast")
    pr_t = ((ch, 4 * LANES), F32, "fast")
    z_rows = 4 * ch + 8
    sz_t = ((z_rows, LANES), F32, "fast")
    work = 4 * 2 * 5 * 3 * ch * ch * nodes

    h, e0, w, own, sze, szo = call(
        functools.partial(unpack_kernel, sizes),
        (),
        (features, edge_state, multiplicity),
        (h_t, e_t, w_t, ((4, z_rows, LANES), F32, "fast"), sz_t, sz_t),
        (
            pltpu.VMEM((4, ch * rows, nz), F32),
            pltpu.VMEM(features.shape, BF16),
            pltpu.VMEM(edge_state.shape, BF16),
            pltpu.VMEM(multiplicity.shape, jnp.int32),
            pltpu.SemaphoreType.DMA((5,)),
        ),
    )
    rze, rzo = exchange(sze, szo, "gz", "gx")
    edge = (edge_in, edge_out, edge_bias)
    node = (node_in, node_out, node_bias)
    e, p = call(
        functools.partial(first_edges, sizes), (h, e0, w, *edge), (), (e_t, p_t), flops=work
    )
    hr, er, wr, pr, sxe, sxo = call(
        functools.partial(first_rim, sizes),
        (p, own, rze, rzo, *edge),
        (),
        (hr_t, er_t, wr_t, pr_t, sx_t, sx_t),
    )
    for layer in range(layers):
        got_x = exchange(sxe, sxo, "gx", "gz")
        sye, syo, pr = call(
            functools.partial(y_faces, sizes), (p, pr, *got_x), (), (sy_t, sy_t, pr_t)
        )
        got = (*got_x, *exchange(sye, syo, "gy", "gx"))
        if layer + 1 < layers:
            last = layer + 2 == layers
            h_new, p_new, e_new, w_new = call(
                functools.partial(inner_kernel, sizes, layer, last),
                (h, p, *got_x, *node, *edge),
                (e, w),
                (h_t, p_t, e_t, w_t),
                (pltpu.SemaphoreType.DMA((2,)),),
                flops=work,
            )
        else:
            (res,) = call(
                functools.partial(last_inner, sizes, layer),
                (h, p, *got_x, *node),
                (),
                (((ch, nodes), F32, "fast"),),
                flops=work,
            )
        if layer + 1 < layers:
            outs = (hr_t, pr_t, sx_t, sx_t) if last else (e_t, hr_t, er_t, pr_t, sx_t, sx_t)
            args = (h, p, hr, er, wr, pr, *got, *node, *edge, w_new, h_new, p_new, e_new)
            n = len(args)
            moved = call(
                functools.partial(outer_kernel, sizes, layer, last),
                args,
                (),
                (h_t, p_t, *outs),
                aliases=((n - 3, 0), (n - 2, 1)) + (() if last else ((n - 1, 2),)),
            )
            if last:
                h, p, hr, pr, sxe, sxo = moved
            else:
                h, p, e, hr, er, pr, sxe, sxo = moved
        else:
            (out,) = call(
                functools.partial(last_kernel, sizes, layer),
                (h, p, hr, pr, *got, *node, res),
                (),
                ((features.shape, BF16, "out"),),
                (pltpu.VMEM((ch * rows, nz), F32),),
            )
    return out


def solution(mesh):
    placed = (
        P(None, "gx", "gy", "gz"),
        P(None, None, "gx", "gy", "gz"),
        P("gx", "gy", "gz"),
        P(),
        P(),
        P(),
        P(),
        P(),
        P(),
    )
    return jax.shard_map(
        on_device, mesh=mesh, in_specs=placed, out_specs=P(None, "gx", "gy", "gz"), check_vma=False
    )
```

```python
import functools

import jax
import jax.numpy as jnp
from jax import lax
from jax.experimental import pallas as pl
from jax.experimental.pallas import tpu as pltpu
from jax.sharding import PartitionSpec as P


F32 = jnp.float32
BF16 = jnp.bfloat16
LANES = 128
AXES = ("gx", "gy", "gz")


def even_pairs(count):
    return [(i, i ^ 1) for i in range(count)]


def odd_pairs(axis, spare):
    sizes = [lax.axis_size(a) for a in AXES]
    at, other = AXES.index(axis), AXES.index(spare)
    pairs = []
    for i in range(sizes[0]):
        for j in range(sizes[1]):
            for k in range(sizes[2]):
                here = [i, j, k]
                there = list(here)
                if 0 < here[at] < sizes[at] - 1:
                    there[at] = ((here[at] + 1) ^ 1) - 1
                else:
                    there[other] = here[other] ^ 1
                flat = [(v[0] * sizes[1] + v[1]) * sizes[2] + v[2] for v in (here, there)]
                pairs.append(tuple(flat))
    return pairs


def exchange(even, odd, axis, spare):
    got_odd = lax.ppermute(odd, AXES, odd_pairs(axis, spare))
    got_even = lax.ppermute(even, axis, even_pairs(lax.axis_size(axis)))
    return got_even, got_odd


def silu(v):
    half = 0.5 * v
    return half + half * jnp.tanh(half)


def column(row):
    width = row.shape[1]
    eye = lax.broadcasted_iota(jnp.int32, (width, width), 0) == lax.broadcasted_iota(
        jnp.int32, (width, width), 1
    )
    return jnp.sum(jnp.where(eye, row, 0.0), axis=1, keepdims=True)


def tile(values, k):
    return values[:, k * LANES : (k + 1) * LANES]


def turn(values, shift):
    shift %= LANES
    return pltpu.roll(values, shift, 1) if shift else values


def place(axis, got_even, got_odd):
    position, count = lax.axis_index(axis), lax.axis_size(axis)
    is_even = position % 2 == 0
    low = jnp.where(is_even, got_odd, got_even)
    high = jnp.where(is_even, got_even, got_odd)
    low = jnp.where(position > 0, low, 0.0)
    high = jnp.where(position < count - 1, high, 0.0)
    return low, high


def lanes_of(rows=32):
    return lax.broadcasted_iota(jnp.int32, (rows, LANES), 1)


def perceptron(w_in, bias, w_out, pieces):
    stacked = jnp.concatenate([p.astype(BF16) for p in pieces], axis=0)
    pre = jnp.dot(w_in, stacked, preferred_element_type=F32) + bias
    return jnp.dot(w_out, silu(pre).astype(BF16), preferred_element_type=F32)


def batch(w_in, bias, w_out, groups):
    stacked = [jnp.concatenate([p.astype(BF16) for p in pieces], axis=0) for pieces in groups]
    out = perceptron(w_in, bias, w_out, [jnp.concatenate(stacked, axis=1)])
    ends, results = 0, []
    for piece in stacked:
        results.append(out[:, ends : ends + piece.shape[1]])
        ends += piece.shape[1]
    return results


def rim_groups(sizes, h, e):
    nx, ny = sizes
    lane = lanes_of()
    at, y_at = lane % 4, (lane // 4) % ny
    x_step = 4 * ny
    outer = len(h) == 5
    a, b, d, t = h[:4]
    o = h[4] if outer else jnp.zeros_like(a)
    ahead_z = [
        jnp.where(at < 3, turn(a, -1), 0.0),
        jnp.where(at < 3, turn(b, -1), d),
        jnp.where(at < 2, turn(d, -1), jnp.where(at == 2, o, turn(o, 2))),
        jnp.where(at == 0, a, jnp.where(at < 3, turn(t, -1), 0.0)),
    ]
    if outer:
        ahead_z.append(jnp.where(at == 0, t, jnp.where(at == 3, turn(t, 2), 0.0)))
    ahead_x = [jnp.where(lane < x_step * (nx - 1), turn(v, -x_step), 0.0) for v in h]
    ahead_y = [jnp.where(y_at < ny - 1, turn(v, -4), 0.0) for v in h]
    cur = jnp.concatenate(h, axis=1)
    return [
        [cur, jnp.concatenate(shifted, axis=1), e[k]]
        for k, shifted in enumerate((ahead_x, ahead_y, ahead_z))
    ]


def rim_sums(sizes, messages, w):
    at = lanes_of() % 4
    count = len(w)
    wx, wy, wz = (
        [tile(msg, i) * w[i][k : k + 1, :] for i in range(count)] for k, msg in enumerate(messages)
    )
    wo = wz[4] if count == 5 else jnp.zeros_like(wz[0])
    behind = [
        jnp.where(at == 0, wz[3], turn(wz[0], 1)),
        jnp.where(at == 0, 0.0, turn(wz[1], 1)),
        jnp.where(at == 3, wz[1], jnp.where(at == 0, 0.0, turn(wz[2], 1))),
        jnp.where(at == 0, wo, jnp.where(at == 1, turn(wo, -2), turn(wz[3], 1))),
    ]
    return [
        wx[i] + wy[i] + wz[i] + turn(wx[i], 4 * sizes[1]) + turn(wy[i], 4) + behind[i]
        for i in range(4)
    ]


def quarters(lane, parts):
    q = lane // 32
    return jnp.where(
        q == 0, parts[0], jnp.where(q == 1, parts[1], jnp.where(q == 2, parts[2], parts[3]))
    )


def rim_x_faces(sums):
    lane = lanes_of()
    low = quarters(lane, [turn(v, 32 * i) for i, v in enumerate(sums)])
    high = quarters(lane, [turn(v, 32 * i - 64) for i, v in enumerate(sums)])
    return low, high


def rim_add_x(sums, low, high):
    q = lanes_of() // 32
    return [
        v
        + jnp.where(q == 0, turn(low, -32 * i), 0.0)
        + jnp.where(q == 2, turn(high, 64 - 32 * i), 0.0)
        for i, v in enumerate(sums)
    ]


def rim_y_faces(sums):
    group = (lanes_of() // 4) % 8
    faces = []
    for first in (0, 28):
        face = jnp.zeros_like(sums[0])
        for i, v in enumerate(sums):
            face = jnp.where(group == i, turn(v, 4 * i - first), face)
        faces.append(jnp.where(group[:16] < 4, face[:16], turn(face[16:], 16)))
    return faces


def rim_add_y(sums, low, high):
    group = (lanes_of() // 4) % 8
    low, high = (jnp.concatenate([v, turn(v, -16)], axis=0) for v in (low, high))
    return [
        v
        + jnp.where(group == 0, turn(low, -4 * i), 0.0)
        + jnp.where(group == 7, turn(high, 28 - 4 * i), 0.0)
        for i, v in enumerate(sums)
    ]


def rim_join_z(sums):
    a, b, d, t = sums
    at = lanes_of() % 4
    return [
        a + jnp.where(at == 3, turn(d, 3), 0.0),
        b + jnp.where(at == 0, turn(t, -3), 0.0),
        d + jnp.where(at == 0, turn(a, -3), 0.0),
        t + jnp.where(at == 3, turn(b, 3), 0.0),
    ]


def span_of(first, count):
    return slice(first * LANES, (first + count) * LANES)


def ahead_along_z(values):
    lane = lanes_of()
    return jnp.concatenate(
        [
            jnp.where(lane < LANES - 1, turn(tile(values, k).astype(F32), -1), 0.0).astype(BF16)
            for k in range(values.shape[1] // LANES)
        ],
        axis=1,
    )


def edge_rows(sizes, first, count, last, h_ref, e_in, e_out, w_ref, w_in, w_out, bias, p_ref):
    nx, ny = sizes
    whole = first + count == ny
    groups = []
    for x in range(nx):
        k0 = x * ny + first
        cur = h_ref[:, span_of(k0, count)]
        ahead_x = h_ref[:, span_of(k0 + ny, count)] if x + 1 < nx else jnp.zeros_like(cur)
        ahead_y = cur[:, LANES:]
        if whole:
            ahead_y = jnp.concatenate([ahead_y, jnp.zeros((32, LANES), BF16)], axis=1)
        for d, shifted in enumerate((ahead_x, ahead_y, ahead_along_z(cur))):
            n = shifted.shape[1]
            groups.append([cur[:, :n], shifted, e_in[d, :, k0 * LANES : k0 * LANES + n]])
    messages = batch(w_in, bias, w_out, groups)
    prev_x = None
    for x in range(nx):
        k0 = x * ny + first
        mine = messages[3 * x : 3 * x + 3]
        weighted = []
        for d, msg in enumerate(mine):
            n = msg.shape[1]
            if not last:
                part = slice(k0 * LANES, k0 * LANES + n)
                e_out[d, :, part] = (groups[3 * x + d][2].astype(F32) + msg).astype(BF16)
            weighted.append(
                [tile(msg, i) * w_ref[k0 + i, d : d + 1, :] for i in range(n // LANES)]
            )
        wx, wy, wz = weighted
        for i in range(count):
            acc = wx[i] + wz[i] + turn(wz[i], 1)
            if i < len(wy):
                acc = acc + wy[i]
            if i > 0:
                acc = acc + wy[i - 1]
            if x > 0:
                acc = acc + prev_x[i]
            p_ref[:, span_of(k0 + i, 1)] = acc
        prev_x = wx


def write_x_faces(sizes, p_ref, sums, sxe, sxo):
    nx, ny = sizes
    span = ny * LANES
    low_rim, high_rim = rim_x_faces(sums)
    is_even = lax.axis_index("gx") % 2 == 0
    sxe[:, span:] = jnp.where(is_even, high_rim, low_rim)
    sxo[:, span:] = jnp.where(is_even, low_rim, high_rim)
    low = slice(0, span)
    high = slice((nx - 1) * span, nx * span)

    @pl.when(is_even)
    def _():
        sxe[:, :span] = p_ref[:, high]
        sxo[:, :span] = p_ref[:, low]

    @pl.when(jnp.logical_not(is_even))
    def _():
        sxe[:, :span] = p_ref[:, low]
        sxo[:, :span] = p_ref[:, high]


ENDS = ((-1, 4), (0, 0))
NEXT = ((1, -4), (-2, 8))


def collect(dest, first, size, parts, rows, row_of):
    group = lanes_of(size) // 4
    found = [jnp.zeros((size, LANES), F32)] * len(parts)
    for k in range(rows):
        turned = turn(row_of(k), 4 * k)
        for i, (step, _) in enumerate(parts):
            found[i] = jnp.where(group == (k + step) % 32, turned, found[i])
    for i, (_, back) in enumerate(parts):
        dest[i, first : first + size, :] = turn(found[i], back)


def unpack_kernel(
    sizes, f_in, es_in, m_in, buf, w_ref, own_ref, sze, szo, f_ref, es_ref, m_ref, sems
):
    nx, ny = sizes
    rows = nx * ny
    fetches = [pltpu.make_async_copy(m_in, m_ref, sems.at[0])]
    fetches.append(pltpu.make_async_copy(f_in, f_ref, sems.at[1]))
    for d in range(3):
        fetches.append(pltpu.make_async_copy(es_in.at[d], es_ref.at[d], sems.at[2 + d]))
    for fetch in fetches:
        fetch.start()
    fetches[0].wait()
    counts = m_ref[...]
    fluid = counts[1, 1:2, 1:2] > 0
    lane = lax.broadcasted_iota(jnp.int32, (ny, LANES), 1)
    sub = lax.broadcasted_iota(jnp.int32, (ny, LANES), 0)
    for x in range(nx):
        here = counts[x]
        shares = []
        for d in range(3):
            if d == 0:
                there = counts[x + 1] if x + 1 < nx else jnp.zeros_like(here)
            elif d == 1:
                there = jnp.where(sub < ny - 1, pltpu.roll(here, ny - 1, 0), 0)
            else:
                there = jnp.where(lane < LANES - 1, pltpu.roll(here, LANES - 1, 1), 0)
            shared = jnp.minimum(here, there)
            share = 1.0 / jnp.maximum(shared, 1).astype(F32)
            shares.append(jnp.where(fluid & (shared > 0), share, 0.0))
        for y in range(ny):
            for d in range(3):
                w_ref[x * ny + y, d : d + 1, :] = shares[d][y : y + 1, :]
            w_ref[x * ny + y, 3:8, :] = jnp.zeros((5, LANES), F32)

    for field in range(4):
        fetches[1 + field].wait()
        source = f_ref[...] if field == 0 else es_ref[field - 1]
        buf[field] = source.astype(F32).reshape(buf.shape[1:])
        collect(
            own_ref, 32 * field, 32, ENDS, rows,
            lambda k, field=field: buf[field, pl.ds(k, 32, stride=rows), :],
        )
    collect(own_ref, 128, 8, ENDS, rows, lambda k: w_ref[k])
    is_even = lax.axis_index("gz") % 2 == 0
    sze[...] = jnp.where(is_even, own_ref[0], own_ref[1])
    szo[...] = jnp.where(is_even, own_ref[1], own_ref[0])


def first_edges(sizes, buf, w_ref, win, wout, bias, h_ref, e_out, p_ref, next_ref, e_ref):
    nx, ny = sizes
    rows = nx * ny
    for field in range(4):

        def row_of(k, field=field):
            t = buf[field, pl.ds(k, 32, stride=rows), :]
            if field == 0:
                h_ref[:, span_of(k, 1)] = t.astype(BF16)
            else:
                e_ref[field - 1, :, span_of(k, 1)] = t.astype(BF16)
            return t

        collect(next_ref, 32 * field, 32, NEXT, rows, row_of)
    collect(next_ref, 128, 8, NEXT, rows, lambda k: w_ref[k])
    edge_rows(
        sizes, 0, ny, False, h_ref, e_ref, e_out, w_ref, win[0], wout[0], column(bias[0:1, :]), p_ref
    )


def first_rim(
    sizes, p_ref, own_ref, next_ref, rze, rzo, win, wout, bias, hr_out, er_out, wr_out, pr_out, sxe, sxo
):
    at = lanes_of(own_ref.shape[1]) % 4
    own_a, own_b = own_ref[0], own_ref[1]
    upper, lower = next_ref[0], next_ref[1]
    prev, nxt = place("gz", rze[...], rzo[...])
    tiles = [
        own_a,
        own_b,
        jnp.where(at == 3, turn(upper, 3), nxt),
        jnp.where(at == 0, turn(lower, -3), prev),
        jnp.where(
            at == 0,
            turn(lower, -2),
            jnp.where(at == 1, upper, jnp.where(at == 2, turn(nxt, -1), turn(prev, 3))),
        ),
    ]
    h = [t[0:32] for t in tiles]
    e = [jnp.concatenate([t[32 * (d + 1) : 32 * (d + 2)] for t in tiles], axis=1) for d in range(3)]
    w = [t[128:136] for t in tiles]
    messages = batch(win[0], column(bias[0:1, :]), wout[0], rim_groups(sizes, h, e))
    sums = rim_sums(sizes, messages, w)
    for i in range(4):
        hr_out[:, i * LANES : (i + 1) * LANES] = h[i].astype(BF16)
        wr_out[:, i * LANES : (i + 1) * LANES] = w[i]
    for d in range(3):
        er_out[d] = (e[d] + messages[d])[:, : 4 * LANES].astype(BF16)
    write_x_faces(sizes, p_ref, sums, sxe, sxo)
    for i in range(4):
        pr_out[:, i * LANES : (i + 1) * LANES] = sums[i]


def y_faces(sizes, p_ref, pr_ref, rxe, rxo, sye, syo, pr_out):
    nx, ny = sizes
    low_x, high_x = place("gx", rxe[...], rxo[...])
    sums = rim_add_x([tile(pr_ref, i) for i in range(4)], tile(low_x, ny), tile(high_x, ny))
    for i in range(4):
        pr_out[:, i * LANES : (i + 1) * LANES] = sums[i]
    faces = []
    for y, rim in zip((0, ny - 1), rim_y_faces(sums)):
        pieces = []
        for x in range(nx):
            t = p_ref[:, (x * ny + y) * LANES : (x * ny + y + 1) * LANES]
            if x == 0:
                t = t + tile(low_x, y)
            if x == nx - 1:
                t = t + tile(high_x, y)
            pieces.append(t)
        faces.append(jnp.concatenate(pieces + [rim], axis=0))
    low, high = faces
    is_even = lax.axis_index("gy") % 2 == 0
    sye[...] = jnp.where(is_even, high, low)
    syo[...] = jnp.where(is_even, low, high)


def incoming(sizes, p_ref, faces_x, faces_y, x, y):
    nx, ny = sizes
    t = p_ref[:, span_of(x * ny + y, 1)]
    if x == 0:
        t = t + tile(faces_x[0], y)
    if x == nx - 1:
        t = t + tile(faces_x[1], y)
    if y == 0:
        t = t + faces_y[0][32 * x : 32 * x + 32]
    if y == ny - 1:
        t = t + faces_y[1][32 * x : 32 * x + 32]
    return t.astype(BF16)


def inner_nodes(sizes, layer, h_in, p_in, rxe, rxo, nin, nout, nbias, write):
    nx, ny = sizes
    faces_x = place("gx", rxe[...], rxo[...])
    w_in, w_out = nin[layer], nout[layer]
    b = column(nbias[layer : layer + 1, :])
    spans = [span_of(x * ny + 1, ny - 2) for x in range(nx)]
    groups = []
    for x in range(nx):
        pieces = [incoming(sizes, p_in, faces_x, None, x, y) for y in range(1, ny - 1)]
        groups.append([h_in[:, spans[x]], jnp.concatenate(pieces, axis=1)])
    for rows, group, res in zip(spans, groups, batch(w_in, b, w_out, groups)):
        write(rows, group[0].astype(F32) + res)


def outer_nodes(sizes, layer, h_in, p_in, hr_in, pr_in, rxe, rxo, rye, ryo, nin, nout, nbias):
    nx, ny = sizes
    faces_x = place("gx", rxe[...], rxo[...])
    faces_y = place("gy", rye[...], ryo[...])
    w_in, w_out = nin[layer], nout[layer]
    b = column(nbias[layer : layer + 1, :])
    sums = [tile(pr_in, i) for i in range(4)]
    rim = rim_join_z(rim_add_y(sums, faces_y[0][32 * nx :], faces_y[1][32 * nx :]))
    outer = [(x, y) for x in range(nx) for y in (0, ny - 1)]
    cur = jnp.concatenate(
        [hr_in[...]] + [h_in[:, span_of(x * ny + y, 1)] for x, y in outer], axis=1
    )
    inc = jnp.concatenate(
        [t.astype(BF16) for t in rim]
        + [incoming(sizes, p_in, faces_x, faces_y, x, y) for x, y in outer],
        axis=1,
    )
    new = cur.astype(F32) + perceptron(w_in, b, w_out, [cur, inc])
    return new[:, : 4 * LANES], new[:, 4 * LANES :]


def inner_kernel(
    sizes, layer, last, h_in, p_in, rxe, rxo, nin, nout, nbias, win, wout, bias, e_in, w_in,
    h_out, p_out, e_out, w_out, sems,
):
    ny = sizes[1]
    fetch_e = pltpu.make_async_copy(e_in, e_out, sems.at[0])
    fetch_w = pltpu.make_async_copy(w_in, w_out, sems.at[1])
    fetch_e.start()
    fetch_w.start()

    def write(rows, value):
        h_out[:, rows] = value.astype(BF16)

    inner_nodes(sizes, layer, h_in, p_in, rxe, rxo, nin, nout, nbias, write)
    layer += 1
    fetch_e.wait()
    fetch_w.wait()
    edge_rows(
        sizes, 1, ny - 2, last, h_out, e_out, e_out, w_out, win[layer], wout[layer],
        column(bias[layer : layer + 1, :]), p_out,
    )


def outer_kernel(
    sizes, layer, last, h_in, p_in, hr_in, er_in, wr_in, pr_in, rxe, rxo, rye, ryo, nin, nout, nbias,
    win, wout, bias, w_ref, h_new, p_new, e_new, *outs,
):
    nx, ny = sizes
    if last:
        h_out, p_out, hr_out, pr_out, sxe, sxo = outs
    else:
        h_out, p_out, e_out, hr_out, er_out, pr_out, sxe, sxo = outs
    rim_h, edge_h = outer_nodes(
        sizes, layer, h_in, p_in, hr_in, pr_in, rxe, rxo, rye, ryo, nin, nout, nbias
    )
    rim_h, edge_h = rim_h.astype(BF16), edge_h.astype(BF16)
    hr_out[...] = rim_h
    outer = [(x, y) for x in range(nx) for y in (0, ny - 1)]
    for i, (x, y) in enumerate(outer):
        h_out[:, span_of(x * ny + y, 1)] = tile(edge_h, i)
    layer += 1
    b = column(bias[layer : layer + 1, :])
    w_in, w_out = win[layer], wout[layer]
    zero = jnp.zeros((32, LANES), BF16)
    mine = {place_of: tile(edge_h, i) for i, place_of in enumerate(outer)}
    cross = [(x, y) for x in range(nx) for y in (0, ny - 2, ny - 1)]
    from_y, to_y = [], []
    for x, y in cross:
        from_y.append(mine[x, y] if (x, y) in mine else h_new[:, span_of(x * ny + y, 1)])
        to_y.append(
            h_new[:, span_of(x * ny + 1, 1)] if y == 0 else mine[x, ny - 1] if y == ny - 2 else zero
        )
    ahead_x = jnp.concatenate([edge_h[:, 2 * LANES :], zero, zero], axis=1)
    kinds = (
        (outer, edge_h, ahead_x),
        (cross, jnp.concatenate(from_y, axis=1), jnp.concatenate(to_y, axis=1)),
        (outer, edge_h, ahead_along_z(edge_h)),
    )
    groups = rim_groups(
        sizes, [tile(rim_h, i).astype(F32) for i in range(4)], [er_in[d] for d in range(3)]
    )
    for d, (at, cur, ahead) in enumerate(kinds):
        edge = jnp.concatenate([e_new[d, :, span_of(x * ny + y, 1)] for x, y in at], axis=1)
        groups.append([cur, ahead, edge])
    messages = batch(w_in, b, w_out, groups)
    sums = rim_sums(sizes, messages[:3], [tile(wr_in, i) for i in range(4)])
    for i in range(4):
        pr_out[:, i * LANES : (i + 1) * LANES] = sums[i]
    if not last:
        for d in range(3):
            er_out[d] = (er_in[d].astype(F32) + messages[d]).astype(BF16)
    weighted = []
    for d, (at, _, _) in enumerate(kinds):
        msg = messages[3 + d]
        if not last:
            value = (groups[3 + d][2].astype(F32) + msg).astype(BF16)
            for i, (x, y) in enumerate(at):
                e_out[d, :, span_of(x * ny + y, 1)] = tile(value, i)
        weighted.append(
            {
                (x, y): tile(msg, i) * w_ref[x * ny + y, d : d + 1, :]
                for i, (x, y) in enumerate(at)
            }
        )
    wx, wy, wz = weighted
    for x in range(nx):
        for y in (0, ny - 1):
            acc = wx[x, y] + wz[x, y] + turn(wz[x, y], 1) + wy[x, y]
            if x > 0:
                acc = acc + wx[x - 1, y]
            if y > 0:
                acc = acc + wy[x, y - 1]
            p_out[:, span_of(x * ny + y, 1)] = acc
        for y, add in ((1, wy[x, 0]), (ny - 2, wy[x, ny - 2])):
            p_out[:, span_of(x * ny + y, 1)] = p_new[:, span_of(x * ny + y, 1)] + add
    write_x_faces(sizes, p_out, sums, sxe, sxo)


def last_inner(sizes, layer, h_in, p_in, rxe, rxo, nin, nout, nbias, res):
    def write(rows, value):
        res[:, rows] = value

    inner_nodes(sizes, layer, h_in, p_in, rxe, rxo, nin, nout, nbias, write)


def last_kernel(
    sizes, layer, h_in, p_in, hr_in, pr_in, rxe, rxo, rye, ryo, nin, nout, nbias, res, out, buf
):
    nx, ny = sizes
    rows = nx * ny
    rim_h, edge_h = outer_nodes(
        sizes, layer, h_in, p_in, hr_in, pr_in, rxe, rxo, rye, ryo, nin, nout, nbias
    )
    lane = lanes_of()
    upper = turn(tile(rim_h, 0), -4)
    lower = tile(rim_h, 1)
    for k in range(rows):
        x, y = divmod(k, ny)
        inside = 0 < y < ny - 1
        t = res[:, span_of(k, 1)] if inside else tile(edge_h, 2 * x + (y > 0))
        t = jnp.where(lane < 3, turn(lower, -4 * k), t)
        t = jnp.where(lane >= LANES - 3, turn(upper, -4 * k), t)
        buf[pl.ds(k, 32, stride=rows), :] = t
    out[...] = buf[...].reshape(out.shape).astype(BF16)


def call(body, fast, slow, outs, scratch=(), flops=0, aliases=()):
    vmem = pl.BlockSpec(memory_space=pltpu.VMEM)
    anywhere = pl.BlockSpec(memory_space=pl.ANY)
    fast = [pltpu.with_memory_space_constraint(a, pltpu.VMEM) for a in fast]
    if not fast:
        anywhere = pl.BlockSpec(memory_space=pltpu.HBM)
        slow = [pltpu.with_memory_space_constraint(a, pltpu.HBM) for a in slow]
    return pl.pallas_call(
        body,
        out_shape=[
            pltpu.VMEM(s, d) if where == "fast" else jax.ShapeDtypeStruct(s, d)
            for s, d, where in outs
        ],
        in_specs=[vmem] * len(fast) + [anywhere] * len(slow),
        out_specs=[vmem] * len(outs),
        scratch_shapes=list(scratch),
        input_output_aliases=dict(aliases),
        compiler_params=pltpu.CompilerParams(vmem_limit_bytes=12 * 2**20),
        cost_estimate=pl.CostEstimate(flops=flops, bytes_accessed=0, transcendentals=0),
    )(*fast, *slow)


def on_device(
    features, edge_state, multiplicity, edge_in, edge_out, edge_bias, node_in, node_out, node_bias
):
    ch, nx, ny, nz = features.shape
    layers = edge_in.shape[0]
    sizes = (nx, ny)
    rows = nx * ny
    nodes = rows * nz
    h_t = ((ch, nodes), BF16, "fast")
    p_t = ((ch, nodes), F32, "fast")
    e_shape = (3, ch, nodes)
    e_t = (e_shape, BF16, "fast")
    w_t = ((rows, 8, nz), F32, "fast")
    sx_t = ((ch, (ny + 1) * nz), F32, "fast")
    sy_t = ((ch * nx + ch // 2, nz), F32, "fast")
    hr_t = ((ch, 4 * LANES), BF16, "fast")
    er_t = ((3, ch, 4 * LANES), BF16, "fast")
    wr_t = ((8, 4 * LANES), F32, "fast")
    pr_t = ((ch, 4 * LANES), F32, "fast")
    z_rows = 4 * ch + 8
    sz_t = ((z_rows, LANES), F32, "fast")
    work = 4 * 2 * 5 * 3 * ch * ch * nodes

    ends_t = ((2, z_rows, LANES), F32, "fast")
    buf, w, own, sze, szo = call(
        functools.partial(unpack_kernel, sizes),
        (),
        (features, edge_state, multiplicity),
        (((4, ch * rows, nz), F32, "fast"), w_t, ends_t, sz_t, sz_t),
        (
            pltpu.VMEM(features.shape, BF16),
            pltpu.VMEM(edge_state.shape, BF16),
            pltpu.VMEM(multiplicity.shape, jnp.int32),
            pltpu.SemaphoreType.DMA((5,)),
        ),
    )
    rze, rzo = exchange(sze, szo, "gz", "gx")
    edge = (edge_in, edge_out, edge_bias)
    node = (node_in, node_out, node_bias)
    h, e, p, nearby = call(
        functools.partial(first_edges, sizes),
        (buf, w, *edge),
        (),
        (h_t, e_t, p_t, ends_t),
        (pltpu.VMEM(e_shape, BF16),),
        flops=work,
    )
    hr, er, wr, pr, sxe, sxo = call(
        functools.partial(first_rim, sizes),
        (p, own, nearby, rze, rzo, *edge),
        (),
        (hr_t, er_t, wr_t, pr_t, sx_t, sx_t),
    )
    for layer in range(layers):
        got_x = exchange(sxe, sxo, "gx", "gz")
        sye, syo, pr = call(
            functools.partial(y_faces, sizes), (p, pr, *got_x), (), (sy_t, sy_t, pr_t)
        )
        got = (*got_x, *exchange(sye, syo, "gy", "gx"))
        if layer + 1 < layers:
            last = layer + 2 == layers
            h_new, p_new, e_new, w_new = call(
                functools.partial(inner_kernel, sizes, layer, last),
                (h, p, *got_x, *node, *edge),
                (e, w),
                (h_t, p_t, e_t, w_t),
                (pltpu.SemaphoreType.DMA((2,)),),
                flops=work,
            )
        else:
            (res,) = call(
                functools.partial(last_inner, sizes, layer),
                (h, p, *got_x, *node),
                (),
                (((ch, nodes), F32, "fast"),),
                flops=work,
            )
        if layer + 1 < layers:
            outs = (hr_t, pr_t, sx_t, sx_t) if last else (e_t, hr_t, er_t, pr_t, sx_t, sx_t)
            args = (h, p, hr, er, wr, pr, *got, *node, *edge, w_new, h_new, p_new, e_new)
            n = len(args)
            moved = call(
                functools.partial(outer_kernel, sizes, layer, last),
                args,
                (),
                (h_t, p_t, *outs),
                aliases=((n - 3, 0), (n - 2, 1)) + (() if last else ((n - 1, 2),)),
            )
            if last:
                h, p, hr, pr, sxe, sxo = moved
            else:
                h, p, e, hr, er, pr, sxe, sxo = moved
        else:
            (out,) = call(
                functools.partial(last_kernel, sizes, layer),
                (h, p, hr, pr, *got, *node, res),
                (),
                ((features.shape, BF16, "out"),),
                (pltpu.VMEM((ch * rows, nz), F32),),
            )
    return out


def solution(mesh):
    placed = (
        P(None, "gx", "gy", "gz"),
        P(None, None, "gx", "gy", "gz"),
        P("gx", "gy", "gz"),
        P(),
        P(),
        P(),
        P(),
        P(),
        P(),
    )
    return jax.shard_map(
        on_device, mesh=mesh, in_specs=placed, out_specs=P(None, "gx", "gy", "gz"), check_vma=False
    )
```

```python
import functools

import jax
import jax.numpy as jnp
from jax import lax
from jax.experimental import pallas as pl
from jax.experimental.pallas import tpu as pltpu
from jax.sharding import PartitionSpec as P


F32 = jnp.float32
BF16 = jnp.bfloat16
LANES = 128
AXES = ("gx", "gy", "gz")


def even_pairs(count):
    return [(i, i ^ 1) for i in range(count)]


def odd_pairs(axis, spare):
    sizes = [lax.axis_size(a) for a in AXES]
    at, other = AXES.index(axis), AXES.index(spare)
    pairs = []
    for i in range(sizes[0]):
        for j in range(sizes[1]):
            for k in range(sizes[2]):
                here = [i, j, k]
                there = list(here)
                if 0 < here[at] < sizes[at] - 1:
                    there[at] = ((here[at] + 1) ^ 1) - 1
                else:
                    there[other] = here[other] ^ 1
                flat = [(v[0] * sizes[1] + v[1]) * sizes[2] + v[2] for v in (here, there)]
                pairs.append(tuple(flat))
    return pairs


def send_even(values, axis):
    return lax.ppermute(values, axis, even_pairs(lax.axis_size(axis)))


def send_odd(values, axis, spare):
    return lax.ppermute(values, AXES, odd_pairs(axis, spare))


def exchange(even, odd, axis, spare):
    return send_even(even, axis), send_odd(odd, axis, spare)


def silu(v):
    half = 0.5 * v
    return half + half * jnp.tanh(half)


def column(row):
    width = row.shape[1]
    eye = lax.broadcasted_iota(jnp.int32, (width, width), 0) == lax.broadcasted_iota(
        jnp.int32, (width, width), 1
    )
    return jnp.sum(jnp.where(eye, row, 0.0), axis=1, keepdims=True)


def tile(values, k):
    return values[:, k * LANES : (k + 1) * LANES]


def turn(values, shift):
    shift %= LANES
    return pltpu.roll(values, shift, 1) if shift else values


def place(axis, got_even, got_odd):
    position, count = lax.axis_index(axis), lax.axis_size(axis)
    is_even = position % 2 == 0
    low = jnp.where(is_even, got_odd, got_even)
    high = jnp.where(is_even, got_even, got_odd)
    low = jnp.where(position > 0, low, 0.0)
    high = jnp.where(position < count - 1, high, 0.0)
    return low, high


def lanes_of(rows=32):
    return lax.broadcasted_iota(jnp.int32, (rows, LANES), 1)


def perceptron(w_in, bias, w_out, pieces):
    stacked = jnp.concatenate([p.astype(BF16) for p in pieces], axis=0)
    pre = jnp.dot(w_in, stacked, preferred_element_type=F32) + bias
    return jnp.dot(w_out, silu(pre).astype(BF16), preferred_element_type=F32)


def batch(w_in, bias, w_out, groups):
    stacked = [jnp.concatenate([p.astype(BF16) for p in pieces], axis=0) for pieces in groups]
    out = perceptron(w_in, bias, w_out, [jnp.concatenate(stacked, axis=1)])
    ends, results = 0, []
    for piece in stacked:
        results.append(out[:, ends : ends + piece.shape[1]])
        ends += piece.shape[1]
    return results


def rim_groups(sizes, h, e):
    nx, ny = sizes
    lane = lanes_of()
    at, y_at = lane % 4, (lane // 4) % ny
    x_step = 4 * ny
    outer = len(h) == 5
    a, b, d, t = h[:4]
    o = h[4] if outer else jnp.zeros_like(a)
    ahead_z = [
        jnp.where(at < 3, turn(a, -1), 0.0),
        jnp.where(at < 3, turn(b, -1), d),
        jnp.where(at < 2, turn(d, -1), jnp.where(at == 2, o, turn(o, 2))),
        jnp.where(at == 0, a, jnp.where(at < 3, turn(t, -1), 0.0)),
    ]
    if outer:
        ahead_z.append(jnp.where(at == 0, t, jnp.where(at == 3, turn(t, 2), 0.0)))
    ahead_x = [jnp.where(lane < x_step * (nx - 1), turn(v, -x_step), 0.0) for v in h]
    ahead_y = [jnp.where(y_at < ny - 1, turn(v, -4), 0.0) for v in h]
    cur = jnp.concatenate(h, axis=1)
    return [
        [cur, jnp.concatenate(shifted, axis=1), e[k]]
        for k, shifted in enumerate((ahead_x, ahead_y, ahead_z))
    ]


def rim_sums(sizes, messages, w):
    at = lanes_of() % 4
    count = len(w)
    wx, wy, wz = (
        [tile(msg, i) * w[i][k : k + 1, :] for i in range(count)] for k, msg in enumerate(messages)
    )
    wo = wz[4] if count == 5 else jnp.zeros_like(wz[0])
    behind = [
        jnp.where(at == 0, wz[3], turn(wz[0], 1)),
        jnp.where(at == 0, 0.0, turn(wz[1], 1)),
        jnp.where(at == 3, wz[1], jnp.where(at == 0, 0.0, turn(wz[2], 1))),
        jnp.where(at == 0, wo, jnp.where(at == 1, turn(wo, -2), turn(wz[3], 1))),
    ]
    return [
        wx[i] + wy[i] + wz[i] + turn(wx[i], 4 * sizes[1]) + turn(wy[i], 4) + behind[i]
        for i in range(4)
    ]


def quarters(lane, parts):
    q = lane // 32
    return jnp.where(
        q == 0, parts[0], jnp.where(q == 1, parts[1], jnp.where(q == 2, parts[2], parts[3]))
    )


def rim_x_faces(sums):
    lane = lanes_of()
    low = quarters(lane, [turn(v, 32 * i) for i, v in enumerate(sums)])
    high = quarters(lane, [turn(v, 32 * i - 64) for i, v in enumerate(sums)])
    return low, high


def rim_add_x(sums, low, high):
    q = lanes_of() // 32
    return [
        v
        + jnp.where(q == 0, turn(low, -32 * i), 0.0)
        + jnp.where(q == 2, turn(high, 64 - 32 * i), 0.0)
        for i, v in enumerate(sums)
    ]


def rim_y_faces(sums):
    group = (lanes_of() // 4) % 8
    faces = []
    for first in (0, 28):
        face = jnp.zeros_like(sums[0])
        for i, v in enumerate(sums):
            face = jnp.where(group == i, turn(v, 4 * i - first), face)
        faces.append(jnp.where(group[:16] < 4, face[:16], turn(face[16:], 16)))
    return faces


def rim_add_y(sums, low, high):
    group = (lanes_of() // 4) % 8
    low, high = (jnp.concatenate([v, turn(v, -16)], axis=0) for v in (low, high))
    return [
        v
        + jnp.where(group == 0, turn(low, -4 * i), 0.0)
        + jnp.where(group == 7, turn(high, 28 - 4 * i), 0.0)
        for i, v in enumerate(sums)
    ]


def rim_join_z(sums):
    a, b, d, t = sums
    at = lanes_of() % 4
    return [
        a + jnp.where(at == 3, turn(d, 3), 0.0),
        b + jnp.where(at == 0, turn(t, -3), 0.0),
        d + jnp.where(at == 0, turn(a, -3), 0.0),
        t + jnp.where(at == 3, turn(b, 3), 0.0),
    ]


def span_of(first, count):
    return slice(first * LANES, (first + count) * LANES)


def ahead_along_z(values):
    lane = lanes_of()
    return jnp.concatenate(
        [
            jnp.where(lane < LANES - 1, turn(tile(values, k).astype(F32), -1), 0.0).astype(BF16)
            for k in range(values.shape[1] // LANES)
        ],
        axis=1,
    )


def edge_rows(sizes, first, count, last, h_ref, e_in, e_out, w_ref, w_in, w_out, bias, p_ref):
    nx, ny = sizes
    whole = first + count == ny
    groups = []
    for x in range(nx):
        k0 = x * ny + first
        cur = h_ref[:, span_of(k0, count)]
        ahead_x = h_ref[:, span_of(k0 + ny, count)] if x + 1 < nx else jnp.zeros_like(cur)
        ahead_y = cur[:, LANES:]
        if whole:
            ahead_y = jnp.concatenate([ahead_y, jnp.zeros((32, LANES), BF16)], axis=1)
        for d, shifted in enumerate((ahead_x, ahead_y, ahead_along_z(cur))):
            n = shifted.shape[1]
            groups.append([cur[:, :n], shifted, e_in[d, :, k0 * LANES : k0 * LANES + n]])
    messages = batch(w_in, bias, w_out, groups)
    prev_x = None
    for x in range(nx):
        k0 = x * ny + first
        mine = messages[3 * x : 3 * x + 3]
        weighted = []
        for d, msg in enumerate(mine):
            n = msg.shape[1]
            if not last:
                part = slice(k0 * LANES, k0 * LANES + n)
                e_out[d, :, part] = (groups[3 * x + d][2].astype(F32) + msg).astype(BF16)
            weighted.append(
                [tile(msg, i) * w_ref[k0 + i, d : d + 1, :] for i in range(n // LANES)]
            )
        wx, wy, wz = weighted
        for i in range(count):
            acc = wx[i] + wz[i] + turn(wz[i], 1)
            if i < len(wy):
                acc = acc + wy[i]
            if i > 0:
                acc = acc + wy[i - 1]
            if x > 0:
                acc = acc + prev_x[i]
            p_ref[:, span_of(k0 + i, 1)] = acc
        prev_x = wx


def write_x_faces(sizes, p_ref, sums, sxe, sxa, sxb):
    nx, ny = sizes
    span = ny * LANES
    low_rim, high_rim = rim_x_faces(sums)
    is_even = lax.axis_index("gx") % 2 == 0
    sxe[:, span:] = jnp.where(is_even, high_rim, low_rim)
    sxa[:, 2 * LANES :] = jnp.where(is_even, low_rim, high_rim)
    low, high = 0, (nx - 1) * ny

    def odd(first):
        sxa[:, :LANES] = p_ref[:, span_of(first, 1)]
        sxa[:, LANES : 2 * LANES] = p_ref[:, span_of(first + ny - 1, 1)]
        sxb[...] = p_ref[:, span_of(first + 1, ny - 2)]

    @pl.when(is_even)
    def _():
        sxe[:, :span] = p_ref[:, span_of(high, ny)]
        odd(low)

    @pl.when(jnp.logical_not(is_even))
    def _():
        sxe[:, :span] = p_ref[:, span_of(low, ny)]
        odd(high)


def outer_x(ny, rxe, rxa, y):
    return place("gx", tile(rxe, y), tile(rxa, {0: 0, ny - 1: 1, ny: 2}[y]))


ENDS = ((-1, 4), (0, 0))
NEXT = ((1, -4), (-2, 8))


def collect(dest, first, size, parts, rows, row_of):
    group = lanes_of(size) // 4
    found = [jnp.zeros((size, LANES), F32)] * len(parts)
    for k in range(rows):
        turned = turn(row_of(k), 4 * k)
        for i, (step, _) in enumerate(parts):
            found[i] = jnp.where(group == (k + step) % 32, turned, found[i])
    for i, (_, back) in enumerate(parts):
        dest[i, first : first + size, :] = turn(found[i], back)


def unpack_kernel(
    sizes, f_in, es_in, m_in, buf, w_ref, own_ref, sze, szo, f_ref, es_ref, m_ref, sems
):
    nx, ny = sizes
    rows = nx * ny
    fetches = [pltpu.make_async_copy(m_in, m_ref, sems.at[0])]
    fetches.append(pltpu.make_async_copy(f_in, f_ref, sems.at[1]))
    for d in range(3):
        fetches.append(pltpu.make_async_copy(es_in.at[d], es_ref.at[d], sems.at[2 + d]))
    for fetch in fetches:
        fetch.start()
    fetches[0].wait()
    counts = m_ref[...]
    fluid = counts[1, 1:2, 1:2] > 0
    lane = lax.broadcasted_iota(jnp.int32, (ny, LANES), 1)
    sub = lax.broadcasted_iota(jnp.int32, (ny, LANES), 0)
    for x in range(nx):
        here = counts[x]
        shares = []
        for d in range(3):
            if d == 0:
                there = counts[x + 1] if x + 1 < nx else jnp.zeros_like(here)
            elif d == 1:
                there = jnp.where(sub < ny - 1, pltpu.roll(here, ny - 1, 0), 0)
            else:
                there = jnp.where(lane < LANES - 1, pltpu.roll(here, LANES - 1, 1), 0)
            shared = jnp.minimum(here, there)
            share = 1.0 / jnp.maximum(shared, 1).astype(F32)
            shares.append(jnp.where(fluid & (shared > 0), share, 0.0))
        for y in range(ny):
            for d in range(3):
                w_ref[x * ny + y, d : d + 1, :] = shares[d][y : y + 1, :]
            w_ref[x * ny + y, 3:8, :] = jnp.zeros((5, LANES), F32)

    for field in range(4):
        fetches[1 + field].wait()
        source = f_ref[...] if field == 0 else es_ref[field - 1]
        buf[field] = source.astype(F32).reshape(buf.shape[1:])
        collect(
            own_ref, 32 * field, 32, ENDS, rows,
            lambda k, field=field: buf[field, pl.ds(k, 32, stride=rows), :],
        )
    collect(own_ref, 128, 8, ENDS, rows, lambda k: w_ref[k])
    is_even = lax.axis_index("gz") % 2 == 0
    sze[...] = jnp.where(is_even, own_ref[0], own_ref[1])
    szo[...] = jnp.where(is_even, own_ref[1], own_ref[0])


def first_edges(sizes, buf, w_ref, win, wout, bias, h_ref, e_out, p_ref, next_ref, e_ref):
    nx, ny = sizes
    rows = nx * ny
    for field in range(4):

        def row_of(k, field=field):
            t = buf[field, pl.ds(k, 32, stride=rows), :]
            if field == 0:
                h_ref[:, span_of(k, 1)] = t.astype(BF16)
            else:
                e_ref[field - 1, :, span_of(k, 1)] = t.astype(BF16)
            return t

        collect(next_ref, 32 * field, 32, NEXT, rows, row_of)
    collect(next_ref, 128, 8, NEXT, rows, lambda k: w_ref[k])
    edge_rows(
        sizes, 0, ny, False, h_ref, e_ref, e_out, w_ref, win[0], wout[0], column(bias[0:1, :]), p_ref
    )


def first_rim(
    sizes, p_ref, own_ref, next_ref, rze, rzo, win, wout, bias, hr_out, er_out, wr_out, pr_out, sxe, sxa, sxb
):
    at = lanes_of(own_ref.shape[1]) % 4
    own_a, own_b = own_ref[0], own_ref[1]
    upper, lower = next_ref[0], next_ref[1]
    prev, nxt = place("gz", rze[...], rzo[...])
    tiles = [
        own_a,
        own_b,
        jnp.where(at == 3, turn(upper, 3), nxt),
        jnp.where(at == 0, turn(lower, -3), prev),
        jnp.where(
            at == 0,
            turn(lower, -2),
            jnp.where(at == 1, upper, jnp.where(at == 2, turn(nxt, -1), turn(prev, 3))),
        ),
    ]
    h = [t[0:32] for t in tiles]
    e = [jnp.concatenate([t[32 * (d + 1) : 32 * (d + 2)] for t in tiles], axis=1) for d in range(3)]
    w = [t[128:136] for t in tiles]
    messages = batch(win[0], column(bias[0:1, :]), wout[0], rim_groups(sizes, h, e))
    sums = rim_sums(sizes, messages, w)
    for i in range(4):
        hr_out[:, i * LANES : (i + 1) * LANES] = h[i].astype(BF16)
        wr_out[:, i * LANES : (i + 1) * LANES] = w[i]
    for d in range(3):
        er_out[d] = (e[d] + messages[d])[:, : 4 * LANES].astype(BF16)
    write_x_faces(sizes, p_ref, sums, sxe, sxa, sxb)
    for i in range(4):
        pr_out[:, i * LANES : (i + 1) * LANES] = sums[i]


def y_faces(sizes, p_ref, pr_ref, rxe, rxa, sye, syo, pr_out):
    nx, ny = sizes
    sums = rim_add_x([tile(pr_ref, i) for i in range(4)], *outer_x(ny, rxe, rxa, ny))
    for i in range(4):
        pr_out[:, i * LANES : (i + 1) * LANES] = sums[i]
    faces = []
    for y, rim in zip((0, ny - 1), rim_y_faces(sums)):
        low_x, high_x = outer_x(ny, rxe, rxa, y)
        pieces = []
        for x in range(nx):
            t = p_ref[:, span_of(x * ny + y, 1)]
            if x == 0:
                t = t + low_x
            if x == nx - 1:
                t = t + high_x
            pieces.append(t)
        faces.append(jnp.concatenate(pieces + [rim], axis=0))
    low, high = faces
    is_even = lax.axis_index("gy") % 2 == 0
    sye[...] = jnp.where(is_even, high, low)
    syo[...] = jnp.where(is_even, low, high)


def incoming(sizes, p_ref, faces_x, faces_y, x, y):
    nx, ny = sizes
    t = p_ref[:, span_of(x * ny + y, 1)]
    if x == 0:
        t = t + faces_x[y][0]
    if x == nx - 1:
        t = t + faces_x[y][1]
    if y == 0:
        t = t + faces_y[0][32 * x : 32 * x + 32]
    if y == ny - 1:
        t = t + faces_y[1][32 * x : 32 * x + 32]
    return t.astype(BF16)


def inner_nodes(sizes, layer, h_in, p_in, rxe, rxb, nin, nout, nbias, write):
    nx, ny = sizes
    faces_x = {y: place("gx", tile(rxe, y), tile(rxb, y - 1)) for y in range(1, ny - 1)}
    w_in, w_out = nin[layer], nout[layer]
    b = column(nbias[layer : layer + 1, :])
    spans = [span_of(x * ny + 1, ny - 2) for x in range(nx)]
    groups = []
    for x in range(nx):
        pieces = [incoming(sizes, p_in, faces_x, None, x, y) for y in range(1, ny - 1)]
        groups.append([h_in[:, spans[x]], jnp.concatenate(pieces, axis=1)])
    for rows, group, res in zip(spans, groups, batch(w_in, b, w_out, groups)):
        write(rows, group[0].astype(F32) + res)


def outer_nodes(sizes, layer, h_in, p_in, hr_in, pr_in, rxe, rxa, rye, ryo, nin, nout, nbias):
    nx, ny = sizes
    faces_x = {y: outer_x(ny, rxe, rxa, y) for y in (0, ny - 1)}
    faces_y = place("gy", rye[...], ryo[...])
    w_in, w_out = nin[layer], nout[layer]
    b = column(nbias[layer : layer + 1, :])
    sums = [tile(pr_in, i) for i in range(4)]
    rim = rim_join_z(rim_add_y(sums, faces_y[0][32 * nx :], faces_y[1][32 * nx :]))
    outer = [(x, y) for x in range(nx) for y in (0, ny - 1)]
    cur = jnp.concatenate(
        [hr_in[...]] + [h_in[:, span_of(x * ny + y, 1)] for x, y in outer], axis=1
    )
    inc = jnp.concatenate(
        [t.astype(BF16) for t in rim]
        + [incoming(sizes, p_in, faces_x, faces_y, x, y) for x, y in outer],
        axis=1,
    )
    new = cur.astype(F32) + perceptron(w_in, b, w_out, [cur, inc])
    return new[:, : 4 * LANES], new[:, 4 * LANES :]


def inner_kernel(
    sizes, layer, last, h_in, p_in, rxe, rxb, nin, nout, nbias, win, wout, bias, e_in, w_in,
    h_out, p_out, e_out, w_out, sems,
):
    ny = sizes[1]
    fetch_e = pltpu.make_async_copy(e_in, e_out, sems.at[0])
    fetch_w = pltpu.make_async_copy(w_in, w_out, sems.at[1])
    fetch_e.start()
    fetch_w.start()

    def write(rows, value):
        h_out[:, rows] = value.astype(BF16)

    inner_nodes(sizes, layer, h_in, p_in, rxe, rxb, nin, nout, nbias, write)
    layer += 1
    fetch_e.wait()
    fetch_w.wait()
    edge_rows(
        sizes, 1, ny - 2, last, h_out, e_out, e_out, w_out, win[layer], wout[layer],
        column(bias[layer : layer + 1, :]), p_out,
    )


def outer_kernel(
    sizes, layer, last, h_in, p_in, hr_in, er_in, wr_in, pr_in, rxe, rxa, rye, ryo, nin, nout, nbias,
    win, wout, bias, w_ref, h_new, p_new, e_new, *outs,
):
    nx, ny = sizes
    if last:
        h_out, p_out, hr_out, pr_out, sxe, sxa, sxb = outs
    else:
        h_out, p_out, e_out, hr_out, er_out, pr_out, sxe, sxa, sxb = outs
    rim_h, edge_h = outer_nodes(
        sizes, layer, h_in, p_in, hr_in, pr_in, rxe, rxa, rye, ryo, nin, nout, nbias
    )
    rim_h, edge_h = rim_h.astype(BF16), edge_h.astype(BF16)
    hr_out[...] = rim_h
    outer = [(x, y) for x in range(nx) for y in (0, ny - 1)]
    for i, (x, y) in enumerate(outer):
        h_out[:, span_of(x * ny + y, 1)] = tile(edge_h, i)
    layer += 1
    b = column(bias[layer : layer + 1, :])
    w_in, w_out = win[layer], wout[layer]
    zero = jnp.zeros((32, LANES), BF16)
    mine = {place_of: tile(edge_h, i) for i, place_of in enumerate(outer)}
    cross = [(x, y) for x in range(nx) for y in (0, ny - 2, ny - 1)]
    from_y, to_y = [], []
    for x, y in cross:
        from_y.append(mine[x, y] if (x, y) in mine else h_new[:, span_of(x * ny + y, 1)])
        to_y.append(
            h_new[:, span_of(x * ny + 1, 1)] if y == 0 else mine[x, ny - 1] if y == ny - 2 else zero
        )
    ahead_x = jnp.concatenate([edge_h[:, 2 * LANES :], zero, zero], axis=1)
    kinds = (
        (outer, edge_h, ahead_x),
        (cross, jnp.concatenate(from_y, axis=1), jnp.concatenate(to_y, axis=1)),
        (outer, edge_h, ahead_along_z(edge_h)),
    )
    groups = rim_groups(
        sizes, [tile(rim_h, i).astype(F32) for i in range(4)], [er_in[d] for d in range(3)]
    )
    for d, (at, cur, ahead) in enumerate(kinds):
        edge = jnp.concatenate([e_new[d, :, span_of(x * ny + y, 1)] for x, y in at], axis=1)
        groups.append([cur, ahead, edge])
    messages = batch(w_in, b, w_out, groups)
    sums = rim_sums(sizes, messages[:3], [tile(wr_in, i) for i in range(4)])
    for i in range(4):
        pr_out[:, i * LANES : (i + 1) * LANES] = sums[i]
    if not last:
        for d in range(3):
            er_out[d] = (er_in[d].astype(F32) + messages[d]).astype(BF16)
    weighted = []
    for d, (at, _, _) in enumerate(kinds):
        msg = messages[3 + d]
        if not last:
            value = (groups[3 + d][2].astype(F32) + msg).astype(BF16)
            for i, (x, y) in enumerate(at):
                e_out[d, :, span_of(x * ny + y, 1)] = tile(value, i)
        weighted.append(
            {
                (x, y): tile(msg, i) * w_ref[x * ny + y, d : d + 1, :]
                for i, (x, y) in enumerate(at)
            }
        )
    wx, wy, wz = weighted
    for x in range(nx):
        for y in (0, ny - 1):
            acc = wx[x, y] + wz[x, y] + turn(wz[x, y], 1) + wy[x, y]
            if x > 0:
                acc = acc + wx[x - 1, y]
            if y > 0:
                acc = acc + wy[x, y - 1]
            p_out[:, span_of(x * ny + y, 1)] = acc
        for y, add in ((1, wy[x, 0]), (ny - 2, wy[x, ny - 2])):
            p_out[:, span_of(x * ny + y, 1)] = p_new[:, span_of(x * ny + y, 1)] + add
    write_x_faces(sizes, p_out, sums, sxe, sxa, sxb)


def last_inner(sizes, layer, h_in, p_in, rxe, rxb, nin, nout, nbias, res):
    def write(rows, value):
        res[:, rows] = value

    inner_nodes(sizes, layer, h_in, p_in, rxe, rxb, nin, nout, nbias, write)


def last_kernel(
    sizes, layer, h_in, p_in, hr_in, pr_in, rxe, rxa, rye, ryo, nin, nout, nbias, res, out, buf
):
    nx, ny = sizes
    rows = nx * ny
    rim_h, edge_h = outer_nodes(
        sizes, layer, h_in, p_in, hr_in, pr_in, rxe, rxa, rye, ryo, nin, nout, nbias
    )
    lane = lanes_of()
    upper = turn(tile(rim_h, 0), -4)
    lower = tile(rim_h, 1)
    for k in range(rows):
        x, y = divmod(k, ny)
        inside = 0 < y < ny - 1
        t = res[:, span_of(k, 1)] if inside else tile(edge_h, 2 * x + (y > 0))
        t = jnp.where(lane < 3, turn(lower, -4 * k), t)
        t = jnp.where(lane >= LANES - 3, turn(upper, -4 * k), t)
        buf[pl.ds(k, 32, stride=rows), :] = t
    out[...] = buf[...].reshape(out.shape).astype(BF16)


def call(body, fast, slow, outs, scratch=(), flops=0, aliases=()):
    vmem = pl.BlockSpec(memory_space=pltpu.VMEM)
    anywhere = pl.BlockSpec(memory_space=pl.ANY)
    fast = [pltpu.with_memory_space_constraint(a, pltpu.VMEM) for a in fast]
    if not fast:
        anywhere = pl.BlockSpec(memory_space=pltpu.HBM)
        slow = [pltpu.with_memory_space_constraint(a, pltpu.HBM) for a in slow]
    return pl.pallas_call(
        body,
        out_shape=[
            pltpu.VMEM(s, d) if where == "fast" else jax.ShapeDtypeStruct(s, d)
            for s, d, where in outs
        ],
        in_specs=[vmem] * len(fast) + [anywhere] * len(slow),
        out_specs=[vmem] * len(outs),
        scratch_shapes=list(scratch),
        input_output_aliases=dict(aliases),
        compiler_params=pltpu.CompilerParams(vmem_limit_bytes=12 * 2**20),
        cost_estimate=pl.CostEstimate(flops=flops, bytes_accessed=0, transcendentals=0),
    )(*fast, *slow)


def on_device(
    features, edge_state, multiplicity, edge_in, edge_out, edge_bias, node_in, node_out, node_bias
):
    ch, nx, ny, nz = features.shape
    layers = edge_in.shape[0]
    sizes = (nx, ny)
    rows = nx * ny
    nodes = rows * nz
    h_t = ((ch, nodes), BF16, "fast")
    p_t = ((ch, nodes), F32, "fast")
    e_shape = (3, ch, nodes)
    e_t = (e_shape, BF16, "fast")
    w_t = ((rows, 8, nz), F32, "fast")
    sx_t = tuple(((ch, n * nz), F32, "fast") for n in (ny + 1, 3, ny - 2))
    sy_t = ((ch * nx + ch // 2, nz), F32, "fast")
    hr_t = ((ch, 4 * LANES), BF16, "fast")
    er_t = ((3, ch, 4 * LANES), BF16, "fast")
    wr_t = ((8, 4 * LANES), F32, "fast")
    pr_t = ((ch, 4 * LANES), F32, "fast")
    z_rows = 4 * ch + 8
    sz_t = ((z_rows, LANES), F32, "fast")
    work = 4 * 2 * 5 * 3 * ch * ch * nodes

    ends_t = ((2, z_rows, LANES), F32, "fast")
    buf, w, own, sze, szo = call(
        functools.partial(unpack_kernel, sizes),
        (),
        (features, edge_state, multiplicity),
        (((4, ch * rows, nz), F32, "fast"), w_t, ends_t, sz_t, sz_t),
        (
            pltpu.VMEM(features.shape, BF16),
            pltpu.VMEM(edge_state.shape, BF16),
            pltpu.VMEM(multiplicity.shape, jnp.int32),
            pltpu.SemaphoreType.DMA((5,)),
        ),
    )
    rze, rzo = exchange(sze, szo, "gz", "gx")
    edge = (edge_in, edge_out, edge_bias)
    node = (node_in, node_out, node_bias)
    h, e, p, nearby = call(
        functools.partial(first_edges, sizes),
        (buf, w, *edge),
        (),
        (h_t, e_t, p_t, ends_t),
        (pltpu.VMEM(e_shape, BF16),),
        flops=work,
    )
    hr, er, wr, pr, sxe, sxa, sxb = call(
        functools.partial(first_rim, sizes),
        (p, own, nearby, rze, rzo, *edge),
        (),
        (hr_t, er_t, wr_t, pr_t, *sx_t),
    )
    for layer in range(layers):
        rxe = send_even(sxe, "gx")
        rxa = send_odd(sxa, "gx", "gz")
        rxb = send_odd(sxb, "gx", "gz")
        sye, syo, pr = call(
            functools.partial(y_faces, sizes), (p, pr, rxe, rxa), (), (sy_t, sy_t, pr_t)
        )
        got = (rxe, rxa, *exchange(sye, syo, "gy", "gx"))
        if layer + 1 < layers:
            last = layer + 2 == layers
            h_new, p_new, e_new, w_new = call(
                functools.partial(inner_kernel, sizes, layer, last),
                (h, p, rxe, rxb, *node, *edge),
                (e, w),
                (h_t, p_t, e_t, w_t),
                (pltpu.SemaphoreType.DMA((2,)),),
                flops=work,
            )
        else:
            (res,) = call(
                functools.partial(last_inner, sizes, layer),
                (h, p, rxe, rxb, *node),
                (),
                (((ch, nodes), F32, "fast"),),
                flops=work,
            )
        if layer + 1 < layers:
            outs = (hr_t, pr_t, *sx_t) if last else (e_t, hr_t, er_t, pr_t, *sx_t)
            args = (h, p, hr, er, wr, pr, *got, *node, *edge, w_new, h_new, p_new, e_new)
            n = len(args)
            moved = call(
                functools.partial(outer_kernel, sizes, layer, last),
                args,
                (),
                (h_t, p_t, *outs),
                aliases=((n - 3, 0), (n - 2, 1)) + (() if last else ((n - 1, 2),)),
            )
            if last:
                h, p, hr, pr, sxe, sxa, sxb = moved
            else:
                h, p, e, hr, er, pr, sxe, sxa, sxb = moved
        else:
            (out,) = call(
                functools.partial(last_kernel, sizes, layer),
                (h, p, hr, pr, *got, *node, res),
                (),
                ((features.shape, BF16, "out"),),
                (pltpu.VMEM((ch * rows, nz), F32),),
            )
    return out


def solution(mesh):
    placed = (
        P(None, "gx", "gy", "gz"),
        P(None, None, "gx", "gy", "gz"),
        P("gx", "gy", "gz"),
        P(),
        P(),
        P(),
        P(),
        P(),
        P(),
    )
    return jax.shard_map(
        on_device, mesh=mesh, in_specs=placed, out_specs=P(None, "gx", "gy", "gz"), check_vma=False
    )
```

```python
import functools

import jax
import jax.numpy as jnp
from jax import lax
from jax.experimental import pallas as pl
from jax.experimental.pallas import tpu as pltpu
from jax.sharding import PartitionSpec as P


F32 = jnp.float32
BF16 = jnp.bfloat16
LANES = 128
AXES = ("gx", "gy", "gz")


def even_pairs(count):
    return [(i, i ^ 1) for i in range(count)]


def odd_pairs(axis, spare):
    sizes = [lax.axis_size(a) for a in AXES]
    at, other = AXES.index(axis), AXES.index(spare)
    pairs = []
    for i in range(sizes[0]):
        for j in range(sizes[1]):
            for k in range(sizes[2]):
                here = [i, j, k]
                there = list(here)
                if 0 < here[at] < sizes[at] - 1:
                    there[at] = ((here[at] + 1) ^ 1) - 1
                else:
                    there[other] = here[other] ^ 1
                flat = [(v[0] * sizes[1] + v[1]) * sizes[2] + v[2] for v in (here, there)]
                pairs.append(tuple(flat))
    return pairs


def send_even(values, axis):
    return lax.ppermute(values, axis, even_pairs(lax.axis_size(axis)))


def send_odd(values, axis, spare):
    return lax.ppermute(values, AXES, odd_pairs(axis, spare))


def exchange(even, odd, axis, spare):
    return send_even(even, axis), send_odd(odd, axis, spare)


def silu(v):
    half = 0.5 * v
    return half + half * jnp.tanh(half)


def column(row):
    width = row.shape[1]
    eye = lax.broadcasted_iota(jnp.int32, (width, width), 0) == lax.broadcasted_iota(
        jnp.int32, (width, width), 1
    )
    return jnp.sum(jnp.where(eye, row, 0.0), axis=1, keepdims=True)


def tile(values, k):
    return values[:, k * LANES : (k + 1) * LANES]


def turn(values, shift):
    shift %= LANES
    return pltpu.roll(values, shift, 1) if shift else values


def place(axis, got_even, got_odd):
    position, count = lax.axis_index(axis), lax.axis_size(axis)
    is_even = position % 2 == 0
    low = jnp.where(is_even, got_odd, got_even)
    high = jnp.where(is_even, got_even, got_odd)
    low = jnp.where(position > 0, low, 0.0)
    high = jnp.where(position < count - 1, high, 0.0)
    return low, high


def lanes_of(rows=32):
    return lax.broadcasted_iota(jnp.int32, (rows, LANES), 1)


def perceptron(w_in, bias, w_out, pieces):
    stacked = jnp.concatenate([p.astype(BF16) for p in pieces], axis=0)
    pre = jnp.dot(w_in, stacked, preferred_element_type=F32) + bias
    return jnp.dot(w_out, silu(pre).astype(BF16), preferred_element_type=F32)


def batch(w_in, bias, w_out, groups):
    stacked = [jnp.concatenate([p.astype(BF16) for p in pieces], axis=0) for pieces in groups]
    out = perceptron(w_in, bias, w_out, [jnp.concatenate(stacked, axis=1)])
    ends, results = 0, []
    for piece in stacked:
        results.append(out[:, ends : ends + piece.shape[1]])
        ends += piece.shape[1]
    return results


def rim_groups(sizes, h, e):
    nx, ny = sizes
    lane = lanes_of()
    at, y_at = lane % 4, (lane // 4) % ny
    x_step = 4 * ny
    outer = len(h) == 5
    a, b, d, t = h[:4]
    o = h[4] if outer else jnp.zeros_like(a)
    ahead_z = [
        jnp.where(at < 3, turn(a, -1), 0.0),
        jnp.where(at < 3, turn(b, -1), d),
        jnp.where(at < 2, turn(d, -1), jnp.where(at == 2, o, turn(o, 2))),
        jnp.where(at == 0, a, jnp.where(at < 3, turn(t, -1), 0.0)),
    ]
    if outer:
        ahead_z.append(jnp.where(at == 0, t, jnp.where(at == 3, turn(t, 2), 0.0)))
    ahead_x = [jnp.where(lane < x_step * (nx - 1), turn(v, -x_step), 0.0) for v in h]
    ahead_y = [jnp.where(y_at < ny - 1, turn(v, -4), 0.0) for v in h]
    cur = jnp.concatenate(h, axis=1)
    return [
        [cur, jnp.concatenate(shifted, axis=1), e[k]]
        for k, shifted in enumerate((ahead_x, ahead_y, ahead_z))
    ]


def rim_sums(sizes, messages, w):
    at = lanes_of() % 4
    count = len(w)
    wx, wy, wz = (
        [tile(msg, i) * w[i][k : k + 1, :] for i in range(count)] for k, msg in enumerate(messages)
    )
    wo = wz[4] if count == 5 else jnp.zeros_like(wz[0])
    behind = [
        jnp.where(at == 0, wz[3], turn(wz[0], 1)),
        jnp.where(at == 0, 0.0, turn(wz[1], 1)),
        jnp.where(at == 3, wz[1], jnp.where(at == 0, 0.0, turn(wz[2], 1))),
        jnp.where(at == 0, wo, jnp.where(at == 1, turn(wo, -2), turn(wz[3], 1))),
    ]
    return [
        wx[i] + wy[i] + wz[i] + turn(wx[i], 4 * sizes[1]) + turn(wy[i], 4) + behind[i]
        for i in range(4)
    ]


def quarters(lane, parts):
    q = lane // 32
    return jnp.where(
        q == 0, parts[0], jnp.where(q == 1, parts[1], jnp.where(q == 2, parts[2], parts[3]))
    )


def rim_x_faces(sums):
    lane = lanes_of()
    low = quarters(lane, [turn(v, 32 * i) for i, v in enumerate(sums)])
    high = quarters(lane, [turn(v, 32 * i - 64) for i, v in enumerate(sums)])
    return low, high


def rim_add_x(sums, low, high):
    q = lanes_of() // 32
    return [
        v
        + jnp.where(q == 0, turn(low, -32 * i), 0.0)
        + jnp.where(q == 2, turn(high, 64 - 32 * i), 0.0)
        for i, v in enumerate(sums)
    ]


def rim_y_faces(sums):
    group = (lanes_of() // 4) % 8
    faces = []
    for first in (0, 28):
        face = jnp.zeros_like(sums[0])
        for i, v in enumerate(sums):
            face = jnp.where(group == i, turn(v, 4 * i - first), face)
        faces.append(jnp.where(group[:16] < 4, face[:16], turn(face[16:], 16)))
    return faces


def rim_add_y(sums, low, high):
    group = (lanes_of() // 4) % 8
    low, high = (jnp.concatenate([v, turn(v, -16)], axis=0) for v in (low, high))
    return [
        v
        + jnp.where(group == 0, turn(low, -4 * i), 0.0)
        + jnp.where(group == 7, turn(high, 28 - 4 * i), 0.0)
        for i, v in enumerate(sums)
    ]


def rim_join_z(sums):
    a, b, d, t = sums
    at = lanes_of() % 4
    return [
        a + jnp.where(at == 3, turn(d, 3), 0.0),
        b + jnp.where(at == 0, turn(t, -3), 0.0),
        d + jnp.where(at == 0, turn(a, -3), 0.0),
        t + jnp.where(at == 3, turn(b, 3), 0.0),
    ]


def span_of(first, count):
    return slice(first * LANES, (first + count) * LANES)


def ahead_along_z(values):
    lane = lanes_of()
    return jnp.concatenate(
        [
            jnp.where(lane < LANES - 1, turn(tile(values, k).astype(F32), -1), 0.0).astype(BF16)
            for k in range(values.shape[1] // LANES)
        ],
        axis=1,
    )


def edge_rows(sizes, first, count, last, h_ref, e_in, e_out, w_ref, w_in, w_out, bias, p_ref):
    nx, ny = sizes
    whole = first + count == ny
    groups = []
    for x in range(nx):
        k0 = x * ny + first
        cur = h_ref[:, span_of(k0, count)]
        ahead_x = h_ref[:, span_of(k0 + ny, count)] if x + 1 < nx else jnp.zeros_like(cur)
        ahead_y = cur[:, LANES:]
        if whole:
            ahead_y = jnp.concatenate([ahead_y, jnp.zeros((32, LANES), BF16)], axis=1)
        for d, shifted in enumerate((ahead_x, ahead_y, ahead_along_z(cur))):
            n = shifted.shape[1]
            groups.append([cur[:, :n], shifted, e_in[d, :, k0 * LANES : k0 * LANES + n]])
    messages = batch(w_in, bias, w_out, groups)
    prev_x = None
    for x in range(nx):
        k0 = x * ny + first
        mine = messages[3 * x : 3 * x + 3]
        weighted = []
        for d, msg in enumerate(mine):
            n = msg.shape[1]
            if not last:
                part = slice(k0 * LANES, k0 * LANES + n)
                e_out[d, :, part] = (groups[3 * x + d][2].astype(F32) + msg).astype(BF16)
            weighted.append(
                [tile(msg, i) * w_ref[k0 + i, d : d + 1, :] for i in range(n // LANES)]
            )
        wx, wy, wz = weighted
        for i in range(count):
            acc = wx[i] + wz[i] + turn(wz[i], 1)
            if i < len(wy):
                acc = acc + wy[i]
            if i > 0:
                acc = acc + wy[i - 1]
            if x > 0:
                acc = acc + prev_x[i]
            p_ref[:, span_of(k0 + i, 1)] = acc
        prev_x = wx


def write_x_faces(sizes, p_ref, sums, sxe, sxa, sxb):
    nx, ny = sizes
    span = ny * LANES
    low_rim, high_rim = rim_x_faces(sums)
    is_even = lax.axis_index("gx") % 2 == 0
    sxe[:, span:] = jnp.where(is_even, high_rim, low_rim)
    sxa[:, 2 * LANES :] = jnp.where(is_even, low_rim, high_rim)
    low, high = 0, (nx - 1) * ny

    def odd(first):
        sxa[:, :LANES] = p_ref[:, span_of(first, 1)]
        sxa[:, LANES : 2 * LANES] = p_ref[:, span_of(first + ny - 1, 1)]
        sxb[...] = p_ref[:, span_of(first + 1, ny - 2)]

    @pl.when(is_even)
    def _():
        sxe[:, :span] = p_ref[:, span_of(high, ny)]
        odd(low)

    @pl.when(jnp.logical_not(is_even))
    def _():
        sxe[:, :span] = p_ref[:, span_of(low, ny)]
        odd(high)


def outer_x(ny, rxe, rxa, y):
    return place("gx", tile(rxe, y), tile(rxa, {0: 0, ny - 1: 1, ny: 2}[y]))


ENDS = ((-1, 4), (0, 0))
NEXT = ((1, -4), (-2, 8))


def collect(dest, first, size, parts, rows, row_of):
    group = lanes_of(size) // 4
    found = [jnp.zeros((size, LANES), F32)] * len(parts)
    for k in range(rows):
        turned = turn(row_of(k), 4 * k)
        for i, (step, _) in enumerate(parts):
            found[i] = jnp.where(group == (k + step) % 32, turned, found[i])
    for i, (_, back) in enumerate(parts):
        dest[i, first : first + size, :] = turn(found[i], back)


def pack_ends(v):
    free = lanes_of() >= 96
    e_z = v[96:128]
    pieces = [
        jnp.where(free, turn(e_z, 96 - 32 * i), v[32 * i : 32 * i + 32]) for i in range(3)
    ]
    return jnp.concatenate(pieces + [v[128:136]], axis=0)


def unpack_ends(v):
    lane = lanes_of()
    pieces = [v[32 * i : 32 * i + 32] for i in range(3)]
    e_z = jnp.zeros_like(pieces[0])
    for i, piece in enumerate(pieces):
        e_z = jnp.where(lane // 32 == i, turn(piece, 32 + 32 * i), e_z)
    pieces = [jnp.where(lane < 96, piece, 0.0) for piece in pieces]
    return jnp.concatenate(pieces + [e_z, v[96:104]], axis=0)


def unpack_kernel(
    sizes, f_in, es_in, m_in, *rest
):
    nx, ny = sizes
    rows = nx * ny
    weights, (buf, w_ref, own_ref, sze, szo), rest = rest[:6], rest[6:11], rest[11:]
    weights_out, (f_ref, es_ref, m_ref, sems) = rest[:6], rest[6:]
    fetches = [pltpu.make_async_copy(m_in, m_ref, sems.at[0])]
    fetches.append(pltpu.make_async_copy(f_in, f_ref, sems.at[1]))
    for d in range(3):
        fetches.append(pltpu.make_async_copy(es_in.at[d], es_ref.at[d], sems.at[2 + d]))
    for i, (source, dest) in enumerate(zip(weights, weights_out)):
        fetches.append(pltpu.make_async_copy(source, dest, sems.at[5 + i]))
    for fetch in fetches[:1] + fetches[5:] + fetches[1:5]:
        fetch.start()
    fetches[0].wait()
    counts = m_ref[...]
    fluid = counts[1, 1:2, 1:2] > 0
    lane = lax.broadcasted_iota(jnp.int32, (ny, LANES), 1)
    sub = lax.broadcasted_iota(jnp.int32, (ny, LANES), 0)
    for x in range(nx):
        here = counts[x]
        shares = []
        for d in range(3):
            if d == 0:
                there = counts[x + 1] if x + 1 < nx else jnp.zeros_like(here)
            elif d == 1:
                there = jnp.where(sub < ny - 1, pltpu.roll(here, ny - 1, 0), 0)
            else:
                there = jnp.where(lane < LANES - 1, pltpu.roll(here, LANES - 1, 1), 0)
            shared = jnp.minimum(here, there)
            share = 1.0 / jnp.maximum(shared, 1).astype(F32)
            shares.append(jnp.where(fluid & (shared > 0), share, 0.0))
        for y in range(ny):
            for d in range(3):
                w_ref[x * ny + y, d : d + 1, :] = shares[d][y : y + 1, :]
            w_ref[x * ny + y, 3:8, :] = jnp.zeros((5, LANES), F32)

    for field in range(4):
        fetches[1 + field].wait()
        source = f_ref[...] if field == 0 else es_ref[field - 1]
        buf[field] = source.astype(F32).reshape(buf.shape[1:])
        collect(
            own_ref, 32 * field, 32, ENDS, rows,
            lambda k, field=field: buf[field, pl.ds(k, 32, stride=rows), :],
        )
    collect(own_ref, 128, 8, ENDS, rows, lambda k: w_ref[k])
    is_even = lax.axis_index("gz") % 2 == 0
    lower, upper = pack_ends(own_ref[0]), pack_ends(own_ref[1])
    sze[...] = jnp.where(is_even, lower, upper)
    szo[...] = jnp.where(is_even, upper, lower)
    for fetch in fetches[5:]:
        fetch.wait()


def first_edges(sizes, buf, w_ref, win, wout, bias, h_ref, e_out, p_ref, next_ref, e_ref):
    nx, ny = sizes
    rows = nx * ny
    for field in range(4):

        def row_of(k, field=field):
            t = buf[field, pl.ds(k, 32, stride=rows), :]
            if field == 0:
                h_ref[:, span_of(k, 1)] = t.astype(BF16)
            else:
                e_ref[field - 1, :, span_of(k, 1)] = t.astype(BF16)
            return t

        collect(next_ref, 32 * field, 32, NEXT, rows, row_of)
    collect(next_ref, 128, 8, NEXT, rows, lambda k: w_ref[k])
    edge_rows(
        sizes, 0, ny, False, h_ref, e_ref, e_out, w_ref, win[0], wout[0], column(bias[0:1, :]), p_ref
    )


def first_rim(
    sizes, p_ref, own_ref, next_ref, rze, rzo, win, wout, bias, hr_out, er_out, wr_out, pr_out, sxe, sxa, sxb
):
    at = lanes_of(own_ref.shape[1]) % 4
    own_a, own_b = own_ref[0], own_ref[1]
    upper, lower = next_ref[0], next_ref[1]
    prev, nxt = (unpack_ends(v) for v in place("gz", rze[...], rzo[...]))
    tiles = [
        own_a,
        own_b,
        jnp.where(at == 3, turn(upper, 3), nxt),
        jnp.where(at == 0, turn(lower, -3), prev),
        jnp.where(
            at == 0,
            turn(lower, -2),
            jnp.where(at == 1, upper, jnp.where(at == 2, turn(nxt, -1), turn(prev, 3))),
        ),
    ]
    h = [t[0:32] for t in tiles]
    e = [jnp.concatenate([t[32 * (d + 1) : 32 * (d + 2)] for t in tiles], axis=1) for d in range(3)]
    w = [t[128:136] for t in tiles]
    messages = batch(win[0], column(bias[0:1, :]), wout[0], rim_groups(sizes, h, e))
    sums = rim_sums(sizes, messages, w)
    for i in range(4):
        hr_out[:, i * LANES : (i + 1) * LANES] = h[i].astype(BF16)
        wr_out[:, i * LANES : (i + 1) * LANES] = w[i]
    for d in range(3):
        er_out[d] = (e[d] + messages[d])[:, : 4 * LANES].astype(BF16)
    write_x_faces(sizes, p_ref, sums, sxe, sxa, sxb)
    for i in range(4):
        pr_out[:, i * LANES : (i + 1) * LANES] = sums[i]


def y_faces(sizes, p_ref, pr_ref, rxe, rxa, sye, syo, pr_out):
    nx, ny = sizes
    sums = rim_add_x([tile(pr_ref, i) for i in range(4)], *outer_x(ny, rxe, rxa, ny))
    for i in range(4):
        pr_out[:, i * LANES : (i + 1) * LANES] = sums[i]
    faces = []
    for y, rim in zip((0, ny - 1), rim_y_faces(sums)):
        low_x, high_x = outer_x(ny, rxe, rxa, y)
        pieces = []
        for x in range(nx):
            t = p_ref[:, span_of(x * ny + y, 1)]
            if x == 0:
                t = t + low_x
            if x == nx - 1:
                t = t + high_x
            pieces.append(t)
        faces.append(jnp.concatenate(pieces + [rim], axis=0))
    low, high = faces
    is_even = lax.axis_index("gy") % 2 == 0
    sye[...] = jnp.where(is_even, high, low)
    syo[...] = jnp.where(is_even, low, high)


def incoming(sizes, p_ref, faces_x, faces_y, x, y):
    nx, ny = sizes
    t = p_ref[:, span_of(x * ny + y, 1)]
    if x == 0:
        t = t + faces_x[y][0]
    if x == nx - 1:
        t = t + faces_x[y][1]
    if y == 0:
        t = t + faces_y[0][32 * x : 32 * x + 32]
    if y == ny - 1:
        t = t + faces_y[1][32 * x : 32 * x + 32]
    return t.astype(BF16)


def inner_nodes(sizes, layer, h_in, p_in, rxe, rxb, nin, nout, nbias, write):
    nx, ny = sizes
    faces_x = {y: place("gx", tile(rxe, y), tile(rxb, y - 1)) for y in range(1, ny - 1)}
    w_in, w_out = nin[layer], nout[layer]
    b = column(nbias[layer : layer + 1, :])
    spans = [span_of(x * ny + 1, ny - 2) for x in range(nx)]
    groups = []
    for x in range(nx):
        pieces = [incoming(sizes, p_in, faces_x, None, x, y) for y in range(1, ny - 1)]
        groups.append([h_in[:, spans[x]], jnp.concatenate(pieces, axis=1)])
    for rows, group, res in zip(spans, groups, batch(w_in, b, w_out, groups)):
        write(rows, group[0].astype(F32) + res)


def outer_nodes(sizes, layer, h_in, p_in, hr_in, pr_in, rxe, rxa, rye, ryo, nin, nout, nbias):
    nx, ny = sizes
    faces_x = {y: outer_x(ny, rxe, rxa, y) for y in (0, ny - 1)}
    faces_y = place("gy", rye[...], ryo[...])
    w_in, w_out = nin[layer], nout[layer]
    b = column(nbias[layer : layer + 1, :])
    sums = [tile(pr_in, i) for i in range(4)]
    rim = rim_join_z(rim_add_y(sums, faces_y[0][32 * nx :], faces_y[1][32 * nx :]))
    outer = [(x, y) for x in range(nx) for y in (0, ny - 1)]
    cur = jnp.concatenate(
        [hr_in[...]] + [h_in[:, span_of(x * ny + y, 1)] for x, y in outer], axis=1
    )
    inc = jnp.concatenate(
        [t.astype(BF16) for t in rim]
        + [incoming(sizes, p_in, faces_x, faces_y, x, y) for x, y in outer],
        axis=1,
    )
    new = cur.astype(F32) + perceptron(w_in, b, w_out, [cur, inc])
    return new[:, : 4 * LANES], new[:, 4 * LANES :]


def inner_kernel(
    sizes, layer, last, h_in, p_in, rxe, rxb, nin, nout, nbias, win, wout, bias, e_in, w_in,
    h_out, p_out, e_out, w_out, sems,
):
    ny = sizes[1]
    fetch_e = pltpu.make_async_copy(e_in, e_out, sems.at[0])
    fetch_w = pltpu.make_async_copy(w_in, w_out, sems.at[1])
    fetch_e.start()
    fetch_w.start()

    def write(rows, value):
        h_out[:, rows] = value.astype(BF16)

    inner_nodes(sizes, layer, h_in, p_in, rxe, rxb, nin, nout, nbias, write)
    layer += 1
    fetch_e.wait()
    fetch_w.wait()
    edge_rows(
        sizes, 1, ny - 2, last, h_out, e_out, e_out, w_out, win[layer], wout[layer],
        column(bias[layer : layer + 1, :]), p_out,
    )


def outer_kernel(
    sizes, layer, last, h_in, p_in, hr_in, er_in, wr_in, pr_in, rxe, rxa, rye, ryo, nin, nout, nbias,
    win, wout, bias, w_ref, h_new, p_new, e_new, *outs,
):
    nx, ny = sizes
    if last:
        h_out, p_out, hr_out, pr_out, sxe, sxa, sxb = outs
    else:
        h_out, p_out, e_out, hr_out, er_out, pr_out, sxe, sxa, sxb = outs
    rim_h, edge_h = outer_nodes(
        sizes, layer, h_in, p_in, hr_in, pr_in, rxe, rxa, rye, ryo, nin, nout, nbias
    )
    rim_h, edge_h = rim_h.astype(BF16), edge_h.astype(BF16)
    hr_out[...] = rim_h
    outer = [(x, y) for x in range(nx) for y in (0, ny - 1)]
    for i, (x, y) in enumerate(outer):
        h_out[:, span_of(x * ny + y, 1)] = tile(edge_h, i)
    layer += 1
    b = column(bias[layer : layer + 1, :])
    w_in, w_out = win[layer], wout[layer]
    zero = jnp.zeros((32, LANES), BF16)
    mine = {place_of: tile(edge_h, i) for i, place_of in enumerate(outer)}
    cross = [(x, y) for x in range(nx) for y in (0, ny - 2, ny - 1)]
    from_y, to_y = [], []
    for x, y in cross:
        from_y.append(mine[x, y] if (x, y) in mine else h_new[:, span_of(x * ny + y, 1)])
        to_y.append(
            h_new[:, span_of(x * ny + 1, 1)] if y == 0 else mine[x, ny - 1] if y == ny - 2 else zero
        )
    ahead_x = jnp.concatenate([edge_h[:, 2 * LANES :], zero, zero], axis=1)
    kinds = (
        (outer, edge_h, ahead_x),
        (cross, jnp.concatenate(from_y, axis=1), jnp.concatenate(to_y, axis=1)),
        (outer, edge_h, ahead_along_z(edge_h)),
    )
    groups = rim_groups(
        sizes, [tile(rim_h, i).astype(F32) for i in range(4)], [er_in[d] for d in range(3)]
    )
    for d, (at, cur, ahead) in enumerate(kinds):
        edge = jnp.concatenate([e_new[d, :, span_of(x * ny + y, 1)] for x, y in at], axis=1)
        groups.append([cur, ahead, edge])
    messages = batch(w_in, b, w_out, groups)
    sums = rim_sums(sizes, messages[:3], [tile(wr_in, i) for i in range(4)])
    for i in range(4):
        pr_out[:, i * LANES : (i + 1) * LANES] = sums[i]
    if not last:
        for d in range(3):
            er_out[d] = (er_in[d].astype(F32) + messages[d]).astype(BF16)
    weighted = []
    for d, (at, _, _) in enumerate(kinds):
        msg = messages[3 + d]
        if not last:
            value = (groups[3 + d][2].astype(F32) + msg).astype(BF16)
            for i, (x, y) in enumerate(at):
                e_out[d, :, span_of(x * ny + y, 1)] = tile(value, i)
        weighted.append(
            {
                (x, y): tile(msg, i) * w_ref[x * ny + y, d : d + 1, :]
                for i, (x, y) in enumerate(at)
            }
        )
    wx, wy, wz = weighted
    for x in range(nx):
        for y in (0, ny - 1):
            acc = wx[x, y] + wz[x, y] + turn(wz[x, y], 1) + wy[x, y]
            if x > 0:
                acc = acc + wx[x - 1, y]
            if y > 0:
                acc = acc + wy[x, y - 1]
            p_out[:, span_of(x * ny + y, 1)] = acc
        for y, add in ((1, wy[x, 0]), (ny - 2, wy[x, ny - 2])):
            p_out[:, span_of(x * ny + y, 1)] = p_new[:, span_of(x * ny + y, 1)] + add
    write_x_faces(sizes, p_out, sums, sxe, sxa, sxb)


def last_inner(sizes, layer, h_in, p_in, rxe, rxb, nin, nout, nbias, res):
    def write(rows, value):
        res[:, rows] = value

    inner_nodes(sizes, layer, h_in, p_in, rxe, rxb, nin, nout, nbias, write)


def last_kernel(
    sizes, layer, h_in, p_in, hr_in, pr_in, rxe, rxa, rye, ryo, nin, nout, nbias, res, out, buf, done, sems
):
    nx, ny = sizes
    rows = nx * ny
    rim_h, edge_h = outer_nodes(
        sizes, layer, h_in, p_in, hr_in, pr_in, rxe, rxa, rye, ryo, nin, nout, nbias
    )
    lane = lanes_of()
    upper = turn(tile(rim_h, 0), -4)
    lower = tile(rim_h, 1)
    sends = []
    for k in range(rows):
        x, y = divmod(k, ny)
        inside = 0 < y < ny - 1
        t = res[:, span_of(k, 1)] if inside else tile(edge_h, 2 * x + (y > 0))
        t = jnp.where(lane < 3, turn(lower, -4 * k), t)
        t = jnp.where(lane >= LANES - 3, turn(upper, -4 * k), t)
        buf[x, pl.ds(y, 32, stride=ny), :] = t
        if y == ny - 1:
            done[x] = buf[x].reshape(done.shape[1:]).astype(BF16)
            sends.append(pltpu.make_async_copy(done.at[x], out.at[:, x], sems.at[x]))
            sends[-1].start()
    for send in sends:
        send.wait()


def call(body, fast, slow, outs, scratch=(), flops=0, aliases=()):
    vmem = pl.BlockSpec(memory_space=pltpu.VMEM)
    anywhere = pl.BlockSpec(memory_space=pl.ANY)
    fast = [pltpu.with_memory_space_constraint(a, pltpu.VMEM) for a in fast]
    if not fast:
        anywhere = pl.BlockSpec(memory_space=pltpu.HBM)
        slow = [pltpu.with_memory_space_constraint(a, pltpu.HBM) for a in slow]
    return pl.pallas_call(
        body,
        out_shape=[
            pltpu.VMEM(s, d) if where == "fast" else jax.ShapeDtypeStruct(s, d)
            for s, d, where in outs
        ],
        in_specs=[vmem] * len(fast) + [anywhere] * len(slow),
        out_specs=[
            pl.BlockSpec(memory_space=pltpu.HBM) if where == "out" else vmem for _, _, where in outs
        ],
        scratch_shapes=list(scratch),
        input_output_aliases=dict(aliases),
        compiler_params=pltpu.CompilerParams(vmem_limit_bytes=12 * 2**20),
        cost_estimate=pl.CostEstimate(flops=flops, bytes_accessed=0, transcendentals=0),
    )(*fast, *slow)


def on_device(
    features, edge_state, multiplicity, edge_in, edge_out, edge_bias, node_in, node_out, node_bias
):
    ch, nx, ny, nz = features.shape
    layers = edge_in.shape[0]
    sizes = (nx, ny)
    rows = nx * ny
    nodes = rows * nz
    h_t = ((ch, nodes), BF16, "fast")
    p_t = ((ch, nodes), F32, "fast")
    e_shape = (3, ch, nodes)
    e_t = (e_shape, BF16, "fast")
    w_t = ((rows, 8, nz), F32, "fast")
    sx_t = tuple(((ch, n * nz), F32, "fast") for n in (ny + 1, 3, ny - 2))
    sy_t = ((ch * nx + ch // 2, nz), F32, "fast")
    hr_t = ((ch, 4 * LANES), BF16, "fast")
    er_t = ((3, ch, 4 * LANES), BF16, "fast")
    wr_t = ((8, 4 * LANES), F32, "fast")
    pr_t = ((ch, 4 * LANES), F32, "fast")
    z_rows = 4 * ch + 8
    sz_t = ((3 * ch + 8, LANES), F32, "fast")
    work = 4 * 2 * 5 * 3 * ch * ch * nodes

    ends_t = ((2, z_rows, LANES), F32, "fast")
    weights = (edge_in, edge_out, edge_bias, node_in, node_out, node_bias)
    buf, w, own, sze, szo, *weights = call(
        functools.partial(unpack_kernel, sizes),
        (),
        (features, edge_state, multiplicity, *weights),
        (
            ((4, ch * rows, nz), F32, "fast"), w_t, ends_t, sz_t, sz_t,
            *((v.shape, v.dtype, "fast") for v in weights),
        ),
        (
            pltpu.VMEM(features.shape, BF16),
            pltpu.VMEM(edge_state.shape, BF16),
            pltpu.VMEM(multiplicity.shape, jnp.int32),
            pltpu.SemaphoreType.DMA((11,)),
        ),
    )
    rze, rzo = exchange(sze, szo, "gz", "gx")
    edge, node = weights[:3], weights[3:]
    h, e, p, nearby = call(
        functools.partial(first_edges, sizes),
        (buf, w, *edge),
        (),
        (h_t, e_t, p_t, ends_t),
        (pltpu.VMEM(e_shape, BF16),),
        flops=work,
    )
    hr, er, wr, pr, sxe, sxa, sxb = call(
        functools.partial(first_rim, sizes),
        (p, own, nearby, rze, rzo, *edge),
        (),
        (hr_t, er_t, wr_t, pr_t, *sx_t),
    )
    for layer in range(layers):
        rxe = send_even(sxe, "gx")
        rxa = send_odd(sxa, "gx", "gz")
        rxb = send_odd(sxb, "gx", "gz")
        sye, syo, pr = call(
            functools.partial(y_faces, sizes), (p, pr, rxe, rxa), (), (sy_t, sy_t, pr_t)
        )
        got = (rxe, rxa, *exchange(sye, syo, "gy", "gx"))
        if layer + 1 < layers:
            last = layer + 2 == layers
            h_new, p_new, e_new, w_new = call(
                functools.partial(inner_kernel, sizes, layer, last),
                (h, p, rxe, rxb, *node, *edge),
                (e, w),
                (h_t, p_t, e_t, w_t),
                (pltpu.SemaphoreType.DMA((2,)),),
                flops=work,
            )
        else:
            (res,) = call(
                functools.partial(last_inner, sizes, layer),
                (h, p, rxe, rxb, *node),
                (),
                (((ch, nodes), F32, "fast"),),
                flops=work,
            )
        if layer + 1 < layers:
            outs = (hr_t, pr_t, *sx_t) if last else (e_t, hr_t, er_t, pr_t, *sx_t)
            args = (h, p, hr, er, wr, pr, *got, *node, *edge, w_new, h_new, p_new, e_new)
            n = len(args)
            moved = call(
                functools.partial(outer_kernel, sizes, layer, last),
                args,
                (),
                (h_t, p_t, *outs),
                aliases=((n - 3, 0), (n - 2, 1)) + (() if last else ((n - 1, 2),)),
            )
            if last:
                h, p, hr, pr, sxe, sxa, sxb = moved
            else:
                h, p, e, hr, er, pr, sxe, sxa, sxb = moved
        else:
            (out,) = call(
                functools.partial(last_kernel, sizes, layer),
                (h, p, hr, pr, *got, *node, res),
                (),
                ((features.shape, BF16, "out"),),
                (
                    pltpu.VMEM((nx, ch * ny, nz), F32),
                    pltpu.VMEM((nx, ch, ny, nz), BF16),
                    pltpu.SemaphoreType.DMA((nx,)),
                ),
            )
    return out


def solution(mesh):
    placed = (
        P(None, "gx", "gy", "gz"),
        P(None, None, "gx", "gy", "gz"),
        P("gx", "gy", "gz"),
        P(),
        P(),
        P(),
        P(),
        P(),
        P(),
    )
    return jax.shard_map(
        on_device, mesh=mesh, in_specs=placed, out_specs=P(None, "gx", "gy", "gz"), check_vma=False
    )
```
